256 devices in a mesh: row: 32 (over x_hi, z, core), col: 8 (over x_lo, y).
Axes of the slice: x: 4 (x_hi: 2, x_lo: 2; x = x_hi * 2 + x_lo), y: 4, z: 8, core: 2. Of those that a mesh axis runs over, the one named last changes fastest.
Arguments:
- occupied_waves: bfloat16 [1024, 32768], P('row', 'col'), may hold values from -6 to 6
- virtual_waves: bfloat16 [512, 32768], P('row', 'col'), may hold values from -6 to 6
- occupied_decay: float32 [1024], replicated, may hold values from 0.02 to 1
- virtual_decay: float32 [512], replicated, may hold values from 0.02 to 1
Outputs:
- spectrum_real: float32 [1024, 32, 1024], P('row', 'col')
- spectrum_imaginary: float32 [1024, 32, 1024], P('row', 'col')
The draws below stay inside these ranges and needn't reach their ends.
All inputs are finite; a program needn't handle non-finite values.
Results may differ from the reference program's by a relative error of at most 0.0041.
Values may be sent and summed in bfloat16 or wider, within the bound.
A program may use at most 64 MiB of HBM per device.

```python
import math
import jax
import jax.numpy as jnp
from jax import lax

NOCC = 1024
NVIR = 512
NA = 32
NB = 32
NC = 32
ROWS_DEV = 32
NGRID = 32768
N_ROW = 32


def steps_of(key, dims, pieces, smallest, high):
    loudness, own = 1.0, jax.random.fold_in(key, 6)
    for position, parts in pieces:
        heights = jnp.exp(jax.random.uniform(jax.random.fold_in(own, position), (parts,), jnp.float32, smallest / len(pieces), high / len(pieces)))
        loudness = loudness * jnp.repeat(heights, dims[position] // parts).reshape([-1 if axis == position else 1 for axis in range(len(dims))])
    return loudness


def noise(rng, extent, scale, limit, split=(), kind=jnp.bfloat16):
    drawn = scale * jax.random.normal(rng, extent, jnp.float32)
    if split:
        drawn = drawn * steps_of(rng, extent, split, -0.22, 0.18)
    return jnp.clip(drawn, -limit, limit).astype(kind)


def setup_inputs(seed: int = 0) -> dict:
    keys = jax.random.split(jax.random.key(seed), 5)
    return {
        "occupied_waves": noise(keys[0], (NOCC, NGRID), 1.0, 6.0, ((0, 32), (1, 8))),
        "virtual_waves": noise(keys[1], (NVIR, NGRID), 1.0, 6.0, ((0, 32), (1, 8))),
        "occupied_decay": jnp.clip(jnp.exp(jax.random.uniform(keys[2], (NOCC,), jnp.float32, math.log(0.02), math.log(1.0))), 0.02, 1.0),
        "virtual_decay": jnp.clip(jnp.exp(jax.random.uniform(keys[3], (NVIR,), jnp.float32, math.log(0.02), math.log(1.0))), 0.02, 1.0),
    }


def reference(occupied_waves, virtual_waves, occupied_decay, virtual_decay):
    rows_all = ROWS_DEV * N_ROW
    width = math.gcd(rows_all, 512)
    factor = -1.0 / math.sqrt(NOCC * NVIR)
    contract = (((0,), (0,)), ((), ()))

    def block(index):
        first = (index * width).astype(jnp.int32)
        occ_rows = lax.dynamic_slice_in_dim(occupied_waves, first, width, 1)
        occ_rows = (occ_rows.astype(jnp.float32) * occupied_decay[:, None]).astype(jnp.bfloat16)
        vir_rows = lax.dynamic_slice_in_dim(virtual_waves, first, width, 1)
        vir_rows = (vir_rows.astype(jnp.float32) * virtual_decay[:, None]).astype(jnp.bfloat16)
        green_occ = lax.dot_general(occupied_waves, occ_rows, contract, preferred_element_type=jnp.float32)
        green_vir = lax.dot_general(virtual_waves, vir_rows, contract, preferred_element_type=jnp.float32)
        polar = green_occ * green_vir * factor
        cube = polar.reshape(NA, NB, NC, width)
        spectrum = jnp.fft.fftn(cube, axes=(0, 1, 2)) / math.sqrt(NGRID)
        spectrum = jnp.transpose(spectrum, (3, 2, 0, 1)).reshape(width, NC, NA * NB)
        return (jnp.real(spectrum).astype(jnp.float32), jnp.imag(spectrum).astype(jnp.float32))
    real_part, imag_part = lax.map(block, jnp.arange(rows_all // width, dtype=jnp.int32))
    real_part = real_part.reshape(rows_all, NC, NA * NB)
    imag_part = imag_part.reshape(rows_all, NC, NA * NB)
    return (real_part, imag_part)
```

```python
import functools
import math

import jax
import jax.numpy as jnp
import numpy as np
from jax import lax
from jax.experimental import pallas as pl
from jax.experimental.pallas import tpu as pltpu
from jax.sharding import PartitionSpec as P

MESH = pl.DeviceIdType.MESH
F32 = jnp.float32
BF16 = jnp.bfloat16
SCALE = -(2.0**-17)
DIST = (1, 7, 2, 6, 3, 5, 4)


def angle_table(length):
    k = np.arange(length)
    phase = np.outer(k, k) % length
    angle = 2.0 * np.pi * phase / length
    return np.cos(angle), np.sin(angle)


def c_table():
    cos, sin = angle_table(32)
    cos, sin = cos.reshape(32, 8, 1, 4), -sin.reshape(32, 8, 1, 4)
    both = np.stack([cos, sin], axis=2)
    return np.broadcast_to(both, (32, 8, 2, 16, 4)).reshape(32, 1024).astype(np.float32)


def b_table():
    cos, sin = angle_table(32)
    table = np.zeros((2, 2, 16, 4, 2, 4, 32), np.float32)
    for kc in range(4):
        c = cos.reshape(2, 16, 32)
        s = sin.reshape(2, 16, 32)
        table[:, 0, :, kc, 0, kc, :] = c
        table[:, 0, :, kc, 1, kc, :] = -s
        table[:, 1, :, kc, 0, kc, :] = s
        table[:, 1, :, kc, 1, kc, :] = c
    return table.reshape(256, 256)


def fft(parts):
    n = len(parts)
    if n == 1:
        return parts
    half = n // 2
    even, odd = fft(parts[0::2]), fft(parts[1::2])
    low, high = [], []
    for k in range(half):
        (ar, ai), (br, bi) = even[k], odd[k]
        if k == 0:
            tr, ti = br, bi
        elif 4 * k == n:
            tr, ti = bi, -br
        else:
            c, s = math.cos(2 * math.pi * k / n), math.sin(2 * math.pi * k / n)
            tr, ti = c * br + s * bi, c * bi - s * br
        low.append((ar + tr, ai + ti))
        high.append((ar - tr, ai - ti))
    return low + high


def swap_groups(v, lane):
    v = list(v)
    for shift, pairs in ((64, ((0, 2), (1, 3))), (32, ((0, 1), (2, 3)))):
        low = lax.rem(lane, 2 * shift) < shift
        for i, j in pairs:
            a, b = v[i], v[j]
            v[i] = jnp.where(low, a, pltpu.roll(b, shift, 1))
            v[j] = jnp.where(low, pltpu.roll(a, 128 - shift, 1), b)
    return v


def tdot(a, b):
    return lax.dot_general(a, b, (((0,), (0,)), ((), ())), preferred_element_type=F32)


def mdot(a, b):
    return jnp.dot(a, b, preferred_element_type=F32)


def kernel(
    occ, vir, docc, dvir, ctab, btab, out_re, out_im,
    inb, dov, dvv, ctv, btv, mhi, mlo, nhi, nlo,
    pz, pb, rs, ra, rb, rc, yb, xr, zb,
    in_sem, p1s, p1r, p2s, p2r, p3s, p3r, ras, rar, rbs, rbr, rcs, rcr, ys, yr,
):
    row, col = lax.axis_index("row"), lax.axis_index("col")
    core = lax.rem(row, 2)
    z = lax.rem(lax.div(row, 2), 8)
    xh = lax.div(row, 16)
    y, xl = lax.rem(col, 4), lax.div(col, 4)
    x = 2 * xh + xl

    def row_of(xh_, z_, k_):
        return (xh_ * 8 + z_) * 2 + k_

    loads = [
        pltpu.make_async_copy(occ, inb.at[pl.ds(0, 32)], in_sem.at[0]),
        pltpu.make_async_copy(vir, inb.at[pl.ds(32, 16)], in_sem.at[1]),
        pltpu.make_async_copy(docc, dov, in_sem.at[2]),
        pltpu.make_async_copy(dvir, dvv, in_sem.at[3]),
        pltpu.make_async_copy(ctab, ctv, in_sem.at[4]),
        pltpu.make_async_copy(btab, btv, in_sem.at[5]),
    ]
    for load in loads:
        load.start()

    barrier = pltpu.get_barrier_semaphore()

    def greet(i, c):
        pl.semaphore_signal(
            barrier, inc=1, device_id=(xh * 16 + lax.div(i, 8), lax.rem(i, 8)), device_id_type=MESH
        )
        return c

    lax.fori_loop(0, 128, greet, 0)

    def greet_other(i, c):
        pl.semaphore_signal(
            barrier, inc=1, device_id=(row_of(1 - xh, z, core), i), device_id_type=MESH
        )
        return c

    lax.fori_loop(0, 8, greet_other, 0)

    for load in loads:
        load.wait()

    @pl.when(col == 0)
    def _():
        lane = lax.broadcasted_iota(jnp.int32, (32, 1024), 1)
        band = lax.broadcasted_iota(jnp.int32, (32, 1024), 0)
        dec = jnp.sum(jnp.where(lane == band + 32 * row, dov[...], 0.0), axis=1, keepdims=True)
        rs[0:32, :] = (inb[0:32, 0:1024].astype(F32) * dec).astype(BF16)
        lane = lax.broadcasted_iota(jnp.int32, (16, 512), 1)
        band = lax.broadcasted_iota(jnp.int32, (16, 512), 0)
        dec = jnp.sum(jnp.where(lane == band + 16 * row, dvv[...], 0.0), axis=1, keepdims=True)
        rs[32:48, :] = (inb[32:48, 0:1024].astype(F32) * dec).astype(BF16)

    pl.semaphore_wait(barrier, 136)

    def a_copy(s, c):
        lanes = pl.ds(pl.multiple_of(512 * s + 128 * lax.rem(c, 4), 128), 128)
        return pltpu.make_async_remote_copy(
            src_ref=rs.at[:, lanes], dst_ref=ra.at[xh], send_sem=ras.at[s, c], recv_sem=rar.at[xh],
            device_id=(row_of(s, z, core), c), device_id_type=MESH,
        )

    def a_wait(xs):
        pltpu.make_async_copy(ra.at[xs], ra.at[xs], rar.at[xs]).wait()

    def p1_copy(dz):
        zt = lax.rem(z + dz, 8)
        lanes = pl.ds(pl.multiple_of(zt * 512, 512), 512)
        return pltpu.make_async_remote_copy(
            src_ref=inb.at[:, lanes], dst_ref=pz.at[z], send_sem=p1s.at[dz], recv_sem=p1r.at[z],
            device_id=(row_of(xh, zt, core), col), device_id_type=MESH,
        )

    def p1_wait(zs):
        pltpu.make_async_copy(pz.at[zs], pz.at[zs], p1r.at[zs]).wait()

    def b_copy(dz):
        zt = lax.rem(z + dz, 8)
        return pltpu.make_async_remote_copy(
            src_ref=ra, dst_ref=rb.at[z], send_sem=rbs.at[dz], recv_sem=rbr.at[z],
            device_id=(row_of(xh, zt, core), col), device_id_type=MESH,
        )

    def b_wait(zs):
        pltpu.make_async_copy(rb.at[zs], rb.at[zs], rbr.at[zs]).wait()

    def p2_copy(src, zs, side):
        xt = lax.rem(x + 1 + 2 * side, 4)
        return pltpu.make_async_remote_copy(
            src_ref=src, dst_ref=pb.at[xh, core, zs], send_sem=p2s.at[side, zs], recv_sem=p2r.at[xh, zs],
            device_id=(row_of(lax.div(xt, 2), z, core), lax.rem(xt, 2) * 4 + y), device_id_type=MESH,
        )

    def p2_wait(xs, zs):
        pltpu.make_async_copy(pb.at[xs, core, zs], pb.at[xs, core, zs], p2r.at[xs, zs]).wait()

    def p3_copy(xs, zs):
        return pltpu.make_async_remote_copy(
            src_ref=pb.at[xs, core, zs], dst_ref=pb.at[xs, core, zs], send_sem=p3s.at[xs, zs],
            recv_sem=p3r.at[xs, zs], device_id=(row + 1 - 2 * core, col), device_id_type=MESH,
        )

    def p3_wait(xs, zs):
        other = 1 - core
        pltpu.make_async_copy(pb.at[xs, other, zs], pb.at[xs, other, zs], p3r.at[xs, zs]).wait()

    def c_copy(zs, yt):
        return pltpu.make_async_remote_copy(
            src_ref=rb.at[zs], dst_ref=rc.at[lax.rem(y, 2), core, zs], send_sem=rcs.at[yt, zs],
            recv_sem=rcr.at[lax.rem(y, 2), core, zs],
            device_id=(row_of(xh, z, lax.div(y, 2)), xl * 4 + yt), device_id_type=MESH,
        )

    def c_wait(yp, ks, zs):
        pltpu.make_async_copy(rc.at[yp, ks, zs], rc.at[yp, ks, zs], rcr.at[yp, ks, zs]).wait()

    own_half = core == lax.div(y, 2)

    @pl.when(col == 0)
    def _():
        def send(i, carry):
            s, c = lax.div(i, 8), lax.rem(i, 8)

            @pl.when(jnp.logical_or(s != xh, c != 0))
            def _():
                a_copy(s, c).start()

            return carry

        lax.fori_loop(0, 16, send, 0)
        ra[xh] = rs[:, pl.ds(pl.multiple_of(512 * xh, 512), 128)]

    for dz in DIST[:2]:
        p1_copy(dz).start()

    mine = pl.ds(pl.multiple_of(z * 512, 512), 512)
    for side in range(2):
        p2_copy(inb.at[:, mine], z, side).start()

    for xs in range(2):
        @pl.when(jnp.logical_or(col != 0, xh != xs))
        def _():
            a_wait(xs)

    for dz in DIST:
        b_copy(dz).start()
    for dz in DIST[2:]:
        p1_copy(dz).start()

    blane = lax.rem(lax.div(lax.broadcasted_iota(jnp.int32, (32, 1024), 1), 4), 16)
    ct = ctv[...]
    ct_hi = ct.astype(BF16).astype(F32)
    ct_lo = ct - ct_hi

    def table(b, c):
        rows = pl.ds(pl.multiple_of(b * 32, 32), 32)
        mhi[rows, :] = jnp.where(blane == b, ct_hi, 0.0).astype(BF16)
        mlo[rows, :] = jnp.where(blane == b, ct_lo, 0.0).astype(BF16)
        return c

    lax.fori_loop(0, 16, table, 0)
    bt = btv[...]
    bt_hi = bt.astype(BF16)
    nhi[...] = bt_hi
    nlo[...] = (bt - bt_hi.astype(F32)).astype(BF16)

    rb[z] = ra[...]

    def c_sends(zs):
        def one(yt, carry):
            @pl.when(jnp.logical_or(yt != y, jnp.logical_not(own_half)))
            def _():
                c_copy(zs, yt).start()

            return carry

        lax.fori_loop(0, 4, one, 0)

        @pl.when(own_half)
        def _():
            rc[lax.rem(y, 2), core, zs] = rb[zs]

    c_sends(z)

    def step(i, carry):
        dz = lax.rem(i, 2) * lax.div(i + 1, 2) + (1 - lax.rem(i, 2)) * (8 - lax.div(i, 2))
        zs = lax.rem(z + 8 - dz, 8)
        p1_wait(zs)
        p2_copy(pz.at[zs], zs, 0).start()
        p2_copy(pz.at[zs], zs, 1).start()
        b_wait(zs)
        c_sends(zs)
        return carry

    lax.fori_loop(1, 8, step, 0)

    def forward(i, carry):
        dz = lax.rem(i, 2) * lax.div(i + 1, 2) + (1 - lax.rem(i, 2)) * lax.rem(8 - lax.div(i, 2), 8)
        zs = lax.rem(z + 8 - dz, 8)
        for xs in range(2):
            p2_wait(xs, zs)
            p3_copy(xs, zs).start()
        return carry

    lax.fori_loop(0, 8, forward, 0)

    def arrive(zs, carry):
        for xs in range(2):
            p3_wait(xs, zs)
        for yp in range(2):
            for ks in range(2):
                @pl.when(jnp.logical_or(y != 2 * core + yp, ks != core))
                def _():
                    c_wait(yp, ks, zs)
        return carry

    lax.fori_loop(0, 8, arrive, 0)

    for yp in range(2):
        acc_o = jnp.zeros((128, 512), F32)
        acc_v = jnp.zeros((128, 512), F32)
        for xs in range(2):
            for ks in range(2):
                acc_o += tdot(
                    rc[yp, ks, :, xs, 0:32, :].reshape(256, 128), pb[xs, ks, :, 0:32, :].reshape(256, 512)
                )
                acc_v += tdot(
                    rc[yp, ks, :, xs, 32:48, :].reshape(128, 128), pb[xs, ks, :, 32:48, :].reshape(128, 512)
                )
        polar = acc_o * acc_v * SCALE
        hi = polar.astype(BF16)
        lo = (polar - hi.astype(F32)).astype(BF16)
        yb[128 * yp : 128 * yp + 128, :] = (mdot(hi, mhi[...]) + mdot(hi, mlo[...]) + mdot(lo, mhi[...])).astype(BF16)

    slot = ((1 - xl) * 4 + y) * 8 + z
    has_self = lax.div(z, 4) == core

    def y_copy(m, c):
        rows = pl.ds(pl.multiple_of(m * 32, 32), 32)
        lanes = pl.ds(pl.multiple_of(c * 128, 128), 128)
        return pltpu.make_async_remote_copy(
            src_ref=yb.at[rows, lanes], dst_ref=xr.at[slot], send_sem=ys, recv_sem=yr,
            device_id=(16 * xh + 8 * core + m, c), device_id_type=MESH,
        )

    def y_send(i, carry):
        m = lax.rem(lax.div(i, 8) + 2 * z, 8)
        c = lax.rem(lax.rem(i, 8) + col, 8)

        @pl.when(jnp.logical_or(16 * xh + 8 * core + m != row, c != col))
        def _():
            y_copy(m, c).start()

        return carry

    lax.fori_loop(0, 64, y_send, 0)

    @pl.when(has_self)
    def _():
        m = row - 16 * xh - 8 * core
        xr[slot] = yb[pl.ds(pl.multiple_of(m * 32, 32), 32), pl.ds(pl.multiple_of(col * 128, 128), 128)]
        pltpu.make_async_copy(xr.at[pl.ds(0, 63)], xr.at[pl.ds(0, 63)], yr).wait()

    @pl.when(jnp.logical_not(has_self))
    def _():
        pltpu.make_async_copy(xr, xr, yr).wait()

    def b_step(i, carry):
        part = xr[pl.ds(pl.multiple_of(8 * i, 8), 8)].reshape(4, 2, 32, 128)
        both = jnp.concatenate([part[:, 0].reshape(128, 128), part[:, 1].reshape(128, 128)], axis=1)
        res = mdot(both, nhi[...]) + mdot(both, nlo[...])
        zb[pl.ds(4 * i, 4)] = res.reshape(4, 32, 256)
        return carry

    lax.fori_loop(0, 8, b_step, 0)

    lane = lax.broadcasted_iota(jnp.int32, (8, 128), 1)

    def a_step(i, carry):
        rows = pl.ds(pl.multiple_of(8 * i, 8), 8)
        res = fft([(zb[a, rows, 0:128], zb[a, rows, 128:256]) for a in range(32)])
        for j in range(8):
            for part, out in ((0, out_re), (1, out_im)):
                moved = swap_groups([res[4 * j + t][part] for t in range(4)], lane)
                for kc in range(4):
                    out[pl.ds(i * 256 + j * 4 + kc, 8, stride=32), :] = moved[kc]
        return carry

    lax.fori_loop(0, 4, a_step, 0)

    @pl.when(col == 0)
    def _():
        def sent(i, carry):
            s, c = lax.div(i, 8), lax.rem(i, 8)

            @pl.when(jnp.logical_or(s != xh, c != 0))
            def _():
                a_copy(s, c).wait_send()

            return carry

        lax.fori_loop(0, 16, sent, 0)

    def sent_z(dz, carry):
        p1_copy(dz).wait_send()
        b_copy(dz).wait_send()
        return carry

    lax.fori_loop(1, 8, sent_z, 0)

    def sent_zs(zs, carry):
        for side in range(2):
            p2_copy(pz.at[zs], zs, side).wait_send()
            p3_copy(side, zs).wait_send()

        def one(yt, c):
            @pl.when(jnp.logical_or(yt != y, jnp.logical_not(own_half)))
            def _():
                c_copy(zs, yt).wait_send()

            return c

        return lax.fori_loop(0, 4, one, carry)

    lax.fori_loop(0, 8, sent_zs, 0)

    @pl.when(has_self)
    def _():
        pltpu.make_async_copy(xr.at[pl.ds(0, 63)], xr.at[pl.ds(0, 63)], ys).wait()

    @pl.when(jnp.logical_not(has_self))
    def _():
        pltpu.make_async_copy(xr, xr, ys).wait()


def on_device(occ, vir, docc, dvir):
    anyspace = pl.BlockSpec(memory_space=pl.ANY)
    vmem = pl.BlockSpec(memory_space=pltpu.VMEM)
    dma = pltpu.SemaphoreType.DMA
    out = jax.ShapeDtypeStruct((1024, 128), F32)
    res = pl.pallas_call(
        kernel,
        out_shape=(out, out),
        in_specs=[anyspace] * 6,
        out_specs=(vmem, vmem),
        scratch_shapes=[
            pltpu.VMEM((48, 4096), BF16),
            pltpu.VMEM((1, 1024), F32),
            pltpu.VMEM((1, 512), F32),
            pltpu.VMEM((32, 1024), F32),
            pltpu.VMEM((256, 256), F32),
            pltpu.VMEM((512, 1024), BF16),
            pltpu.VMEM((512, 1024), BF16),
            pltpu.VMEM((256, 256), BF16),
            pltpu.VMEM((256, 256), BF16),
            pltpu.VMEM((8, 48, 512), BF16),
            pltpu.VMEM((2, 2, 8, 48, 512), BF16),
            pltpu.VMEM((48, 1024), BF16),
            pltpu.VMEM((2, 48, 128), BF16),
            pltpu.VMEM((8, 2, 48, 128), BF16),
            pltpu.VMEM((2, 2, 8, 2, 48, 128), BF16),
            pltpu.VMEM((256, 1024), BF16),
            pltpu.VMEM((64, 32, 128), BF16),
            pltpu.VMEM((32, 32, 256), F32),
            dma((6,)),
            dma((8,)), dma((8,)),
            dma((2, 8)), dma((2, 8)),
            dma((2, 8)), dma((2, 8)),
            dma((2, 8)), dma((2,)),
            dma((8,)), dma((8,)),
            dma((4, 8)), dma((2, 2, 8)),
            dma, dma,
        ],
        compiler_params=pltpu.CompilerParams(collective_id=0, has_side_effects=True),
    )(
        occ, vir, docc.reshape(1, 1024), dvir.reshape(1, 512),
        jnp.asarray(c_table()), jnp.asarray(b_table()),
    )

    def placed(part):
        return jnp.transpose(part.reshape(32, 8, 4, 128), (0, 2, 1, 3)).reshape(32, 4, 1024)

    return placed(res[0]), placed(res[1])


def solution(mesh):
    in_specs = (P("row", "col"), P("row", "col"), P(), P())
    out_specs = (P("row", "col", None), P("row", "col", None))
    return jax.shard_map(
        on_device, mesh=mesh, in_specs=in_specs, out_specs=out_specs, check_vma=False
    )
```

```python
import functools
import math

import jax
import jax.numpy as jnp
import numpy as np
from jax import lax
from jax.experimental import pallas as pl
from jax.experimental.pallas import tpu as pltpu
from jax.sharding import PartitionSpec as P

MESH = pl.DeviceIdType.MESH
F32 = jnp.float32
BF16 = jnp.bfloat16
SCALE = -(2.0**-17)
DIST = (1, 7, 2, 6, 3, 5, 4)


def angle_table(length):
    k = np.arange(length)
    phase = np.outer(k, k) % length
    angle = 2.0 * np.pi * phase / length
    return np.cos(angle), np.sin(angle)


def c_table():
    cos, sin = angle_table(32)
    cos, sin = cos.reshape(32, 8, 1, 4), -sin.reshape(32, 8, 1, 4)
    both = np.stack([cos, sin], axis=2)
    return np.broadcast_to(both, (32, 8, 2, 16, 4)).reshape(32, 1024).astype(np.float32)


def b_table():
    cos, sin = angle_table(32)
    table = np.zeros((2, 2, 16, 4, 2, 4, 32), np.float32)
    for kc in range(4):
        c = cos.reshape(2, 16, 32)
        s = sin.reshape(2, 16, 32)
        table[:, 0, :, kc, 0, kc, :] = c
        table[:, 0, :, kc, 1, kc, :] = -s
        table[:, 1, :, kc, 0, kc, :] = s
        table[:, 1, :, kc, 1, kc, :] = c
    return table.reshape(256, 256)


def fft(parts):
    n = len(parts)
    if n == 1:
        return parts
    half = n // 2
    even, odd = fft(parts[0::2]), fft(parts[1::2])
    low, high = [], []
    for k in range(half):
        (ar, ai), (br, bi) = even[k], odd[k]
        if k == 0:
            tr, ti = br, bi
        elif 4 * k == n:
            tr, ti = bi, -br
        else:
            c, s = math.cos(2 * math.pi * k / n), math.sin(2 * math.pi * k / n)
            tr, ti = c * br + s * bi, c * bi - s * br
        low.append((ar + tr, ai + ti))
        high.append((ar - tr, ai - ti))
    return low + high


def swap_groups(v, lane):
    v = list(v)
    for shift, pairs in ((64, ((0, 2), (1, 3))), (32, ((0, 1), (2, 3)))):
        low = lax.rem(lane, 2 * shift) < shift
        for i, j in pairs:
            a, b = v[i], v[j]
            v[i] = jnp.where(low, a, pltpu.roll(b, shift, 1))
            v[j] = jnp.where(low, pltpu.roll(a, 128 - shift, 1), b)
    return v


def tdot(a, b):
    return lax.dot_general(a, b, (((0,), (0,)), ((), ())), preferred_element_type=F32)


def mdot(a, b):
    return jnp.dot(a, b, preferred_element_type=F32)


def kernel(
    occ, vir, docc, dvir, ctab, btab, out_re, out_im,
    inb, dov, dvv, ctv, btv, mhi, mlo, nhi, nlo,
    pz, pb, rs, ra, rb, rc, yb, xr, zb,
    in_sem, p1s, p1r, p2s, p2r, p3s, p3r, ras, rar, rbs, rbr, rcs, rcr, ys, yr, ready,
):
    row, col = lax.axis_index("row"), lax.axis_index("col")
    core = lax.rem(row, 2)
    z = lax.rem(lax.div(row, 2), 8)
    xh = lax.div(row, 16)
    y, xl = lax.rem(col, 4), lax.div(col, 4)
    x = 2 * xh + xl

    def row_of(xh_, z_, k_):
        return (xh_ * 8 + z_) * 2 + k_

    loads = [
        pltpu.make_async_copy(occ, inb.at[pl.ds(0, 32)], in_sem.at[0]),
        pltpu.make_async_copy(vir, inb.at[pl.ds(32, 16)], in_sem.at[1]),
        pltpu.make_async_copy(docc, dov, in_sem.at[2]),
        pltpu.make_async_copy(dvir, dvv, in_sem.at[3]),
        pltpu.make_async_copy(ctab, ctv, in_sem.at[4]),
        pltpu.make_async_copy(btab, btv, in_sem.at[5]),
    ]
    for load in loads:
        load.start()

    barrier = pltpu.get_barrier_semaphore()

    def greet_z(i, c):
        pl.semaphore_signal(barrier, inc=1, device_id=(row_of(xh, i, core), col), device_id_type=MESH)
        return c

    def greet_slab(i, c):
        pl.semaphore_signal(
            barrier, inc=1, device_id=(row_of(xh, z, lax.rem(i, 2)), lax.div(i, 2)), device_id_type=MESH
        )
        return c

    def greet_other(i, c):
        pl.semaphore_signal(barrier, inc=1, device_id=(row_of(1 - xh, z, core), i), device_id_type=MESH)
        return c

    lax.fori_loop(0, 8, greet_z, 0)
    lax.fori_loop(0, 16, greet_slab, 0)
    lax.fori_loop(0, 8, greet_other, 0)

    for load in loads:
        load.wait()

    @pl.when(col == 0)
    def _():
        lane = lax.broadcasted_iota(jnp.int32, (32, 1024), 1)
        band = lax.broadcasted_iota(jnp.int32, (32, 1024), 0)
        dec = jnp.sum(jnp.where(lane == band + 32 * row, dov[...], 0.0), axis=1, keepdims=True)
        rs[0:32, :] = (inb[0:32, 0:1024].astype(F32) * dec).astype(BF16)
        lane = lax.broadcasted_iota(jnp.int32, (16, 512), 1)
        band = lax.broadcasted_iota(jnp.int32, (16, 512), 0)
        dec = jnp.sum(jnp.where(lane == band + 16 * row, dvv[...], 0.0), axis=1, keepdims=True)
        rs[32:48, :] = (inb[32:48, 0:1024].astype(F32) * dec).astype(BF16)

    pl.semaphore_wait(barrier, 32)

    def greet_ready(i, c):
        pl.semaphore_signal(
            ready, inc=1, device_id=(row_of(xh, z, lax.rem(i, 2)), lax.div(i, 2)), device_id_type=MESH
        )
        return c

    lax.fori_loop(0, 16, greet_ready, 0)

    def a_copy(s, c):
        lanes = pl.ds(pl.multiple_of(512 * s + 128 * lax.rem(c, 4), 128), 128)
        return pltpu.make_async_remote_copy(
            src_ref=rs.at[:, lanes], dst_ref=ra.at[xh], send_sem=ras.at[s, c], recv_sem=rar.at[xh],
            device_id=(row_of(s, z, core), c), device_id_type=MESH,
        )

    def a_wait(xs):
        pltpu.make_async_copy(ra.at[xs], ra.at[xs], rar.at[xs]).wait()

    def p1_copy(dz):
        zt = lax.rem(z + dz, 8)
        lanes = pl.ds(pl.multiple_of(zt * 512, 512), 512)
        return pltpu.make_async_remote_copy(
            src_ref=inb.at[:, lanes], dst_ref=pz.at[z], send_sem=p1s.at[dz], recv_sem=p1r.at[z],
            device_id=(row_of(xh, zt, core), col), device_id_type=MESH,
        )

    def p1_wait(zs):
        pltpu.make_async_copy(pz.at[zs], pz.at[zs], p1r.at[zs]).wait()

    def b_copy(dz):
        zt = lax.rem(z + dz, 8)
        return pltpu.make_async_remote_copy(
            src_ref=ra, dst_ref=rb.at[z], send_sem=rbs.at[dz], recv_sem=rbr.at[z],
            device_id=(row_of(xh, zt, core), col), device_id_type=MESH,
        )

    def b_wait(zs):
        pltpu.make_async_copy(rb.at[zs], rb.at[zs], rbr.at[zs]).wait()

    def p2_copy(src, zs, side):
        xt = lax.rem(x + 1 + 2 * side, 4)
        return pltpu.make_async_remote_copy(
            src_ref=src, dst_ref=pb.at[xh, core, zs], send_sem=p2s.at[side, zs], recv_sem=p2r.at[xh, zs],
            device_id=(row_of(lax.div(xt, 2), z, core), lax.rem(xt, 2) * 4 + y), device_id_type=MESH,
        )

    def p2_wait(xs, zs):
        pltpu.make_async_copy(pb.at[xs, core, zs], pb.at[xs, core, zs], p2r.at[xs, zs]).wait()

    def p3_copy(xs, zs):
        return pltpu.make_async_remote_copy(
            src_ref=pb.at[xs, core, zs], dst_ref=pb.at[xs, core, zs], send_sem=p3s.at[xs, zs],
            recv_sem=p3r.at[xs, zs], device_id=(row + 1 - 2 * core, col), device_id_type=MESH,
        )

    def p3_wait(xs, zs):
        other = 1 - core
        pltpu.make_async_copy(pb.at[xs, other, zs], pb.at[xs, other, zs], p3r.at[xs, zs]).wait()

    def c_copy(zs, yt):
        return pltpu.make_async_remote_copy(
            src_ref=rb.at[zs], dst_ref=rc.at[lax.rem(y, 2), core, zs], send_sem=rcs.at[yt, zs],
            recv_sem=rcr.at[lax.rem(y, 2), core, zs],
            device_id=(row_of(xh, z, lax.div(y, 2)), xl * 4 + yt), device_id_type=MESH,
        )

    def c_wait(yp, ks, zs):
        pltpu.make_async_copy(rc.at[yp, ks, zs], rc.at[yp, ks, zs], rcr.at[yp, ks, zs]).wait()

    own_half = core == lax.div(y, 2)

    @pl.when(col == 0)
    def _():
        def send(i, carry):
            s, c = lax.div(i, 8), lax.rem(i, 8)

            @pl.when(jnp.logical_or(s != xh, c != 0))
            def _():
                a_copy(s, c).start()

            return carry

        lax.fori_loop(0, 16, send, 0)
        ra[xh] = rs[:, pl.ds(pl.multiple_of(512 * xh, 512), 128)]

    for dz in DIST[:2]:
        p1_copy(dz).start()

    mine = pl.ds(pl.multiple_of(z * 512, 512), 512)
    for side in range(2):
        p2_copy(inb.at[:, mine], z, side).start()

    for xs in range(2):
        @pl.when(jnp.logical_or(col != 0, xh != xs))
        def _():
            a_wait(xs)

    for dz in DIST:
        b_copy(dz).start()
    for dz in DIST[2:]:
        p1_copy(dz).start()

    blane = lax.rem(lax.div(lax.broadcasted_iota(jnp.int32, (32, 1024), 1), 4), 16)
    ct = ctv[...]
    ct_hi = ct.astype(BF16).astype(F32)
    ct_lo = ct - ct_hi

    def table(b, c):
        rows = pl.ds(pl.multiple_of(b * 32, 32), 32)
        mhi[rows, :] = jnp.where(blane == b, ct_hi, 0.0).astype(BF16)
        mlo[rows, :] = jnp.where(blane == b, ct_lo, 0.0).astype(BF16)
        return c

    lax.fori_loop(0, 16, table, 0)
    bt = btv[...]
    bt_hi = bt.astype(BF16)
    nhi[...] = bt_hi
    nlo[...] = (bt - bt_hi.astype(F32)).astype(BF16)

    rb[z] = ra[...]

    def c_sends(zs):
        def one(yt, carry):
            @pl.when(jnp.logical_or(yt != y, jnp.logical_not(own_half)))
            def _():
                c_copy(zs, yt).start()

            return carry

        lax.fori_loop(0, 4, one, 0)

        @pl.when(own_half)
        def _():
            rc[lax.rem(y, 2), core, zs] = rb[zs]

    c_sends(z)

    def step(i, carry):
        dz = lax.rem(i, 2) * lax.div(i + 1, 2) + (1 - lax.rem(i, 2)) * (8 - lax.div(i, 2))
        zs = lax.rem(z + 8 - dz, 8)
        p1_wait(zs)
        p2_copy(pz.at[zs], zs, 0).start()
        p2_copy(pz.at[zs], zs, 1).start()
        b_wait(zs)
        c_sends(zs)
        return carry

    lax.fori_loop(1, 8, step, 0)

    def forward(i, carry):
        dz = lax.rem(i, 2) * lax.div(i + 1, 2) + (1 - lax.rem(i, 2)) * lax.rem(8 - lax.div(i, 2), 8)
        zs = lax.rem(z + 8 - dz, 8)
        for xs in range(2):
            p2_wait(xs, zs)
            p3_copy(xs, zs).start()
        return carry

    lax.fori_loop(0, 8, forward, 0)

    def arrive(zs, carry):
        for xs in range(2):
            p3_wait(xs, zs)
        for yp in range(2):
            for ks in range(2):
                @pl.when(jnp.logical_or(y != 2 * core + yp, ks != core))
                def _():
                    c_wait(yp, ks, zs)
        return carry

    lax.fori_loop(0, 8, arrive, 0)

    for yp in range(2):
        acc_o = jnp.zeros((128, 512), F32)
        acc_v = jnp.zeros((128, 512), F32)
        for xs in range(2):
            for ks in range(2):
                acc_o += tdot(
                    rc[yp, ks, :, xs, 0:32, :].reshape(256, 128), pb[xs, ks, :, 0:32, :].reshape(256, 512)
                )
                acc_v += tdot(
                    rc[yp, ks, :, xs, 32:48, :].reshape(128, 128), pb[xs, ks, :, 32:48, :].reshape(128, 512)
                )
        polar = acc_o * acc_v * SCALE
        hi = polar.astype(BF16)
        lo = (polar - hi.astype(F32)).astype(BF16)
        yb[128 * yp : 128 * yp + 128, :] = (mdot(hi, mhi[...]) + mdot(hi, mlo[...]) + mdot(lo, mhi[...])).astype(BF16)

    slot = ((1 - xl) * 4 + y) * 8 + z
    has_self = lax.div(z, 4) == core

    def y_copy(m, c):
        rows = pl.ds(pl.multiple_of(m * 32, 32), 32)
        lanes = pl.ds(pl.multiple_of(c * 128, 128), 128)
        return pltpu.make_async_remote_copy(
            src_ref=yb.at[rows, lanes], dst_ref=xr.at[slot], send_sem=ys, recv_sem=yr,
            device_id=(16 * xh + 8 * core + m, c), device_id_type=MESH,
        )

    def y_send(i, carry):
        m = lax.rem(lax.div(i, 8) + 2 * z, 8)
        c = lax.rem(lax.rem(i, 8) + col, 8)

        @pl.when(jnp.logical_or(16 * xh + 8 * core + m != row, c != col))
        def _():
            y_copy(m, c).start()

        return carry

    pl.semaphore_wait(ready, 16)
    lax.fori_loop(0, 64, y_send, 0)

    @pl.when(has_self)
    def _():
        m = row - 16 * xh - 8 * core
        xr[slot] = yb[pl.ds(pl.multiple_of(m * 32, 32), 32), pl.ds(pl.multiple_of(col * 128, 128), 128)]
        pltpu.make_async_copy(xr.at[pl.ds(0, 63)], xr.at[pl.ds(0, 63)], yr).wait()

    @pl.when(jnp.logical_not(has_self))
    def _():
        pltpu.make_async_copy(xr, xr, yr).wait()

    def b_step(i, carry):
        part = xr[pl.ds(pl.multiple_of(8 * i, 8), 8)].reshape(4, 2, 32, 128)
        both = jnp.concatenate([part[:, 0].reshape(128, 128), part[:, 1].reshape(128, 128)], axis=1)
        res = mdot(both, nhi[...]) + mdot(both, nlo[...])
        zb[pl.ds(4 * i, 4)] = res.reshape(4, 32, 256)
        return carry

    lax.fori_loop(0, 8, b_step, 0)

    lane = lax.broadcasted_iota(jnp.int32, (8, 128), 1)

    def a_step(i, carry):
        rows = pl.ds(pl.multiple_of(8 * i, 8), 8)
        res = fft([(zb[a, rows, 0:128], zb[a, rows, 128:256]) for a in range(32)])
        for j in range(8):
            for part, out in ((0, out_re), (1, out_im)):
                moved = swap_groups([res[4 * j + t][part] for t in range(4)], lane)
                for kc in range(4):
                    out[pl.ds(i * 256 + j * 4 + kc, 8, stride=32), :] = moved[kc]
        return carry

    lax.fori_loop(0, 4, a_step, 0)

    @pl.when(col == 0)
    def _():
        def sent(i, carry):
            s, c = lax.div(i, 8), lax.rem(i, 8)

            @pl.when(jnp.logical_or(s != xh, c != 0))
            def _():
                a_copy(s, c).wait_send()

            return carry

        lax.fori_loop(0, 16, sent, 0)

    def sent_z(dz, carry):
        p1_copy(dz).wait_send()
        b_copy(dz).wait_send()
        return carry

    lax.fori_loop(1, 8, sent_z, 0)

    def sent_zs(zs, carry):
        for side in range(2):
            p2_copy(pz.at[zs], zs, side).wait_send()
            p3_copy(side, zs).wait_send()

        def one(yt, c):
            @pl.when(jnp.logical_or(yt != y, jnp.logical_not(own_half)))
            def _():
                c_copy(zs, yt).wait_send()

            return c

        return lax.fori_loop(0, 4, one, carry)

    lax.fori_loop(0, 8, sent_zs, 0)

    @pl.when(has_self)
    def _():
        pltpu.make_async_copy(xr.at[pl.ds(0, 63)], xr.at[pl.ds(0, 63)], ys).wait()

    @pl.when(jnp.logical_not(has_self))
    def _():
        pltpu.make_async_copy(xr, xr, ys).wait()


def on_device(occ, vir, docc, dvir):
    anyspace = pl.BlockSpec(memory_space=pl.ANY)
    vmem = pl.BlockSpec(memory_space=pltpu.VMEM)
    dma = pltpu.SemaphoreType.DMA
    out = jax.ShapeDtypeStruct((1024, 128), F32)
    res = pl.pallas_call(
        kernel,
        out_shape=(out, out),
        in_specs=[anyspace] * 6,
        out_specs=(vmem, vmem),
        scratch_shapes=[
            pltpu.VMEM((48, 4096), BF16),
            pltpu.VMEM((1, 1024), F32),
            pltpu.VMEM((1, 512), F32),
            pltpu.VMEM((32, 1024), F32),
            pltpu.VMEM((256, 256), F32),
            pltpu.VMEM((512, 1024), BF16),
            pltpu.VMEM((512, 1024), BF16),
            pltpu.VMEM((256, 256), BF16),
            pltpu.VMEM((256, 256), BF16),
            pltpu.VMEM((8, 48, 512), BF16),
            pltpu.VMEM((2, 2, 8, 48, 512), BF16),
            pltpu.VMEM((48, 1024), BF16),
            pltpu.VMEM((2, 48, 128), BF16),
            pltpu.VMEM((8, 2, 48, 128), BF16),
            pltpu.VMEM((2, 2, 8, 2, 48, 128), BF16),
            pltpu.VMEM((256, 1024), BF16),
            pltpu.VMEM((64, 32, 128), BF16),
            pltpu.VMEM((32, 32, 256), F32),
            dma((6,)),
            dma((8,)), dma((8,)),
            dma((2, 8)), dma((2, 8)),
            dma((2, 8)), dma((2, 8)),
            dma((2, 8)), dma((2,)),
            dma((8,)), dma((8,)),
            dma((4, 8)), dma((2, 2, 8)),
            dma, dma,
            pltpu.SemaphoreType.REGULAR,
        ],
        compiler_params=pltpu.CompilerParams(collective_id=0, has_side_effects=True),
    )(
        occ, vir, docc.reshape(1, 1024), dvir.reshape(1, 512),
        jnp.asarray(c_table()), jnp.asarray(b_table()),
    )

    def placed(part):
        return jnp.transpose(part.reshape(32, 8, 4, 128), (0, 2, 1, 3)).reshape(32, 4, 1024)

    return placed(res[0]), placed(res[1])


def solution(mesh):
    in_specs = (P("row", "col"), P("row", "col"), P(), P())
    out_specs = (P("row", "col", None), P("row", "col", None))
    return jax.shard_map(
        on_device, mesh=mesh, in_specs=in_specs, out_specs=out_specs, check_vma=False
    )
```

```python
import functools
import math

import jax
import jax.numpy as jnp
import numpy as np
from jax import lax
from jax.experimental import pallas as pl
from jax.experimental.pallas import tpu as pltpu
from jax.sharding import PartitionSpec as P

MESH = pl.DeviceIdType.MESH
F32 = jnp.float32
BF16 = jnp.bfloat16
SCALE = -(2.0**-17)
NEAR, FAR = (1, 7, 2, 6), (3, 5, 4)
DIST = NEAR + FAR


def angle_table(length):
    k = np.arange(length)
    phase = np.outer(k, k) % length
    angle = 2.0 * np.pi * phase / length
    return np.cos(angle), np.sin(angle)


def c_table():
    cos, sin = angle_table(32)
    cos, sin = cos.reshape(32, 8, 1, 4), -sin.reshape(32, 8, 1, 4)
    both = np.stack([cos, sin], axis=2)
    return np.broadcast_to(both, (32, 8, 2, 16, 4)).reshape(32, 1024).astype(np.float32)


def b_table():
    cos, sin = angle_table(32)
    table = np.zeros((2, 2, 16, 4, 2, 4, 32), np.float32)
    for kc in range(4):
        c = cos.reshape(2, 16, 32)
        s = sin.reshape(2, 16, 32)
        table[:, 0, :, kc, 0, kc, :] = c
        table[:, 0, :, kc, 1, kc, :] = -s
        table[:, 1, :, kc, 0, kc, :] = s
        table[:, 1, :, kc, 1, kc, :] = c
    return table.reshape(256, 256)


def fft(parts):
    n = len(parts)
    if n == 1:
        return parts
    half = n // 2
    even, odd = fft(parts[0::2]), fft(parts[1::2])
    low, high = [], []
    for k in range(half):
        (ar, ai), (br, bi) = even[k], odd[k]
        if k == 0:
            tr, ti = br, bi
        elif 4 * k == n:
            tr, ti = bi, -br
        else:
            c, s = math.cos(2 * math.pi * k / n), math.sin(2 * math.pi * k / n)
            tr, ti = c * br + s * bi, c * bi - s * br
        low.append((ar + tr, ai + ti))
        high.append((ar - tr, ai - ti))
    return low + high


def swap_groups(v, lane):
    v = list(v)
    for shift, pairs in ((64, ((0, 2), (1, 3))), (32, ((0, 1), (2, 3)))):
        low = lax.rem(lane, 2 * shift) < shift
        for i, j in pairs:
            a, b = v[i], v[j]
            v[i] = jnp.where(low, a, pltpu.roll(b, shift, 1))
            v[j] = jnp.where(low, pltpu.roll(a, 128 - shift, 1), b)
    return v


def tdot(a, b):
    return lax.dot_general(a, b, (((0,), (0,)), ((), ())), preferred_element_type=F32)


def mdot(a, b):
    return jnp.dot(a, b, preferred_element_type=F32)


def kernel(
    occ, vir, docc, dvir, ctab, btab, out_re, out_im,
    inb, dov, dvv, ctv, btv, mhi, mlo, nhi, nlo,
    pz, pb, rs, ra, rb, rc, yb, xr, zb,
    in_sem, p1s, p1r, p2s, p2r, p3s, p3r, ras, rar, rbs, rbr, rcs, rcr, ys, yr, ready,
):
    row, col = lax.axis_index("row"), lax.axis_index("col")
    core = lax.rem(row, 2)
    z = lax.rem(lax.div(row, 2), 8)
    xh = lax.div(row, 16)
    y, xl = lax.rem(col, 4), lax.div(col, 4)
    x = 2 * xh + xl

    def row_of(xh_, z_, k_):
        return (xh_ * 8 + z_) * 2 + k_

    loads = [
        pltpu.make_async_copy(occ, inb.at[pl.ds(0, 32)], in_sem.at[0]),
        pltpu.make_async_copy(vir, inb.at[pl.ds(32, 16)], in_sem.at[1]),
        pltpu.make_async_copy(docc, dov, in_sem.at[2]),
        pltpu.make_async_copy(dvir, dvv, in_sem.at[3]),
        pltpu.make_async_copy(ctab, ctv, in_sem.at[4]),
        pltpu.make_async_copy(btab, btv, in_sem.at[5]),
    ]
    for load in loads:
        load.start()

    barrier = pltpu.get_barrier_semaphore()

    def greet_z(i, c):
        pl.semaphore_signal(barrier, inc=1, device_id=(row_of(xh, i, core), col), device_id_type=MESH)
        return c

    def greet_slab(i, c):
        pl.semaphore_signal(
            barrier, inc=1, device_id=(row_of(xh, z, lax.rem(i, 2)), lax.div(i, 2)), device_id_type=MESH
        )
        return c

    def greet_other(i, c):
        pl.semaphore_signal(barrier, inc=1, device_id=(row_of(1 - xh, z, core), i), device_id_type=MESH)
        return c

    lax.fori_loop(0, 8, greet_z, 0)
    lax.fori_loop(0, 16, greet_slab, 0)
    lax.fori_loop(0, 8, greet_other, 0)

    for load in loads:
        load.wait()

    @pl.when(col == 0)
    def _():
        lane = lax.broadcasted_iota(jnp.int32, (32, 1024), 1)
        band = lax.broadcasted_iota(jnp.int32, (32, 1024), 0)
        dec = jnp.sum(jnp.where(lane == band + 32 * row, dov[...], 0.0), axis=1, keepdims=True)
        rs[0:32, :] = (inb[0:32, 0:1024].astype(F32) * dec).astype(BF16)
        lane = lax.broadcasted_iota(jnp.int32, (16, 512), 1)
        band = lax.broadcasted_iota(jnp.int32, (16, 512), 0)
        dec = jnp.sum(jnp.where(lane == band + 16 * row, dvv[...], 0.0), axis=1, keepdims=True)
        rs[32:48, :] = (inb[32:48, 0:1024].astype(F32) * dec).astype(BF16)

    pl.semaphore_wait(barrier, 32)

    def greet_ready(i, c):
        pl.semaphore_signal(
            ready, inc=1, device_id=(row_of(xh, z, lax.rem(i, 2)), lax.div(i, 2)), device_id_type=MESH
        )
        return c

    lax.fori_loop(0, 16, greet_ready, 0)

    def a_copy(s, c):
        lanes = pl.ds(pl.multiple_of(512 * s + 128 * lax.rem(c, 4), 128), 128)
        return pltpu.make_async_remote_copy(
            src_ref=rs.at[:, lanes], dst_ref=ra.at[xh], send_sem=ras.at[s, c], recv_sem=rar.at[xh],
            device_id=(row_of(s, z, core), c), device_id_type=MESH,
        )

    def a_wait(xs):
        pltpu.make_async_copy(ra.at[xs], ra.at[xs], rar.at[xs]).wait()

    def p1_copy(dz):
        zt = lax.rem(z + dz, 8)
        lanes = pl.ds(pl.multiple_of(zt * 512, 512), 512)
        return pltpu.make_async_remote_copy(
            src_ref=inb.at[:, lanes], dst_ref=pz.at[z], send_sem=p1s.at[dz], recv_sem=p1r.at[z],
            device_id=(row_of(xh, zt, core), col), device_id_type=MESH,
        )

    def p1_wait(zs):
        pltpu.make_async_copy(pz.at[zs], pz.at[zs], p1r.at[zs]).wait()

    def b_copy(dz):
        zt = lax.rem(z + dz, 8)
        return pltpu.make_async_remote_copy(
            src_ref=ra, dst_ref=rb.at[z], send_sem=rbs.at[dz], recv_sem=rbr.at[z],
            device_id=(row_of(xh, zt, core), col), device_id_type=MESH,
        )

    def b_wait(zs):
        pltpu.make_async_copy(rb.at[zs], rb.at[zs], rbr.at[zs]).wait()

    def p2_copy(src, zs, side):
        xt = lax.rem(x + 1 + 2 * side, 4)
        return pltpu.make_async_remote_copy(
            src_ref=src, dst_ref=pb.at[xh, core, zs], send_sem=p2s.at[side, zs], recv_sem=p2r.at[xh, zs],
            device_id=(row_of(lax.div(xt, 2), z, core), lax.rem(xt, 2) * 4 + y), device_id_type=MESH,
        )

    def p2_wait(xs, zs):
        pltpu.make_async_copy(pb.at[xs, core, zs], pb.at[xs, core, zs], p2r.at[xs, zs]).wait()

    def p3_copy(xs, zs):
        return pltpu.make_async_remote_copy(
            src_ref=pb.at[xs, core, zs], dst_ref=pb.at[xs, core, zs], send_sem=p3s.at[xs, zs],
            recv_sem=p3r.at[xs, zs], device_id=(row + 1 - 2 * core, col), device_id_type=MESH,
        )

    def p3_wait(xs, zs):
        other = 1 - core
        pltpu.make_async_copy(pb.at[xs, other, zs], pb.at[xs, other, zs], p3r.at[xs, zs]).wait()

    def c_copy(zs, yt):
        return pltpu.make_async_remote_copy(
            src_ref=rb.at[zs], dst_ref=rc.at[lax.rem(y, 2), core, zs], send_sem=rcs.at[yt, zs],
            recv_sem=rcr.at[lax.rem(y, 2), core, zs],
            device_id=(row_of(xh, z, lax.div(y, 2)), xl * 4 + yt), device_id_type=MESH,
        )

    def c_wait(yp, ks, zs):
        pltpu.make_async_copy(rc.at[yp, ks, zs], rc.at[yp, ks, zs], rcr.at[yp, ks, zs]).wait()

    own_half = core == lax.div(y, 2)

    @pl.when(col == 0)
    def _():
        def send(i, carry):
            s, c = lax.div(i, 8), lax.rem(i, 8)

            @pl.when(jnp.logical_or(s != xh, c != 0))
            def _():
                a_copy(s, c).start()

            return carry

        lax.fori_loop(0, 16, send, 0)
        ra[xh] = rs[:, pl.ds(pl.multiple_of(512 * xh, 512), 128)]

    for dz in NEAR:
        p1_copy(dz).start()

    mine = pl.ds(pl.multiple_of(z * 512, 512), 512)
    for side in range(2):
        p2_copy(inb.at[:, mine], z, side).start()

    for xs in range(2):
        @pl.when(jnp.logical_or(col != 0, xh != xs))
        def _():
            a_wait(xs)

    for dz in DIST:
        b_copy(dz).start()
    for dz in FAR:
        p1_copy(dz).start()

    blane = lax.rem(lax.div(lax.broadcasted_iota(jnp.int32, (32, 1024), 1), 4), 16)
    ct = ctv[...]
    ct_hi = ct.astype(BF16).astype(F32)
    ct_lo = ct - ct_hi

    def table(b, c):
        rows = pl.ds(pl.multiple_of(b * 32, 32), 32)
        mhi[rows, :] = jnp.where(blane == b, ct_hi, 0.0).astype(BF16)
        mlo[rows, :] = jnp.where(blane == b, ct_lo, 0.0).astype(BF16)
        return c

    lax.fori_loop(0, 16, table, 0)
    bt = btv[...]
    bt_hi = bt.astype(BF16)
    nhi[...] = bt_hi
    nlo[...] = (bt - bt_hi.astype(F32)).astype(BF16)

    rb[z] = ra[...]

    def c_sends(zs):
        def one(yt, carry):
            @pl.when(jnp.logical_or(yt != y, jnp.logical_not(own_half)))
            def _():
                c_copy(zs, yt).start()

            return carry

        lax.fori_loop(0, 4, one, 0)

        @pl.when(own_half)
        def _():
            rc[lax.rem(y, 2), core, zs] = rb[zs]

    c_sends(z)

    def source(dz):
        return lax.rem(z + 8 - dz, 8)

    def relay(dz):
        zs = source(dz)
        p1_wait(zs)
        p2_copy(pz.at[zs], zs, 0).start()
        p2_copy(pz.at[zs], zs, 1).start()

    def forward(dz):
        zs = source(dz)
        for xs in range(2):
            p2_wait(xs, zs)
            p3_copy(xs, zs).start()

    for dz in NEAR:
        relay(dz)
    for dz in DIST:
        b_wait(source(dz))
        c_sends(source(dz))
    for dz in (0, *NEAR):
        forward(dz)
    for dz in FAR:
        relay(dz)
    for dz in FAR:
        forward(dz)

    def arrive(zs, carry):
        for xs in range(2):
            p3_wait(xs, zs)
        for yp in range(2):
            for ks in range(2):
                @pl.when(jnp.logical_or(y != 2 * core + yp, ks != core))
                def _():
                    c_wait(yp, ks, zs)
        return carry

    lax.fori_loop(0, 8, arrive, 0)

    slot = ((1 - xl) * 4 + y) * 8 + z
    has_self = lax.div(z, 4) == core

    def y_copy(m, c):
        rows = pl.ds(pl.multiple_of(m * 32, 32), 32)
        lanes = pl.ds(pl.multiple_of(c * 128, 128), 128)
        return pltpu.make_async_remote_copy(
            src_ref=yb.at[rows, lanes], dst_ref=xr.at[slot], send_sem=ys, recv_sem=yr,
            device_id=(16 * xh + 8 * core + m, c), device_id_type=MESH,
        )

    pl.semaphore_wait(ready, 16)
    for yp in range(2):
        acc_o = jnp.zeros((128, 512), F32)
        acc_v = jnp.zeros((128, 512), F32)
        for xs in range(2):
            for ks in range(2):
                acc_o += tdot(
                    rc[yp, ks, :, xs, 0:32, :].reshape(256, 128), pb[xs, ks, :, 0:32, :].reshape(256, 512)
                )
                acc_v += tdot(
                    rc[yp, ks, :, xs, 32:48, :].reshape(128, 128), pb[xs, ks, :, 32:48, :].reshape(128, 512)
                )
        polar = acc_o * acc_v * SCALE
        hi = polar.astype(BF16)
        lo = (polar - hi.astype(F32)).astype(BF16)
        yb[128 * yp : 128 * yp + 128, :] = (mdot(hi, mhi[...]) + mdot(hi, mlo[...]) + mdot(lo, mhi[...])).astype(BF16)

        def y_send(i, carry):
            m = 4 * yp + lax.rem(i, 4)
            c = lax.rem(lax.div(i, 4) + col, 8)

            @pl.when(jnp.logical_or(16 * xh + 8 * core + m != row, c != col))
            def _():
                y_copy(m, c).start()

            return carry

        lax.fori_loop(0, 32, y_send, 0)

    @pl.when(has_self)
    def _():
        m = row - 16 * xh - 8 * core
        xr[slot] = yb[pl.ds(pl.multiple_of(m * 32, 32), 32), pl.ds(pl.multiple_of(col * 128, 128), 128)]
        pltpu.make_async_copy(xr.at[pl.ds(0, 63)], xr.at[pl.ds(0, 63)], yr).wait()

    @pl.when(jnp.logical_not(has_self))
    def _():
        pltpu.make_async_copy(xr, xr, yr).wait()

    def b_step(i, carry):
        part = xr[pl.ds(pl.multiple_of(8 * i, 8), 8)].reshape(4, 2, 32, 128)
        both = jnp.concatenate([part[:, 0].reshape(128, 128), part[:, 1].reshape(128, 128)], axis=1)
        res = mdot(both, nhi[...]) + mdot(both, nlo[...])
        zb[pl.ds(4 * i, 4)] = res.reshape(4, 32, 256)
        return carry

    lax.fori_loop(0, 8, b_step, 0)

    lane = lax.broadcasted_iota(jnp.int32, (8, 128), 1)

    def a_step(i, carry):
        rows = pl.ds(pl.multiple_of(8 * i, 8), 8)
        res = fft([(zb[a, rows, 0:128], zb[a, rows, 128:256]) for a in range(32)])
        for j in range(8):
            for part, out in ((0, out_re), (1, out_im)):
                moved = swap_groups([res[4 * j + t][part] for t in range(4)], lane)
                for kc in range(4):
                    out[pl.ds(i * 256 + j * 4 + kc, 8, stride=32), :] = moved[kc]
        return carry

    lax.fori_loop(0, 4, a_step, 0)

    @pl.when(col == 0)
    def _():
        def sent(i, carry):
            s, c = lax.div(i, 8), lax.rem(i, 8)

            @pl.when(jnp.logical_or(s != xh, c != 0))
            def _():
                a_copy(s, c).wait_send()

            return carry

        lax.fori_loop(0, 16, sent, 0)

    def sent_z(dz, carry):
        p1_copy(dz).wait_send()
        b_copy(dz).wait_send()
        return carry

    lax.fori_loop(1, 8, sent_z, 0)

    def sent_zs(zs, carry):
        for side in range(2):
            p2_copy(pz.at[zs], zs, side).wait_send()
            p3_copy(side, zs).wait_send()

        def one(yt, c):
            @pl.when(jnp.logical_or(yt != y, jnp.logical_not(own_half)))
            def _():
                c_copy(zs, yt).wait_send()

            return c

        return lax.fori_loop(0, 4, one, carry)

    lax.fori_loop(0, 8, sent_zs, 0)

    @pl.when(has_self)
    def _():
        pltpu.make_async_copy(xr.at[pl.ds(0, 63)], xr.at[pl.ds(0, 63)], ys).wait()

    @pl.when(jnp.logical_not(has_self))
    def _():
        pltpu.make_async_copy(xr, xr, ys).wait()


def on_device(occ, vir, docc, dvir):
    anyspace = pl.BlockSpec(memory_space=pl.ANY)
    vmem = pl.BlockSpec(memory_space=pltpu.VMEM)
    dma = pltpu.SemaphoreType.DMA
    out = jax.ShapeDtypeStruct((1024, 128), F32)
    res = pl.pallas_call(
        kernel,
        out_shape=(out, out),
        in_specs=[anyspace] * 6,
        out_specs=(vmem, vmem),
        scratch_shapes=[
            pltpu.VMEM((48, 4096), BF16),
            pltpu.VMEM((1, 1024), F32),
            pltpu.VMEM((1, 512), F32),
            pltpu.VMEM((32, 1024), F32),
            pltpu.VMEM((256, 256), F32),
            pltpu.VMEM((512, 1024), BF16),
            pltpu.VMEM((512, 1024), BF16),
            pltpu.VMEM((256, 256), BF16),
            pltpu.VMEM((256, 256), BF16),
            pltpu.VMEM((8, 48, 512), BF16),
            pltpu.VMEM((2, 2, 8, 48, 512), BF16),
            pltpu.VMEM((48, 1024), BF16),
            pltpu.VMEM((2, 48, 128), BF16),
            pltpu.VMEM((8, 2, 48, 128), BF16),
            pltpu.VMEM((2, 2, 8, 2, 48, 128), BF16),
            pltpu.VMEM((256, 1024), BF16),
            pltpu.VMEM((64, 32, 128), BF16),
            pltpu.VMEM((32, 32, 256), F32),
            dma((6,)),
            dma((8,)), dma((8,)),
            dma((2, 8)), dma((2, 8)),
            dma((2, 8)), dma((2, 8)),
            dma((2, 8)), dma((2,)),
            dma((8,)), dma((8,)),
            dma((4, 8)), dma((2, 2, 8)),
            dma, dma,
            pltpu.SemaphoreType.REGULAR,
        ],
        compiler_params=pltpu.CompilerParams(collective_id=0, has_side_effects=True),
    )(
        occ, vir, docc.reshape(1, 1024), dvir.reshape(1, 512),
        jnp.asarray(c_table()), jnp.asarray(b_table()),
    )

    def placed(part):
        return jnp.transpose(part.reshape(32, 8, 4, 128), (0, 2, 1, 3)).reshape(32, 4, 1024)

    return placed(res[0]), placed(res[1])


def solution(mesh):
    in_specs = (P("row", "col"), P("row", "col"), P(), P())
    out_specs = (P("row", "col", None), P("row", "col", None))
    return jax.shard_map(
        on_device, mesh=mesh, in_specs=in_specs, out_specs=out_specs, check_vma=False
    )
```

```python
import functools
import math

import jax
import jax.numpy as jnp
import numpy as np
from jax import lax
from jax.experimental import pallas as pl
from jax.experimental.pallas import tpu as pltpu
from jax.sharding import PartitionSpec as P

MESH = pl.DeviceIdType.MESH
F32 = jnp.float32
BF16 = jnp.bfloat16
SCALE = -(2.0**-17)
NEAR, FAR = (1, 7, 2, 6), (3, 5, 4)
DIST = NEAR + FAR


def angle_table(length):
    k = np.arange(length)
    phase = np.outer(k, k) % length
    angle = 2.0 * np.pi * phase / length
    return np.cos(angle), np.sin(angle)


def c_table():
    cos, sin = angle_table(32)
    cos, sin = cos.reshape(32, 8, 1, 4), -sin.reshape(32, 8, 1, 4)
    both = np.stack([cos, sin], axis=2)
    return np.broadcast_to(both, (32, 8, 2, 16, 4)).reshape(32, 1024).astype(np.float32)


def b_table():
    cos, sin = angle_table(32)
    table = np.zeros((2, 2, 16, 4, 2, 4, 32), np.float32)
    for kc in range(4):
        c = cos.reshape(2, 16, 32)
        s = sin.reshape(2, 16, 32)
        table[:, 0, :, kc, 0, kc, :] = c
        table[:, 0, :, kc, 1, kc, :] = -s
        table[:, 1, :, kc, 0, kc, :] = s
        table[:, 1, :, kc, 1, kc, :] = c
    return table.reshape(256, 256)


def fft(parts):
    n = len(parts)
    if n == 1:
        return parts
    half = n // 2
    even, odd = fft(parts[0::2]), fft(parts[1::2])
    low, high = [], []
    for k in range(half):
        (ar, ai), (br, bi) = even[k], odd[k]
        if k == 0:
            tr, ti = br, bi
        elif 4 * k == n:
            tr, ti = bi, -br
        else:
            c, s = math.cos(2 * math.pi * k / n), math.sin(2 * math.pi * k / n)
            tr, ti = c * br + s * bi, c * bi - s * br
        low.append((ar + tr, ai + ti))
        high.append((ar - tr, ai - ti))
    return low + high


def swap_groups(v, lane):
    v = list(v)
    for shift, pairs in ((64, ((0, 2), (1, 3))), (32, ((0, 1), (2, 3)))):
        low = lax.rem(lane, 2 * shift) < shift
        for i, j in pairs:
            a, b = v[i], v[j]
            v[i] = jnp.where(low, a, pltpu.roll(b, shift, 1))
            v[j] = jnp.where(low, pltpu.roll(a, 128 - shift, 1), b)
    return v


def tdot(a, b):
    return lax.dot_general(a, b, (((0,), (0,)), ((), ())), preferred_element_type=F32)


def mdot(a, b):
    return jnp.dot(a, b, preferred_element_type=F32)


def kernel(
    occ, vir, docc, dvir, ctab, xr,
    inb, dov, dvv, ctv, mhi, mlo,
    pz, pb, rs, rc, yb,
    in_sem, p1s, p1r, p2s, p2r, p3s, p3r, ras, rar, rbs, rbr, rcs, rcr, ys, yr, ready,
):
    row, col = lax.axis_index("row"), lax.axis_index("col")
    core = lax.rem(row, 2)
    z = lax.rem(lax.div(row, 2), 8)
    xh = lax.div(row, 16)
    y, xl = lax.rem(col, 4), lax.div(col, 4)
    x = 2 * xh + xl

    def row_of(xh_, z_, k_):
        return (xh_ * 8 + z_) * 2 + k_

    loads = [
        pltpu.make_async_copy(occ, inb.at[pl.ds(0, 32)], in_sem.at[0]),
        pltpu.make_async_copy(vir, inb.at[pl.ds(32, 16)], in_sem.at[1]),
        pltpu.make_async_copy(docc, dov, in_sem.at[2]),
        pltpu.make_async_copy(dvir, dvv, in_sem.at[3]),
        pltpu.make_async_copy(ctab, ctv, in_sem.at[4]),
    ]
    for load in loads:
        load.start()

    barrier = pltpu.get_barrier_semaphore()

    def greet_z(i, c):
        pl.semaphore_signal(barrier, inc=1, device_id=(row_of(xh, i, core), col), device_id_type=MESH)
        return c

    def greet_slab(i, c):
        pl.semaphore_signal(
            barrier, inc=1, device_id=(row_of(xh, z, lax.rem(i, 2)), lax.div(i, 2)), device_id_type=MESH
        )
        return c

    def greet_other(i, c):
        pl.semaphore_signal(
            barrier, inc=1, device_id=(row_of(1 - xh, z, lax.rem(i, 2)), lax.div(i, 2)), device_id_type=MESH
        )
        return c

    lax.fori_loop(0, 8, greet_z, 0)
    lax.fori_loop(0, 16, greet_slab, 0)
    lax.fori_loop(0, 16, greet_other, 0)

    for load in loads:
        load.wait()

    @pl.when(col == 0)
    def _():
        lane = lax.broadcasted_iota(jnp.int32, (32, 1024), 1)
        band = lax.broadcasted_iota(jnp.int32, (32, 1024), 0)
        dec = jnp.sum(jnp.where(lane == band + 32 * row, dov[...], 0.0), axis=1, keepdims=True)
        rs[0:32, :] = (inb[0:32, 0:1024].astype(F32) * dec).astype(BF16)
        lane = lax.broadcasted_iota(jnp.int32, (16, 512), 1)
        band = lax.broadcasted_iota(jnp.int32, (16, 512), 0)
        dec = jnp.sum(jnp.where(lane == band + 16 * row, dvv[...], 0.0), axis=1, keepdims=True)
        rs[32:48, :] = (inb[32:48, 0:1024].astype(F32) * dec).astype(BF16)

    pl.semaphore_wait(barrier, 40)

    def greet_ready(i, c):
        pl.semaphore_signal(
            ready, inc=1, device_id=(row_of(xh, z, lax.rem(i, 2)), lax.div(i, 2)), device_id_type=MESH
        )
        return c

    lax.fori_loop(0, 16, greet_ready, 0)

    def half(h):
        return pl.ds(128 * h, 128)

    def a_copy(h, i):
        s, kk, xt = lax.div(i, 4), lax.rem(lax.div(i, 2), 2), lax.rem(i, 2)
        lanes = pl.ds(pl.multiple_of(512 * s + 256 * kk + 128 * h, 128), 128)
        b = 2 * xh + core
        return pltpu.make_async_remote_copy(
            src_ref=rs.at[:, lanes], dst_ref=rc.at[b, z, :, half(h)], send_sem=ras.at[h, i], recv_sem=rar.at[h],
            device_id=(row_of(s, z, kk), xt * 4 + b), device_id_type=MESH,
        )

    def a_wait(h):
        ref = rc.at[y, z, :, half(h)]
        pltpu.make_async_copy(ref, ref, rar.at[h]).wait()

    def b_copy(h, dz):
        ref = rc.at[y, z, :, half(h)]
        return pltpu.make_async_remote_copy(
            src_ref=ref, dst_ref=ref, send_sem=rbs.at[h, dz], recv_sem=rbr.at[h, z],
            device_id=(row_of(xh, lax.rem(z + dz, 8), core), col), device_id_type=MESH,
        )

    def b_wait(h, zs):
        ref = rc.at[y, zs, :, half(h)]
        pltpu.make_async_copy(ref, ref, rbr.at[h, zs]).wait()

    def c_copy(h, zs, dy):
        ref = rc.at[y, zs, :, half(h)]
        return pltpu.make_async_remote_copy(
            src_ref=ref, dst_ref=ref, send_sem=rcs.at[h, dy, zs], recv_sem=rcr.at[h, y, zs],
            device_id=(row, xl * 4 + lax.rem(y + dy, 4)), device_id_type=MESH,
        )

    def c_wait(h, b, zs):
        ref = rc.at[b, zs, :, half(h)]
        pltpu.make_async_copy(ref, ref, rcr.at[h, b, zs]).wait()

    def p1_copy(dz):
        zt = lax.rem(z + dz, 8)
        lanes = pl.ds(pl.multiple_of(zt * 512, 512), 512)
        return pltpu.make_async_remote_copy(
            src_ref=inb.at[:, lanes], dst_ref=pz.at[z], send_sem=p1s.at[dz], recv_sem=p1r.at[z],
            device_id=(row_of(xh, zt, core), col), device_id_type=MESH,
        )

    def p1_wait(zs):
        pltpu.make_async_copy(pz.at[zs], pz.at[zs], p1r.at[zs]).wait()

    def p2_copy(src, zs, side):
        xt = lax.rem(x + 1 + 2 * side, 4)
        return pltpu.make_async_remote_copy(
            src_ref=src, dst_ref=pb.at[2 * xh + core, zs], send_sem=p2s.at[side, zs], recv_sem=p2r.at[xh, zs],
            device_id=(row_of(lax.div(xt, 2), z, core), lax.rem(xt, 2) * 4 + y), device_id_type=MESH,
        )

    def p2_wait(xs, zs):
        pltpu.make_async_copy(pb.at[2 * xs + core, zs], pb.at[2 * xs + core, zs], p2r.at[xs, zs]).wait()

    def p3_copy(xs, zs):
        return pltpu.make_async_remote_copy(
            src_ref=pb.at[2 * xs + core, zs], dst_ref=pb.at[2 * xs + core, zs], send_sem=p3s.at[xs, zs],
            recv_sem=p3r.at[xs, zs], device_id=(row + 1 - 2 * core, col), device_id_type=MESH,
        )

    def p3_wait(xs, zs):
        other = 1 - core
        pltpu.make_async_copy(pb.at[2 * xs + other, zs], pb.at[2 * xs + other, zs], p3r.at[xs, zs]).wait()

    self_a = jnp.logical_and(col == 0, jnp.logical_and(xh == 0, core == 0))

    @pl.when(col == 0)
    def _():
        def send(i, carry):
            @pl.when(jnp.logical_or(lax.rem(i, 8) != 0, jnp.logical_not(self_a)))
            def _():
                a_copy(lax.div(i, 8), lax.rem(i, 8)).start()

            return carry

        lax.fori_loop(0, 16, send, 0)

    @pl.when(self_a)
    def _():
        rc[0, z] = rs[:, 0:256]

    def near_y(h, zs):
        for dy in (1, 3, 2):
            c_copy(h, zs, dy).start()

    def scattered(h):
        @pl.when(jnp.logical_not(self_a))
        def _():
            a_wait(h)

        for dz in DIST:
            b_copy(h, dz).start()
        near_y(h, z)

    for dz in NEAR:
        p1_copy(dz).start()

    mine = pl.ds(pl.multiple_of(z * 512, 512), 512)
    for side in range(2):
        p2_copy(inb.at[:, mine], z, side).start()

    scattered(0)
    for dz in FAR:
        p1_copy(dz).start()
    scattered(1)

    blane = lax.rem(lax.div(lax.broadcasted_iota(jnp.int32, (32, 1024), 1), 4), 16)
    ct = ctv[...]
    ct_hi = ct.astype(BF16).astype(F32)
    ct_lo = ct - ct_hi

    def table(b, c):
        rows = pl.ds(pl.multiple_of(b * 32, 32), 32)
        mhi[rows, :] = jnp.where(blane == b, ct_hi, 0.0).astype(BF16)
        mlo[rows, :] = jnp.where(blane == b, ct_lo, 0.0).astype(BF16)
        return c

    lax.fori_loop(0, 16, table, 0)
    def source(dz):
        return lax.rem(z + 8 - dz, 8)

    def relay(dz):
        zs = source(dz)
        p1_wait(zs)
        p2_copy(pz.at[zs], zs, 0).start()
        p2_copy(pz.at[zs], zs, 1).start()

    def forward(dz):
        zs = source(dz)
        for xs in range(2):
            p2_wait(xs, zs)
            p3_copy(xs, zs).start()

    for dz in NEAR:
        relay(dz)
    for dz in DIST:
        b_wait(0, source(dz))
        near_y(0, source(dz))
    for dz in (0, *NEAR):
        forward(dz)
    for dz in FAR:
        relay(dz)
    for dz in DIST:
        b_wait(1, source(dz))
        near_y(1, source(dz))
    for dz in FAR:
        forward(dz)

    def arrive(zs, carry):
        for xs in range(2):
            p3_wait(xs, zs)
        return carry

    lax.fori_loop(0, 8, arrive, 0)

    slot = ((1 - xl) * 4 + y) * 8 + z
    has_self = lax.div(z, 4) == core

    def y_copy(m, c):
        rows = pl.ds(pl.multiple_of(m * 32, 32), 32)
        lanes = pl.ds(pl.multiple_of(c * 128, 128), 128)
        return pltpu.make_async_remote_copy(
            src_ref=yb.at[rows, lanes], dst_ref=xr.at[slot], send_sem=ys, recv_sem=yr,
            device_id=(16 * xh + 8 * core + m, c), device_id_type=MESH,
        )

    pl.semaphore_wait(ready, 16)
    for h in range(2):
        def gathered(zs, carry):
            for dy in range(1, 4):
                c_wait(h, lax.rem(y + dy, 4), zs)
            return carry

        lax.fori_loop(0, 8, gathered, 0)

        acc_o = jnp.zeros((128, 512), F32)
        acc_v = jnp.zeros((128, 512), F32)
        lanes = slice(128 * h, 128 * h + 128)
        for b in range(4):
            acc_o += tdot(rc[b, :, 0:32, lanes].reshape(256, 128), pb[b, :, 0:32, :].reshape(256, 512))
            acc_v += tdot(rc[b, :, 32:48, lanes].reshape(128, 128), pb[b, :, 32:48, :].reshape(128, 512))
        polar = acc_o * acc_v * SCALE
        hi = polar.astype(BF16)
        lo = (polar - hi.astype(F32)).astype(BF16)
        yb[128 * h : 128 * h + 128, :] = (mdot(hi, mhi[...]) + mdot(hi, mlo[...]) + mdot(lo, mhi[...])).astype(BF16)

        def y_send(i, carry):
            m = 4 * h + lax.rem(i, 4)
            c = lax.rem(lax.div(i, 4) + col, 8)

            @pl.when(jnp.logical_or(16 * xh + 8 * core + m != row, c != col))
            def _():
                y_copy(m, c).start()

            return carry

        lax.fori_loop(0, 32, y_send, 0)

    @pl.when(has_self)
    def _():
        m = row - 16 * xh - 8 * core
        xr[slot] = yb[pl.ds(pl.multiple_of(m * 32, 32), 32), pl.ds(pl.multiple_of(col * 128, 128), 128)]
        pltpu.make_async_copy(xr.at[pl.ds(0, 63)], xr.at[pl.ds(0, 63)], yr).wait()

    @pl.when(jnp.logical_not(has_self))
    def _():
        pltpu.make_async_copy(xr, xr, yr).wait()

    @pl.when(col == 0)
    def _():
        def sent(i, carry):
            @pl.when(jnp.logical_or(lax.rem(i, 8) != 0, jnp.logical_not(self_a)))
            def _():
                a_copy(lax.div(i, 8), lax.rem(i, 8)).wait_send()

            return carry

        lax.fori_loop(0, 16, sent, 0)

    def sent_z(dz, carry):
        p1_copy(dz).wait_send()
        for h in range(2):
            b_copy(h, dz).wait_send()
        return carry

    lax.fori_loop(1, 8, sent_z, 0)

    def sent_zs(zs, carry):
        for side in range(2):
            p2_copy(pz.at[zs], zs, side).wait_send()
            p3_copy(side, zs).wait_send()
        for h in range(2):
            for dy in range(1, 4):
                c_copy(h, zs, dy).wait_send()
        return carry

    lax.fori_loop(0, 8, sent_zs, 0)

    @pl.when(has_self)
    def _():
        pltpu.make_async_copy(xr.at[pl.ds(0, 63)], xr.at[pl.ds(0, 63)], ys).wait()

    @pl.when(jnp.logical_not(has_self))
    def _():
        pltpu.make_async_copy(xr, xr, ys).wait()


def finish(xr, btab, out_re, out_im, nhi, nlo, zb, res_re, res_im, sem):
    bt = btab[...]
    bt_hi = bt.astype(BF16)
    nhi[...] = bt_hi
    nlo[...] = (bt - bt_hi.astype(F32)).astype(BF16)

    def b_step(i, carry):
        part = xr[pl.ds(pl.multiple_of(16 * i, 16), 16)].reshape(8, 2, 32, 128)
        both = jnp.concatenate([part[:, 0].reshape(256, 128), part[:, 1].reshape(256, 128)], axis=1)
        res = mdot(both, nhi[...]) + mdot(both, nlo[...])
        zb[pl.ds(8 * i, 8)] = res.reshape(8, 32, 256)
        return carry

    lax.fori_loop(0, 4, b_step, 0)

    lane = lax.broadcasted_iota(jnp.int32, (8, 128), 1)

    def put(i, which):
        res, out = ((res_re, out_re), (res_im, out_im))[which]
        rows = pl.ds(pl.multiple_of(256 * i, 256), 256)
        return pltpu.make_async_copy(res.at[rows], out.at[rows], sem.at[which, i])

    def a_step(i, carry):
        rows = pl.ds(pl.multiple_of(8 * i, 8), 8)
        res = fft([(zb[a, rows, 0:128], zb[a, rows, 128:256]) for a in range(32)])
        for j in range(8):
            for part, out in ((0, res_re), (1, res_im)):
                moved = swap_groups([res[4 * j + t][part] for t in range(4)], lane)
                for kc in range(4):
                    out[pl.ds(i * 256 + j * 4 + kc, 8, stride=32), :] = moved[kc]
        put(i, 0).start()
        put(i, 1).start()
        return carry

    lax.fori_loop(0, 4, a_step, 0)
    for i in range(4):
        put(i, 0).wait()
        put(i, 1).wait()


def on_device(occ, vir, docc, dvir):
    anyspace = pl.BlockSpec(memory_space=pl.ANY)
    vmem = pl.BlockSpec(memory_space=pltpu.VMEM)
    dma = pltpu.SemaphoreType.DMA
    xr = pl.pallas_call(
        kernel,
        out_shape=pltpu.VMEM((64, 32, 128), BF16),
        in_specs=[anyspace] * 5,
        out_specs=vmem,
        scratch_shapes=[
            pltpu.VMEM((48, 4096), BF16),
            pltpu.VMEM((1, 1024), F32),
            pltpu.VMEM((1, 512), F32),
            pltpu.VMEM((32, 1024), F32),
            pltpu.VMEM((512, 1024), BF16),
            pltpu.VMEM((512, 1024), BF16),
            pltpu.VMEM((8, 48, 512), BF16),
            pltpu.VMEM((4, 8, 48, 512), BF16),
            pltpu.VMEM((48, 1024), BF16),
            pltpu.VMEM((4, 8, 48, 256), BF16),
            pltpu.VMEM((256, 1024), BF16),
            dma((5,)),
            dma((8,)), dma((8,)),
            dma((2, 8)), dma((2, 8)),
            dma((2, 8)), dma((2, 8)),
            dma((2, 8)), dma((2,)),
            dma((2, 8)), dma((2, 8)),
            dma((2, 4, 8)), dma((2, 4, 8)),
            dma, dma,
            pltpu.SemaphoreType.REGULAR,
        ],
        compiler_params=pltpu.CompilerParams(collective_id=0, has_side_effects=True),
    )(occ, vir, docc.reshape(1, 1024), dvir.reshape(1, 512), jnp.asarray(c_table()))
    out = jax.ShapeDtypeStruct((1024, 128), F32)
    res = pl.pallas_call(
        finish,
        out_shape=(out, out),
        in_specs=[vmem, vmem],
        out_specs=(anyspace, anyspace),
        scratch_shapes=[
            pltpu.VMEM((256, 256), BF16),
            pltpu.VMEM((256, 256), BF16),
            pltpu.VMEM((32, 32, 256), F32),
            pltpu.VMEM((1024, 128), F32),
            pltpu.VMEM((1024, 128), F32),
            dma((2, 4)),
        ],
    )(pltpu.with_memory_space_constraint(xr, pltpu.VMEM), jnp.asarray(b_table()))

    def placed(part):
        return jnp.transpose(part.reshape(32, 8, 4, 128), (0, 2, 1, 3)).reshape(32, 4, 1024)

    return placed(res[0]), placed(res[1])


def solution(mesh):
    in_specs = (P("row", "col"), P("row", "col"), P(), P())
    out_specs = (P("row", "col", None), P("row", "col", None))
    return jax.shard_map(
        on_device, mesh=mesh, in_specs=in_specs, out_specs=out_specs, check_vma=False
    )
```

```python
import functools
import math

import jax
import jax.numpy as jnp
import numpy as np
from jax import lax
from jax.experimental import pallas as pl
from jax.experimental.pallas import tpu as pltpu
from jax.sharding import PartitionSpec as P

MESH = pl.DeviceIdType.MESH
F32 = jnp.float32
BF16 = jnp.bfloat16
SCALE = -(2.0**-17)
NEAR, FAR = (1, 7, 2, 6), (3, 5, 4)
DIST = NEAR + FAR


def angle_table(length):
    k = np.arange(length)
    phase = np.outer(k, k) % length
    angle = 2.0 * np.pi * phase / length
    return np.cos(angle), np.sin(angle)


def c_table():
    cos, sin = angle_table(32)
    cos, sin = cos.reshape(32, 8, 1, 4), -sin.reshape(32, 8, 1, 4)
    both = np.stack([cos, sin], axis=2)
    return np.broadcast_to(both, (32, 8, 2, 16, 4)).reshape(32, 1024).astype(np.float32)


def b_table():
    cos, sin = angle_table(32)
    table = np.zeros((2, 2, 16, 4, 2, 4, 32), np.float32)
    for kc in range(4):
        c = cos.reshape(2, 16, 32)
        s = sin.reshape(2, 16, 32)
        table[:, 0, :, kc, 0, kc, :] = c
        table[:, 0, :, kc, 1, kc, :] = -s
        table[:, 1, :, kc, 0, kc, :] = s
        table[:, 1, :, kc, 1, kc, :] = c
    return table.reshape(256, 256)


def fft(parts):
    n = len(parts)
    if n == 1:
        return parts
    half = n // 2
    even, odd = fft(parts[0::2]), fft(parts[1::2])
    low, high = [], []
    for k in range(half):
        (ar, ai), (br, bi) = even[k], odd[k]
        if k == 0:
            tr, ti = br, bi
        elif 4 * k == n:
            tr, ti = bi, -br
        else:
            c, s = math.cos(2 * math.pi * k / n), math.sin(2 * math.pi * k / n)
            tr, ti = c * br + s * bi, c * bi - s * br
        low.append((ar + tr, ai + ti))
        high.append((ar - tr, ai - ti))
    return low + high


def swap_groups(v, lane):
    v = list(v)
    for shift, pairs in ((64, ((0, 2), (1, 3))), (32, ((0, 1), (2, 3)))):
        low = lax.rem(lane, 2 * shift) < shift
        for i, j in pairs:
            a, b = v[i], v[j]
            v[i] = jnp.where(low, a, pltpu.roll(b, shift, 1))
            v[j] = jnp.where(low, pltpu.roll(a, 128 - shift, 1), b)
    return v


def tdot(a, b):
    return lax.dot_general(a, b, (((0,), (0,)), ((), ())), preferred_element_type=F32)


def mdot(a, b):
    return jnp.dot(a, b, preferred_element_type=F32)


def kernel(
    occ, vir, docc, dvir, ctab, btab, xr, ntab,
    inb, dov, dvv, ctv, mtab,
    pz, pb, rs, rc, yb,
    in_sem, p1s, p1r, p2s, p2r, p3s, p3r, ras, rar, rbs, rbr, rxs, rxr, rcs, rcr, ys, yr, ready,
):
    row, col = lax.axis_index("row"), lax.axis_index("col")
    core = lax.rem(row, 2)
    z = lax.rem(lax.div(row, 2), 8)
    xh = lax.div(row, 16)
    y, xl = lax.rem(col, 4), lax.div(col, 4)
    x = 2 * xh + xl

    def row_of(xh_, z_, k_):
        return (xh_ * 8 + z_) * 2 + k_

    loads = [
        pltpu.make_async_copy(occ, inb.at[pl.ds(0, 32)], in_sem.at[0]),
        pltpu.make_async_copy(vir, inb.at[pl.ds(32, 16)], in_sem.at[1]),
        pltpu.make_async_copy(docc, dov, in_sem.at[2]),
        pltpu.make_async_copy(dvir, dvv, in_sem.at[3]),
        pltpu.make_async_copy(ctab, ctv, in_sem.at[4]),
        pltpu.make_async_copy(btab, ntab, in_sem.at[5]),
    ]
    for load in loads:
        load.start()

    barrier = pltpu.get_barrier_semaphore()

    def greet_z(i, c):
        pl.semaphore_signal(barrier, inc=1, device_id=(row_of(xh, i, core), col), device_id_type=MESH)
        return c

    def greet_slab(i, c):
        pl.semaphore_signal(
            barrier, inc=1, device_id=(row_of(xh, z, lax.rem(i, 2)), lax.div(i, 2)), device_id_type=MESH
        )
        return c

    def greet_other(i, c):
        pl.semaphore_signal(
            barrier, inc=1, device_id=(row_of(1 - xh, z, lax.rem(i, 2)), lax.div(i, 2)), device_id_type=MESH
        )
        return c

    lax.fori_loop(0, 8, greet_z, 0)
    lax.fori_loop(0, 16, greet_slab, 0)
    lax.fori_loop(0, 16, greet_other, 0)

    for load in loads:
        load.wait()

    @pl.when(col == 0)
    def _():
        lane = lax.broadcasted_iota(jnp.int32, (32, 1024), 1)
        band = lax.broadcasted_iota(jnp.int32, (32, 1024), 0)
        dec = jnp.sum(jnp.where(lane == band + 32 * row, dov[...], 0.0), axis=1, keepdims=True)
        rs[0:32, :] = (inb[0:32, 0:1024].astype(F32) * dec).astype(BF16)
        lane = lax.broadcasted_iota(jnp.int32, (16, 512), 1)
        band = lax.broadcasted_iota(jnp.int32, (16, 512), 0)
        dec = jnp.sum(jnp.where(lane == band + 16 * row, dvv[...], 0.0), axis=1, keepdims=True)
        rs[32:48, :] = (inb[32:48, 0:1024].astype(F32) * dec).astype(BF16)

    pl.semaphore_wait(barrier, 40)

    def greet_ready(i, c):
        pl.semaphore_signal(
            ready, inc=1, device_id=(row_of(xh, z, lax.rem(i, 2)), lax.div(i, 2)), device_id_type=MESH
        )
        return c

    lax.fori_loop(0, 16, greet_ready, 0)

    def landed(ref, sem):
        pltpu.make_async_copy(ref, ref, sem).wait()

    def a_copy(i):
        s, kk, xt = lax.div(i, 4), lax.rem(lax.div(i, 2), 2), lax.rem(i, 2)
        lanes = pl.ds(pl.multiple_of(512 * s + 256 * kk + 128 * xt, 128), 128)
        b = 2 * xh + core
        return pltpu.make_async_remote_copy(
            src_ref=rs.at[:, lanes], dst_ref=rc.at[0, b, z], send_sem=ras, recv_sem=rar,
            device_id=(row_of(s, z, kk), xt * 4 + b), device_id_type=MESH,
        )

    def b_copy(dz):
        ref = rc.at[0, y, z]
        return pltpu.make_async_remote_copy(
            src_ref=ref, dst_ref=ref, send_sem=rbs, recv_sem=rbr.at[z],
            device_id=(row_of(xh, lax.rem(z + dz, 8), core), col), device_id_type=MESH,
        )

    def x_copy(zs):
        return pltpu.make_async_remote_copy(
            src_ref=rc.at[0, y, zs], dst_ref=rc.at[1, y, zs], send_sem=rxs, recv_sem=rxr.at[zs],
            device_id=(row, (1 - xl) * 4 + y), device_id_type=MESH,
        )

    def c_copy(o, zs, dy):
        ref = rc.at[o, y, zs]
        return pltpu.make_async_remote_copy(
            src_ref=ref, dst_ref=ref, send_sem=rcs, recv_sem=rcr.at[o],
            device_id=(row, xl * 4 + lax.rem(y + dy, 4)), device_id_type=MESH,
        )

    def near_y(o, zs):
        for dy in (1, 3, 2):
            c_copy(o, zs, dy).start()

    def p1_copy(dz):
        zt = lax.rem(z + dz, 8)
        lanes = pl.ds(pl.multiple_of(zt * 512, 512), 512)
        return pltpu.make_async_remote_copy(
            src_ref=inb.at[:, lanes], dst_ref=pz.at[z], send_sem=p1s, recv_sem=p1r.at[z],
            device_id=(row_of(xh, zt, core), col), device_id_type=MESH,
        )

    def p2_copy(src, zs, side):
        xt = lax.rem(x + 1 + 2 * side, 4)
        return pltpu.make_async_remote_copy(
            src_ref=src, dst_ref=pb.at[2 * xh + core, zs], send_sem=p2s, recv_sem=p2r.at[zs],
            device_id=(row_of(lax.div(xt, 2), z, core), lax.rem(xt, 2) * 4 + y), device_id_type=MESH,
        )

    def p3_copy(xs, zs):
        return pltpu.make_async_remote_copy(
            src_ref=pb.at[2 * xs + core, zs], dst_ref=pb.at[2 * xs + core, zs], send_sem=p3s,
            recv_sem=p3r, device_id=(row + 1 - 2 * core, col), device_id_type=MESH,
        )

    self_a = jnp.logical_and(col == 0, jnp.logical_and(xh == 0, core == 0))

    @pl.when(col == 0)
    def _():
        def send(i, carry):
            @pl.when(jnp.logical_or(i != 0, jnp.logical_not(self_a)))
            def _():
                a_copy(i).start()

            return carry

        lax.fori_loop(0, 8, send, 0)

    @pl.when(self_a)
    def _():
        rc[0, 0, z] = rs[:, 0:128]

    for dz in NEAR:
        p1_copy(dz).start()

    mine = pl.ds(pl.multiple_of(z * 512, 512), 512)
    for side in range(2):
        p2_copy(inb.at[:, mine], z, side).start()

    @pl.when(jnp.logical_not(self_a))
    def _():
        landed(rc.at[0, y, z], rar)

    for dz in DIST:
        b_copy(dz).start()
    near_y(0, z)
    x_copy(z).start()
    for dz in FAR:
        p1_copy(dz).start()

    blane = lax.rem(lax.div(lax.broadcasted_iota(jnp.int32, (32, 1024), 1), 4), 16)
    ct = ctv[...]

    def table(b, c):
        rows = pl.ds(pl.multiple_of(b * 32, 32), 32)
        mtab[rows, :] = jnp.where(blane == b, ct, 0.0).astype(BF16)
        return c

    lax.fori_loop(0, 16, table, 0)

    def source(dz):
        return lax.rem(z + 8 - dz, 8)

    def relay(dz):
        zs = source(dz)
        landed(pz.at[zs], p1r.at[zs])
        p2_copy(pz.at[zs], zs, 0).start()
        p2_copy(pz.at[zs], zs, 1).start()

    def forward(dz):
        zs = source(dz)
        landed(pb.at[pl.ds(0, 2), zs], p2r.at[zs])
        p3_copy(0, zs).start()
        p3_copy(1, zs).start()

    for dz in NEAR:
        relay(dz)
    for dz in DIST:
        zs = source(dz)
        landed(rc.at[0, y, zs], rbr.at[zs])
        near_y(0, zs)
        x_copy(zs).start()
    for dz in FAR:
        relay(dz)
    for dz in (0, *NEAR):
        forward(dz)
    for dz in (0, *DIST):
        zs = source(dz)
        landed(rc.at[1, y, zs], rxr.at[zs])
        near_y(1, zs)
    for dz in FAR:
        forward(dz)
    landed(pb.at[pl.ds(0, 2)], p3r)

    slot = ((1 - xl) * 4 + y) * 8 + z
    has_self = lax.div(z, 4) == core

    def y_copy(o, i, c):
        rows = pl.ds(pl.multiple_of(o * 128 + i * 32, 32), 32)
        lanes = pl.ds(pl.multiple_of(c * 128, 128), 128)
        return pltpu.make_async_remote_copy(
            src_ref=yb.at[rows, lanes], dst_ref=xr.at[slot], send_sem=ys, recv_sem=yr,
            device_id=(16 * xh + 8 * core + 4 * half(o) + i, c), device_id_type=MESH,
        )

    def half(o):
        return xl + o - 2 * xl * o

    pl.semaphore_wait(ready, 16)
    for o in range(2):
        landed(rc.at[o, pl.ds(0, 3)], rcr.at[o])
        acc_o = jnp.zeros((128, 512), F32)
        acc_v = jnp.zeros((128, 512), F32)
        for b in range(4):
            acc_o += tdot(rc[o, b, :, 0:32, :].reshape(256, 128), pb[b, :, 0:32, :].reshape(256, 512))
            acc_v += tdot(rc[o, b, :, 32:48, :].reshape(128, 128), pb[b, :, 32:48, :].reshape(128, 512))
        polar = (acc_o * acc_v * SCALE).astype(BF16)
        yb[128 * o : 128 * o + 128, :] = mdot(polar, mtab[...]).astype(BF16)

        def y_send(j, carry):
            i = lax.rem(j, 4)
            c = lax.rem(lax.div(j, 4) + col, 8)

            @pl.when(jnp.logical_or(16 * xh + 8 * core + 4 * half(o) + i != row, c != col))
            def _():
                y_copy(o, i, c).start()

            return carry

        lax.fori_loop(0, 32, y_send, 0)

    @pl.when(has_self)
    def _():
        m = row - 16 * xh - 8 * core
        o = jnp.abs(lax.div(m, 4) - xl)
        rows = pl.ds(pl.multiple_of(o * 128 + lax.rem(m, 4) * 32, 32), 32)
        xr[slot] = yb[rows, pl.ds(pl.multiple_of(col * 128, 128), 128)]
        landed(xr.at[pl.ds(0, 63)], yr)

    @pl.when(jnp.logical_not(has_self))
    def _():
        landed(xr, yr)

    @pl.when(jnp.logical_and(col == 0, jnp.logical_not(self_a)))
    def _():
        landed(rc.at[0, 0], ras)

    @pl.when(self_a)
    def _():
        landed(rc.at[0, 0, pl.ds(0, 7)], ras)

    landed(pz.at[pl.ds(0, 7)], p1s)
    landed(rc.at[0, 0, pl.ds(0, 7)], rbs)
    landed(rc.at[0, 0], rxs)
    landed(pb.at[pl.ds(0, 2)], p2s)
    landed(pb.at[pl.ds(0, 2)], p3s)
    landed(rc.at[0, pl.ds(0, 3)], rcs)
    landed(rc.at[1, pl.ds(0, 3)], rcs)

    @pl.when(has_self)
    def _():
        landed(xr.at[pl.ds(0, 63)], ys)

    @pl.when(jnp.logical_not(has_self))
    def _():
        landed(xr, ys)


def finish(xr, ntab, out_re, out_im, zb, res_re, res_im, sem):
    def b_step(i, carry):
        part = xr[pl.ds(pl.multiple_of(16 * i, 16), 16)].reshape(8, 2, 32, 128)
        both = jnp.concatenate([part[:, 0].reshape(256, 128), part[:, 1].reshape(256, 128)], axis=1)
        res = mdot(both, ntab[...])
        zb[pl.ds(8 * i, 8)] = res.reshape(8, 32, 256)
        return carry

    lax.fori_loop(0, 4, b_step, 0)

    lane = lax.broadcasted_iota(jnp.int32, (8, 128), 1)

    def put(i, which):
        res, out = ((res_re, out_re), (res_im, out_im))[which]
        rows = pl.ds(pl.multiple_of(256 * i, 256), 256)
        return pltpu.make_async_copy(res.at[rows], out.at[rows], sem.at[which, i])

    def a_step(i, carry):
        rows = pl.ds(pl.multiple_of(8 * i, 8), 8)
        res = fft([(zb[a, rows, 0:128], zb[a, rows, 128:256]) for a in range(32)])
        for j in range(8):
            for part, out in ((0, res_re), (1, res_im)):
                moved = swap_groups([res[4 * j + t][part] for t in range(4)], lane)
                for kc in range(4):
                    out[pl.ds(i * 256 + j * 4 + kc, 8, stride=32), :] = moved[kc]
        put(i, 0).start()
        put(i, 1).start()
        return carry

    lax.fori_loop(0, 4, a_step, 0)
    for i in range(4):
        put(i, 0).wait()
        put(i, 1).wait()


def on_device(occ, vir, docc, dvir):
    anyspace = pl.BlockSpec(memory_space=pl.ANY)
    vmem = pl.BlockSpec(memory_space=pltpu.VMEM)
    dma = pltpu.SemaphoreType.DMA
    xr, ntab = pl.pallas_call(
        kernel,
        out_shape=(pltpu.VMEM((64, 32, 128), BF16), pltpu.VMEM((256, 256), BF16)),
        in_specs=[anyspace] * 6,
        out_specs=(vmem, vmem),
        scratch_shapes=[
            pltpu.VMEM((48, 4096), BF16),
            pltpu.VMEM((1, 1024), F32),
            pltpu.VMEM((1, 512), F32),
            pltpu.VMEM((32, 1024), F32),
            pltpu.VMEM((512, 1024), BF16),
            pltpu.VMEM((8, 48, 512), BF16),
            pltpu.VMEM((4, 8, 48, 512), BF16),
            pltpu.VMEM((48, 1024), BF16),
            pltpu.VMEM((2, 4, 8, 48, 128), BF16),
            pltpu.VMEM((256, 1024), BF16),
            dma((6,)),
            dma, dma((8,)),
            dma, dma((8,)),
            dma, dma,
            dma, dma,
            dma, dma((8,)),
            dma, dma((8,)),
            dma, dma((2,)),
            dma, dma,
            pltpu.SemaphoreType.REGULAR,
        ],
        compiler_params=pltpu.CompilerParams(collective_id=0, has_side_effects=True),
    )(
        occ, vir, docc.reshape(1, 1024), dvir.reshape(1, 512),
        jnp.asarray(c_table()), jnp.asarray(b_table()).astype(BF16),
    )
    out = jax.ShapeDtypeStruct((1024, 128), F32)
    res = pl.pallas_call(
        finish,
        out_shape=(out, out),
        in_specs=[vmem, vmem],
        out_specs=(anyspace, anyspace),
        scratch_shapes=[
            pltpu.VMEM((32, 32, 256), F32),
            pltpu.VMEM((1024, 128), F32),
            pltpu.VMEM((1024, 128), F32),
            dma((2, 4)),
        ],
    )(pltpu.with_memory_space_constraint(xr, pltpu.VMEM), pltpu.with_memory_space_constraint(ntab, pltpu.VMEM))

    def placed(part):
        return jnp.transpose(part.reshape(32, 8, 4, 128), (0, 2, 1, 3)).reshape(32, 4, 1024)

    return placed(res[0]), placed(res[1])


def solution(mesh):
    in_specs = (P("row", "col"), P("row", "col"), P(), P())
    out_specs = (P("row", "col", None), P("row", "col", None))
    return jax.shard_map(
        on_device, mesh=mesh, in_specs=in_specs, out_specs=out_specs, check_vma=False
    )
```

```python
import functools
import math

import jax
import jax.numpy as jnp
import numpy as np
from jax import lax
from jax.experimental import pallas as pl
from jax.experimental.pallas import tpu as pltpu
from jax.sharding import PartitionSpec as P

MESH = pl.DeviceIdType.MESH
F32 = jnp.float32
BF16 = jnp.bfloat16
SCALE = -(2.0**-17)
NEAR, FAR = (1, 7, 2, 6), (3, 5, 4)
DIST = NEAR + FAR


def angle_table(length):
    k = np.arange(length)
    phase = np.outer(k, k) % length
    angle = 2.0 * np.pi * phase / length
    return np.cos(angle), np.sin(angle)


def c_table():
    cos, sin = angle_table(32)
    cos, sin = cos.reshape(32, 8, 1, 4), -sin.reshape(32, 8, 1, 4)
    both = np.stack([cos, sin], axis=2)
    return np.broadcast_to(both, (32, 8, 2, 16, 4)).reshape(32, 1024).astype(np.float32)


def b_table():
    cos, sin = angle_table(32)
    c, s = cos.reshape(4, 8, 32), sin.reshape(4, 8, 32)
    table = np.zeros((4, 2, 2, 8, 4, 2, 2, 4, 32), np.float32)
    for kc in range(4):
        for h in range(2):
            table[:, 0, h, :, kc, h, 0, kc, :] = c
            table[:, 0, h, :, kc, h, 1, kc, :] = -s
            table[:, 1, h, :, kc, h, 0, kc, :] = s
            table[:, 1, h, :, kc, h, 1, kc, :] = c
    return table.reshape(512, 512)


def fft(parts):
    n = len(parts)
    if n == 1:
        return parts
    half = n // 2
    even, odd = fft(parts[0::2]), fft(parts[1::2])
    low, high = [], []
    for k in range(half):
        (ar, ai), (br, bi) = even[k], odd[k]
        if k == 0:
            tr, ti = br, bi
        elif 4 * k == n:
            tr, ti = bi, -br
        else:
            c, s = math.cos(2 * math.pi * k / n), math.sin(2 * math.pi * k / n)
            tr, ti = c * br + s * bi, c * bi - s * br
        low.append((ar + tr, ai + ti))
        high.append((ar - tr, ai - ti))
    return low + high


def swap_groups(v, lane):
    v = list(v)
    for shift, pairs in ((64, ((0, 2), (1, 3))), (32, ((0, 1), (2, 3)))):
        low = lax.rem(lane, 2 * shift) < shift
        for i, j in pairs:
            a, b = v[i], v[j]
            v[i] = jnp.where(low, a, pltpu.roll(b, shift, 1))
            v[j] = jnp.where(low, pltpu.roll(a, 128 - shift, 1), b)
    return v


def tdot(a, b):
    return lax.dot_general(a, b, (((0,), (0,)), ((), ())), preferred_element_type=F32)


def mdot(a, b):
    return jnp.dot(a, b, preferred_element_type=F32)


def kernel(
    occ, vir, docc, dvir, ctab, btab, xr, ntab,
    inb, dov, dvv, ctv, mtab,
    pz, pb, rs, rc, yb,
    in_sem, p1s, p1r, p2s, p2r, p3s, p3r, ras, rar, rbs, rbr, rxs, rxr, rcs, rcr, ys, yr, ready,
):
    row, col = lax.axis_index("row"), lax.axis_index("col")
    core = lax.rem(row, 2)
    z = lax.rem(lax.div(row, 2), 8)
    xh = lax.div(row, 16)
    y, xl = lax.rem(col, 4), lax.div(col, 4)
    x = 2 * xh + xl

    def row_of(xh_, z_, k_):
        return (xh_ * 8 + z_) * 2 + k_

    loads = [
        pltpu.make_async_copy(occ, inb.at[pl.ds(0, 32)], in_sem.at[0]),
        pltpu.make_async_copy(vir, inb.at[pl.ds(32, 16)], in_sem.at[1]),
        pltpu.make_async_copy(docc, dov, in_sem.at[2]),
        pltpu.make_async_copy(dvir, dvv, in_sem.at[3]),
        pltpu.make_async_copy(ctab, ctv, in_sem.at[4]),
        pltpu.make_async_copy(btab, ntab, in_sem.at[5]),
    ]
    for load in loads:
        load.start()

    barrier = pltpu.get_barrier_semaphore()

    def greet_z(i, c):
        pl.semaphore_signal(barrier, inc=1, device_id=(row_of(xh, i, core), col), device_id_type=MESH)
        return c

    def greet_slab(i, c):
        pl.semaphore_signal(
            barrier, inc=1, device_id=(row_of(xh, z, lax.rem(i, 2)), lax.div(i, 2)), device_id_type=MESH
        )
        return c

    def greet_other(i, c):
        pl.semaphore_signal(
            barrier, inc=1, device_id=(row_of(1 - xh, z, lax.rem(i, 2)), lax.div(i, 2)), device_id_type=MESH
        )
        return c

    lax.fori_loop(0, 8, greet_z, 0)
    lax.fori_loop(0, 16, greet_slab, 0)
    lax.fori_loop(0, 16, greet_other, 0)

    for load in loads:
        load.wait()

    @pl.when(col == 0)
    def _():
        lane = lax.broadcasted_iota(jnp.int32, (32, 1024), 1)
        band = lax.broadcasted_iota(jnp.int32, (32, 1024), 0)
        dec = jnp.sum(jnp.where(lane == band + 32 * row, dov[...], 0.0), axis=1, keepdims=True)
        rs[0:32, :] = (inb[0:32, 0:1024].astype(F32) * dec).astype(BF16)
        lane = lax.broadcasted_iota(jnp.int32, (16, 512), 1)
        band = lax.broadcasted_iota(jnp.int32, (16, 512), 0)
        dec = jnp.sum(jnp.where(lane == band + 16 * row, dvv[...], 0.0), axis=1, keepdims=True)
        rs[32:48, :] = (inb[32:48, 0:1024].astype(F32) * dec).astype(BF16)

    pl.semaphore_wait(barrier, 40)

    def greet_ready(i, c):
        pl.semaphore_signal(
            ready, inc=1, device_id=(row_of(xh, z, lax.rem(i, 2)), lax.div(i, 2)), device_id_type=MESH
        )
        return c

    lax.fori_loop(0, 16, greet_ready, 0)

    def landed(ref, sem):
        pltpu.make_async_copy(ref, ref, sem).wait()

    def a_copy(i):
        s, kk, xt = lax.div(i, 4), lax.rem(lax.div(i, 2), 2), lax.rem(i, 2)
        lanes = pl.ds(pl.multiple_of(512 * s + 256 * kk + 128 * xt, 128), 128)
        b = 2 * xh + core
        return pltpu.make_async_remote_copy(
            src_ref=rs.at[:, lanes], dst_ref=rc.at[0, b, z], send_sem=ras, recv_sem=rar,
            device_id=(row_of(s, z, kk), xt * 4 + b), device_id_type=MESH,
        )

    def b_copy(dz):
        ref = rc.at[0, y, z]
        return pltpu.make_async_remote_copy(
            src_ref=ref, dst_ref=ref, send_sem=rbs, recv_sem=rbr.at[z],
            device_id=(row_of(xh, lax.rem(z + dz, 8), core), col), device_id_type=MESH,
        )

    def x_copy(zs):
        return pltpu.make_async_remote_copy(
            src_ref=rc.at[0, y, zs], dst_ref=rc.at[1, y, zs], send_sem=rxs, recv_sem=rxr.at[zs],
            device_id=(row, (1 - xl) * 4 + y), device_id_type=MESH,
        )

    def c_copy(o, zs, dy):
        ref = rc.at[o, y, zs]
        return pltpu.make_async_remote_copy(
            src_ref=ref, dst_ref=ref, send_sem=rcs, recv_sem=rcr.at[o],
            device_id=(row, xl * 4 + lax.rem(y + dy, 4)), device_id_type=MESH,
        )

    def near_y(o, zs):
        for dy in (1, 3, 2):
            c_copy(o, zs, dy).start()

    def part(zs, p):
        return pl.ds(pl.multiple_of(zs * 512 + p * 256, 256), 256)

    def p1_copy(p, dz):
        zt = lax.rem(z + dz, 8)
        return pltpu.make_async_remote_copy(
            src_ref=inb.at[:, part(zt, p)], dst_ref=pz.at[p, z], send_sem=p1s, recv_sem=p1r.at[p, z],
            device_id=(row_of(xh, zt, core), col), device_id_type=MESH,
        )

    def p2_copy(src, p, zs, side):
        xt = lax.rem(x + 1 + 2 * side, 4)
        return pltpu.make_async_remote_copy(
            src_ref=src, dst_ref=pb.at[p, 2 * xh + core, zs], send_sem=p2s, recv_sem=p2r.at[p, zs],
            device_id=(row_of(lax.div(xt, 2), z, core), lax.rem(xt, 2) * 4 + y), device_id_type=MESH,
        )

    def p3_copy(p, xs, zs):
        ref = pb.at[p, 2 * xs + core, zs]
        return pltpu.make_async_remote_copy(
            src_ref=ref, dst_ref=ref, send_sem=p3s, recv_sem=p3r.at[p],
            device_id=(row + 1 - 2 * core, col), device_id_type=MESH,
        )

    self_a = jnp.logical_and(col == 0, jnp.logical_and(xh == 0, core == 0))

    @pl.when(col == 0)
    def _():
        def send(i, carry):
            @pl.when(jnp.logical_or(i != 0, jnp.logical_not(self_a)))
            def _():
                a_copy(i).start()

            return carry

        lax.fori_loop(0, 8, send, 0)

    @pl.when(self_a)
    def _():
        rc[0, 0, z] = rs[:, 0:128]

    for dz in DIST:
        p1_copy(0, dz).start()
    for p in range(2):
        for side in range(2):
            p2_copy(inb.at[:, part(z, p)], p, z, side).start()

    @pl.when(jnp.logical_not(self_a))
    def _():
        landed(rc.at[0, y, z], rar)

    for dz in DIST:
        b_copy(dz).start()
    near_y(0, z)
    x_copy(z).start()
    for dz in DIST:
        p1_copy(1, dz).start()

    blane = lax.rem(lax.div(lax.broadcasted_iota(jnp.int32, (32, 1024), 1), 4), 16)
    ct = ctv[...]

    def table(b, c):
        rows = pl.ds(pl.multiple_of(b * 32, 32), 32)
        mtab[rows, :] = jnp.where(blane == b, ct, 0.0).astype(BF16)
        return c

    lax.fori_loop(0, 16, table, 0)

    def source(dz):
        return lax.rem(z + 8 - dz, 8)

    def relay(p, dz):
        zs = source(dz)
        landed(pz.at[p, zs], p1r.at[p, zs])
        p2_copy(pz.at[p, zs], p, zs, 0).start()
        p2_copy(pz.at[p, zs], p, zs, 1).start()

    def forward(p, dz):
        zs = source(dz)
        landed(pb.at[p, pl.ds(0, 2), zs], p2r.at[p, zs])
        p3_copy(p, 0, zs).start()
        p3_copy(p, 1, zs).start()

    slot = ((1 - xl) * 4 + y) * 8 + z
    has_self = lax.div(z, 4) == core

    def y_copy(p, o, i, c):
        rows = pl.ds(pl.multiple_of(i * 16, 16), 16)
        lanes = pl.ds(pl.multiple_of(c * 128, 128), 128)
        return pltpu.make_async_remote_copy(
            src_ref=yb.at[p, o, rows, lanes], dst_ref=xr.at[slot, p], send_sem=ys, recv_sem=yr,
            device_id=(16 * xh + 8 * core + 4 * half(o) + i, c), device_id_type=MESH,
        )

    def half(o):
        return xl + o - 2 * xl * o

    def multiply(p, o):
        acc_o = jnp.zeros((128, 256), F32)
        acc_v = jnp.zeros((128, 256), F32)
        for b in range(4):
            acc_o += tdot(rc[o, b, :, 0:32, :].reshape(256, 128), pb[p, b, :, 0:32, :].reshape(256, 256))
            acc_v += tdot(rc[o, b, :, 32:48, :].reshape(128, 128), pb[p, b, :, 32:48, :].reshape(128, 256))
        polar = (acc_o * acc_v * SCALE).astype(BF16).reshape(4, 2, 16, 256)
        both = jnp.concatenate([polar[:, 0].reshape(64, 256), polar[:, 1].reshape(64, 256)], axis=1)
        yb[p, o] = mdot(both, mtab[...]).astype(BF16)

        def y_send(j, carry):
            i = lax.rem(j, 4)
            c = lax.rem(lax.div(j, 4) + col, 8)

            @pl.when(jnp.logical_or(16 * xh + 8 * core + 4 * half(o) + i != row, c != col))
            def _():
                y_copy(p, o, i, c).start()

            return carry

        lax.fori_loop(0, 32, y_send, 0)

    for dz in NEAR:
        relay(0, dz)
    for dz in DIST:
        zs = source(dz)
        landed(rc.at[0, y, zs], rbr.at[zs])
        near_y(0, zs)
        x_copy(zs).start()
    for dz in FAR:
        relay(0, dz)
    for dz in (0, *DIST):
        zs = source(dz)
        landed(rc.at[1, y, zs], rxr.at[zs])
        near_y(1, zs)
    for dz in (0, *DIST):
        forward(0, dz)
    for dz in DIST:
        relay(1, dz)
    landed(pb.at[0, pl.ds(0, 2)], p3r.at[0])
    landed(rc.at[0, pl.ds(0, 3)], rcr.at[0])
    pl.semaphore_wait(ready, 16)
    multiply(0, 0)
    for dz in (0, *DIST):
        forward(1, dz)
    landed(rc.at[1, pl.ds(0, 3)], rcr.at[1])
    multiply(0, 1)
    landed(pb.at[1, pl.ds(0, 2)], p3r.at[1])
    multiply(1, 0)
    multiply(1, 1)

    @pl.when(has_self)
    def _():
        m = row - 16 * xh - 8 * core
        o = jnp.abs(lax.div(m, 4) - xl)
        rows = pl.ds(pl.multiple_of(lax.rem(m, 4) * 16, 16), 16)
        for p in range(2):
            xr[slot, p] = yb[p, o, rows, pl.ds(pl.multiple_of(col * 128, 128), 128)]
        landed(xr.at[pl.ds(0, 63)], yr)

    @pl.when(jnp.logical_not(has_self))
    def _():
        landed(xr, yr)

    @pl.when(jnp.logical_and(col == 0, jnp.logical_not(self_a)))
    def _():
        landed(rc.at[0, 0], ras)

    @pl.when(self_a)
    def _():
        landed(rc.at[0, 0, pl.ds(0, 7)], ras)

    for p in range(2):
        landed(pz.at[p, pl.ds(0, 7)], p1s)
        landed(pb.at[p, pl.ds(0, 2)], p2s)
        landed(pb.at[p, pl.ds(0, 2)], p3s)
    landed(rc.at[0, 0, pl.ds(0, 7)], rbs)
    landed(rc.at[0, 0], rxs)
    landed(rc.at[0, pl.ds(0, 3)], rcs)
    landed(rc.at[1, pl.ds(0, 3)], rcs)

    @pl.when(has_self)
    def _():
        landed(xr.at[pl.ds(0, 63)], ys)

    @pl.when(jnp.logical_not(has_self))
    def _():
        landed(xr, ys)


def finish(xr, ntab, out_re, out_im, zb, res_re, res_im, sem):
    def b_step(i, carry):
        part = xr[pl.ds(pl.multiple_of(16 * i, 16), 16)].reshape(8, 4, 16, 128)
        both = jnp.concatenate([part[:, q].reshape(128, 128) for q in range(4)], axis=1)
        zb[pl.ds(8 * i, 8)] = mdot(both, ntab[...]).reshape(8, 16, 512)
        return carry

    lax.fori_loop(0, 4, b_step, 0)

    lane = lax.broadcasted_iota(jnp.int32, (8, 128), 1)

    def put(i, which):
        res, out = ((res_re, out_re), (res_im, out_im))[which]
        rows = pl.ds(pl.multiple_of(256 * i, 256), 256)
        return pltpu.make_async_copy(res.at[rows], out.at[rows], sem.at[which, i])

    def a_step(i, carry):
        rows = pl.ds(pl.multiple_of(8 * lax.rem(i, 2), 8), 8)
        real = pl.ds(pl.multiple_of(256 * lax.div(i, 2), 128), 128)
        imag = pl.ds(pl.multiple_of(256 * lax.div(i, 2) + 128, 128), 128)
        res = fft([(zb[a, rows, real], zb[a, rows, imag]) for a in range(32)])
        for j in range(8):
            for part, out in ((0, res_re), (1, res_im)):
                moved = swap_groups([res[4 * j + t][part] for t in range(4)], lane)
                for kc in range(4):
                    out[pl.ds(i * 256 + j * 4 + kc, 8, stride=32), :] = moved[kc]
        put(i, 0).start()
        put(i, 1).start()
        return carry

    lax.fori_loop(0, 4, a_step, 0)
    for i in range(4):
        put(i, 0).wait()
        put(i, 1).wait()


def on_device(occ, vir, docc, dvir):
    anyspace = pl.BlockSpec(memory_space=pl.ANY)
    vmem = pl.BlockSpec(memory_space=pltpu.VMEM)
    dma = pltpu.SemaphoreType.DMA
    xr, ntab = pl.pallas_call(
        kernel,
        out_shape=(pltpu.VMEM((64, 2, 16, 128), BF16), pltpu.VMEM((512, 512), BF16)),
        in_specs=[anyspace] * 6,
        out_specs=(vmem, vmem),
        scratch_shapes=[
            pltpu.VMEM((48, 4096), BF16),
            pltpu.VMEM((1, 1024), F32),
            pltpu.VMEM((1, 512), F32),
            pltpu.VMEM((32, 1024), F32),
            pltpu.VMEM((512, 1024), BF16),
            pltpu.VMEM((2, 8, 48, 256), BF16),
            pltpu.VMEM((2, 4, 8, 48, 256), BF16),
            pltpu.VMEM((48, 1024), BF16),
            pltpu.VMEM((2, 4, 8, 48, 128), BF16),
            pltpu.VMEM((2, 2, 64, 1024), BF16),
            dma((6,)),
            dma, dma((2, 8)),
            dma, dma((2, 8)),
            dma, dma((2,)),
            dma, dma,
            dma, dma((8,)),
            dma, dma((8,)),
            dma, dma((2,)),
            dma, dma,
            pltpu.SemaphoreType.REGULAR,
        ],
        compiler_params=pltpu.CompilerParams(collective_id=0, has_side_effects=True),
    )(
        occ, vir, docc.reshape(1, 1024), dvir.reshape(1, 512),
        jnp.asarray(c_table()), jnp.asarray(b_table()).astype(BF16),
    )
    out = jax.ShapeDtypeStruct((1024, 128), F32)
    res = pl.pallas_call(
        finish,
        out_shape=(out, out),
        in_specs=[vmem, vmem],
        out_specs=(anyspace, anyspace),
        scratch_shapes=[
            pltpu.VMEM((32, 16, 512), F32),
            pltpu.VMEM((1024, 128), F32),
            pltpu.VMEM((1024, 128), F32),
            dma((2, 4)),
        ],
    )(pltpu.with_memory_space_constraint(xr, pltpu.VMEM), pltpu.with_memory_space_constraint(ntab, pltpu.VMEM))

    def placed(part):
        return jnp.transpose(part.reshape(32, 8, 4, 128), (0, 2, 1, 3)).reshape(32, 4, 1024)

    return placed(res[0]), placed(res[1])


def solution(mesh):
    in_specs = (P("row", "col"), P("row", "col"), P(), P())
    out_specs = (P("row", "col", None), P("row", "col", None))
    return jax.shard_map(
        on_device, mesh=mesh, in_specs=in_specs, out_specs=out_specs, check_vma=False
    )
```

```python
import functools
import math

import jax
import jax.numpy as jnp
import numpy as np
from jax import lax
from jax.experimental import pallas as pl
from jax.experimental.pallas import tpu as pltpu
from jax.sharding import PartitionSpec as P

MESH = pl.DeviceIdType.MESH
F32 = jnp.float32
BF16 = jnp.bfloat16
SCALE = -(2.0**-17)
NEAR, FAR = (1, 7, 2, 6), (3, 5, 4)
DIST = NEAR + FAR


def angle_table(length):
    k = np.arange(length)
    phase = np.outer(k, k) % length
    angle = 2.0 * np.pi * phase / length
    return np.cos(angle), np.sin(angle)


def c_table():
    cos, sin = angle_table(32)
    cos, sin = cos.reshape(32, 8, 1, 4), -sin.reshape(32, 8, 1, 4)
    both = np.stack([cos, sin], axis=2)
    return np.broadcast_to(both, (32, 8, 2, 16, 4)).reshape(32, 1024).astype(np.float32)


def b_table():
    cos, sin = angle_table(32)
    table = np.zeros((2, 2, 16, 4, 2, 4, 32), np.float32)
    for kc in range(4):
        c = cos.reshape(2, 16, 32)
        s = sin.reshape(2, 16, 32)
        table[:, 0, :, kc, 0, kc, :] = c
        table[:, 0, :, kc, 1, kc, :] = -s
        table[:, 1, :, kc, 0, kc, :] = s
        table[:, 1, :, kc, 1, kc, :] = c
    return table.reshape(256, 256)


def fft(parts):
    n = len(parts)
    if n == 1:
        return parts
    half = n // 2
    even, odd = fft(parts[0::2]), fft(parts[1::2])
    low, high = [], []
    for k in range(half):
        (ar, ai), (br, bi) = even[k], odd[k]
        if k == 0:
            tr, ti = br, bi
        elif 4 * k == n:
            tr, ti = bi, -br
        else:
            c, s = math.cos(2 * math.pi * k / n), math.sin(2 * math.pi * k / n)
            tr, ti = c * br + s * bi, c * bi - s * br
        low.append((ar + tr, ai + ti))
        high.append((ar - tr, ai - ti))
    return low + high


def swap_groups(v, lane):
    v = list(v)
    for shift, pairs in ((64, ((0, 2), (1, 3))), (32, ((0, 1), (2, 3)))):
        low = lax.rem(lane, 2 * shift) < shift
        for i, j in pairs:
            a, b = v[i], v[j]
            v[i] = jnp.where(low, a, pltpu.roll(b, shift, 1))
            v[j] = jnp.where(low, pltpu.roll(a, 128 - shift, 1), b)
    return v


def tdot(a, b):
    return lax.dot_general(a, b, (((0,), (0,)), ((), ())), preferred_element_type=F32)


def mdot(a, b):
    return jnp.dot(a, b, preferred_element_type=F32)


def kernel(
    occ, vir, docc, dvir, ctab, btab, zb,
    inb, dov, dvv, ctv, mtab, ntab,
    pz, pb, rs, rc, rto, rtv, gp, pr, xs, xr,
    in_sem, p1s, p1r, p2s, p2r, p3s, p3r, ras, rar, rbs, rbr, rxs, rxr, rcs, rcr, gs, gr, ys, yr, ready,
):
    row, col = lax.axis_index("row"), lax.axis_index("col")
    core = lax.rem(row, 2)
    z = lax.rem(lax.div(row, 2), 8)
    xh = lax.div(row, 16)
    y, xl = lax.rem(col, 4), lax.div(col, 4)
    x = 2 * xh + xl

    def row_of(xh_, z_, k_):
        return (xh_ * 8 + z_) * 2 + k_

    loads = [
        pltpu.make_async_copy(occ, inb.at[pl.ds(0, 32)], in_sem.at[0]),
        pltpu.make_async_copy(vir, inb.at[pl.ds(32, 16)], in_sem.at[1]),
        pltpu.make_async_copy(docc, dov, in_sem.at[2]),
        pltpu.make_async_copy(dvir, dvv, in_sem.at[3]),
        pltpu.make_async_copy(ctab, ctv, in_sem.at[4]),
        pltpu.make_async_copy(btab, ntab, in_sem.at[5]),
    ]
    for load in loads:
        load.start()

    barrier = pltpu.get_barrier_semaphore()

    def greet_z(i, c):
        pl.semaphore_signal(barrier, inc=1, device_id=(row_of(xh, i, core), col), device_id_type=MESH)
        return c

    def greet_slab(i, c):
        pl.semaphore_signal(
            barrier, inc=1, device_id=(row_of(xh, z, lax.rem(i, 2)), lax.div(i, 2)), device_id_type=MESH
        )
        return c

    def greet_other(i, c):
        pl.semaphore_signal(
            barrier, inc=1, device_id=(row_of(1 - xh, z, lax.rem(i, 2)), lax.div(i, 2)), device_id_type=MESH
        )
        return c

    lax.fori_loop(0, 8, greet_z, 0)
    lax.fori_loop(0, 16, greet_slab, 0)
    lax.fori_loop(0, 16, greet_other, 0)

    for load in loads:
        load.wait()

    @pl.when(col == 0)
    def _():
        lane = lax.broadcasted_iota(jnp.int32, (32, 1024), 1)
        band = lax.broadcasted_iota(jnp.int32, (32, 1024), 0)
        dec = jnp.sum(jnp.where(lane == band + 32 * row, dov[...], 0.0), axis=1, keepdims=True)
        rs[0:32, :] = (inb[0:32, 0:1024].astype(F32) * dec).astype(BF16)
        lane = lax.broadcasted_iota(jnp.int32, (16, 512), 1)
        band = lax.broadcasted_iota(jnp.int32, (16, 512), 0)
        dec = jnp.sum(jnp.where(lane == band + 16 * row, dvv[...], 0.0), axis=1, keepdims=True)
        rs[32:48, :] = (inb[32:48, 0:1024].astype(F32) * dec).astype(BF16)

    pl.semaphore_wait(barrier, 40)

    def greet_ready(i, c):
        pl.semaphore_signal(
            ready, inc=1, device_id=(row_of(xh, z, lax.rem(i, 2)), lax.div(i, 2)), device_id_type=MESH
        )
        return c

    lax.fori_loop(0, 16, greet_ready, 0)

    def landed(ref, sem):
        pltpu.make_async_copy(ref, ref, sem).wait()

    def a_copy(i):
        s, kk, xt = lax.div(i, 4), lax.rem(lax.div(i, 2), 2), lax.rem(i, 2)
        lanes = pl.ds(pl.multiple_of(512 * s + 256 * kk + 128 * xt, 128), 128)
        b = 2 * xh + core
        return pltpu.make_async_remote_copy(
            src_ref=rs.at[:, lanes], dst_ref=rc.at[0, b, z], send_sem=ras, recv_sem=rar,
            device_id=(row_of(s, z, kk), xt * 4 + b), device_id_type=MESH,
        )

    def b_copy(dz):
        ref = rc.at[0, y, z]
        return pltpu.make_async_remote_copy(
            src_ref=ref, dst_ref=ref, send_sem=rbs, recv_sem=rbr.at[z],
            device_id=(row_of(xh, lax.rem(z + dz, 8), core), col), device_id_type=MESH,
        )

    def x_copy(zs):
        return pltpu.make_async_remote_copy(
            src_ref=rc.at[0, y, zs], dst_ref=rc.at[1, y, zs], send_sem=rxs, recv_sem=rxr.at[zs],
            device_id=(row, (1 - xl) * 4 + y), device_id_type=MESH,
        )

    def c_copy(o, zs, dy):
        ref = rc.at[o, y, zs]
        return pltpu.make_async_remote_copy(
            src_ref=ref, dst_ref=ref, send_sem=rcs, recv_sem=rcr.at[o],
            device_id=(row, xl * 4 + lax.rem(y + dy, 4)), device_id_type=MESH,
        )

    def near_y(o, zs):
        for dy in (1, 3, 2):
            c_copy(o, zs, dy).start()

    def lanes_of(p):
        return pl.ds(0, 512) if p is None else pl.ds(256 * p, 256)

    def p1_copy(dz, p=None):
        zt = lax.rem(z + dz, 8)
        start, size = (0, 512) if p is None else (256 * p, 256)
        lanes = pl.ds(pl.multiple_of(zt * 512 + start, 256), size)
        return pltpu.make_async_remote_copy(
            src_ref=inb.at[:, lanes], dst_ref=pz.at[z, :, lanes_of(p)], send_sem=p1s,
            recv_sem=p1r.at[z, p or 0], device_id=(row_of(xh, zt, core), col), device_id_type=MESH,
        )

    def p2_copy(src, zs, side, p=None):
        xt = lax.rem(x + 1 + 2 * side, 4)
        return pltpu.make_async_remote_copy(
            src_ref=src, dst_ref=pb.at[2 * xh + core, zs, :, lanes_of(p)], send_sem=p2s, recv_sem=p2r.at[zs, p or 0],
            device_id=(row_of(lax.div(xt, 2), z, core), lax.rem(xt, 2) * 4 + y), device_id_type=MESH,
        )

    def p3_copy(xs, zs, p=None):
        ref = pb.at[2 * xs + core, zs, :, lanes_of(p)]
        return pltpu.make_async_remote_copy(
            src_ref=ref, dst_ref=ref, send_sem=p3s, recv_sem=p3r,
            device_id=(row + 1 - 2 * core, col), device_id_type=MESH,
        )

    self_a = jnp.logical_and(col == 0, jnp.logical_and(xh == 0, core == 0))

    @pl.when(col == 0)
    def _():
        def send(i, carry):
            @pl.when(jnp.logical_or(i != 0, jnp.logical_not(self_a)))
            def _():
                a_copy(i).start()

            return carry

        lax.fori_loop(0, 8, send, 0)

    @pl.when(self_a)
    def _():
        rc[0, 0, z] = rs[:, 0:128]

    for dz in NEAR:
        p1_copy(dz).start()

    mine = pl.ds(pl.multiple_of(z * 512, 512), 512)
    for side in range(2):
        p2_copy(inb.at[:, mine], z, side).start()

    @pl.when(jnp.logical_not(self_a))
    def _():
        landed(rc.at[0, y, z], rar)

    for dz in DIST:
        b_copy(dz).start()
    near_y(0, z)
    x_copy(z).start()
    for p in range(2):
        for dz in FAR:
            p1_copy(dz, p).start()

    blane = lax.rem(lax.div(lax.broadcasted_iota(jnp.int32, (32, 1024), 1), 4), 16)
    ct = ctv[...]

    def table(b, c):
        rows = pl.ds(pl.multiple_of(b * 32, 32), 32)
        mtab[rows, :] = jnp.where(blane == b, ct, 0.0).astype(BF16)
        return c

    lax.fori_loop(0, 16, table, 0)

    def source(dz):
        return lax.rem(z + 8 - dz, 8)

    def relay(dz, p=None):
        zs = source(dz)
        ref = pz.at[zs, :, lanes_of(p)]
        landed(ref, p1r.at[zs, p or 0])
        p2_copy(ref, zs, 0, p).start()
        p2_copy(ref, zs, 1, p).start()

    def forward(dz, p=None):
        zs = source(dz)
        landed(pb.at[pl.ds(0, 2), zs, :, lanes_of(p)], p2r.at[zs, p or 0])
        p3_copy(0, zs, p).start()
        p3_copy(1, zs, p).start()

    def gathered_z(dz):
        zs = source(dz)
        landed(rc.at[0, y, zs], rbr.at[zs])
        near_y(0, zs)
        x_copy(zs).start()

    def gathered_x(dz):
        zs = source(dz)
        landed(rc.at[1, y, zs], rxr.at[zs])
        near_y(1, zs)

    def gathered_y(o):
        landed(rc.at[o, pl.ds(0, 3)], rcr.at[o])
        for b in range(4):
            rto[o, :, 256 * b : 256 * b + 256] = rc[o, b, :, 0:32, :].reshape(256, 128).T
            rtv[o, :, 128 * b : 128 * b + 128] = rc[o, b, :, 32:48, :].reshape(128, 128).T

    def g_copy(t, kk):
        o = jnp.abs(lax.div(t, 2) - xl)
        rows = pl.ds(pl.multiple_of(64 * lax.rem(t, 2) + 32 * kk, 32), 32)
        return pltpu.make_async_remote_copy(
            src_ref=gp.at[o, rows], dst_ref=pr.at[z], send_sem=gs, recv_sem=gr.at[z],
            device_id=(row_of(xh, 4 * core + t, kk), col), device_id_type=MESH,
        )

    def multiply(o):
        acc_o = jnp.zeros((128, 512), F32)
        acc_v = jnp.zeros((128, 512), F32)
        for b in range(4):
            acc_o += mdot(rto[o, :, 256 * b : 256 * b + 256], pb[b, :, 0:32, :].reshape(256, 512))
            acc_v += mdot(rtv[o, :, 128 * b : 128 * b + 128], pb[b, :, 32:48, :].reshape(128, 512))
        gp[o] = (acc_o * acc_v * SCALE).astype(BF16)

    for dz in NEAR:
        relay(dz)
    for dz in DIST:
        gathered_z(dz)
    for dz in FAR:
        relay(dz, 0)
    for dz in (0, *DIST):
        gathered_x(dz)
    for dz in FAR:
        relay(dz, 1)
    for dz in (0, *NEAR):
        forward(dz)
    for p in range(2):
        for dz in FAR:
            forward(dz, p)
    gathered_y(0)
    gathered_y(1)
    pl.semaphore_wait(ready, 16)
    landed(pb.at[pl.ds(0, 2)], p3r)
    multiply(0)
    multiply(1)

    own = lax.div(z, 4) == core
    place = lax.rem(z, 4)
    for j in range(4):
        inner = jnp.logical_or(place == 1, place == 2)

        def nearest(j):
            t = jnp.where(inner, 1 - j if j < 2 else j, j)
            return jnp.where(place >= 2, 3 - t, t)

        t = jnp.where(own, nearest(j), nearest(3 - j))
        for kk in range(2):
            mine = row == row_of(xh, 4 * core + t, kk)

            @pl.when(jnp.logical_not(mine))
            def _():
                g_copy(t, kk).start()

            @pl.when(mine)
            def _():
                o = jnp.abs(lax.div(t, 2) - xl)
                pr[z] = gp[o, pl.ds(pl.multiple_of(64 * lax.rem(t, 2) + 32 * kk, 32), 32)]

    slot = 8 * ((1 - xl) * 4 + y)

    def y_copy(q, c):
        lanes = pl.ds(pl.multiple_of(c * 128, 128), 128)
        return pltpu.make_async_remote_copy(
            src_ref=xs.at[pl.ds(2 * q, 2), :, lanes], dst_ref=xr.at[pl.ds(slot + 2 * q, 2)],
            send_sem=ys, recv_sem=yr.at[q], device_id=(row, c), device_id_type=MESH,
        )

    def pair(g):
        near = 3 - 2 * lax.rem(z, 2)
        return lax.rem(lax.div(z, 2) + (0, near, 4 - near, 2)[g], 4)

    for g in range(4):
        q = pair(g)
        for t in range(2):
            zs = 2 * q + t

            @pl.when(jnp.logical_or(zs != z, jnp.logical_not(own)))
            def _():
                landed(pr.at[zs], gr.at[zs])

        part = pr[pl.ds(2 * q, 2)].reshape(64, 512)
        xs[pl.ds(2 * q, 2)] = mdot(part, mtab[...]).astype(BF16).reshape(2, 32, 1024)

        def y_send(j, carry):
            y_copy(q, lax.rem(col + j, 8)).start()
            return carry

        lax.fori_loop(1, 8, y_send, 0)
        lanes = pl.ds(pl.multiple_of(col * 128, 128), 128)
        xr[pl.ds(slot + 2 * q, 2)] = xs[pl.ds(2 * q, 2), :, lanes]

    for g in range(4):
        q = pair(g)
        landed(xr.at[pl.ds(0, 14)], yr.at[q])
        parts = [xr[8 * c + 2 * q + t] for t in range(2) for c in range(8)]
        both = jnp.concatenate([jnp.concatenate(parts[8 * t : 8 * t + 8], axis=0) for t in range(2)], axis=1)
        res = mdot(both, ntab[...])
        for c in range(8):
            zb[4 * c + q] = res[32 * c : 32 * c + 32]

    @pl.when(jnp.logical_and(col == 0, jnp.logical_not(self_a)))
    def _():
        landed(rc.at[0, 0], ras)

    @pl.when(self_a)
    def _():
        landed(rc.at[0, 0, pl.ds(0, 7)], ras)

    landed(pz.at[pl.ds(0, 7)], p1s)
    landed(rc.at[0, 0, pl.ds(0, 7)], rbs)
    landed(rc.at[0, 0], rxs)
    landed(pb.at[pl.ds(0, 2)], p2s)
    landed(pb.at[pl.ds(0, 2)], p3s)
    landed(rc.at[0, pl.ds(0, 3)], rcs)
    landed(rc.at[1, pl.ds(0, 3)], rcs)

    landed(xr.at[pl.ds(0, 56)], ys)

    @pl.when(own)
    def _():
        landed(pr.at[pl.ds(0, 7)], gs)

    @pl.when(jnp.logical_not(own))
    def _():
        landed(pr, gs)


def finish(zb, out_re, out_im, res_re, res_im, sem):
    lane = lax.broadcasted_iota(jnp.int32, (8, 128), 1)

    def put(i, which):
        res, out = ((res_re, out_re), (res_im, out_im))[which]
        rows = pl.ds(pl.multiple_of(256 * i, 256), 256)
        return pltpu.make_async_copy(res.at[rows], out.at[rows], sem.at[which, i])

    def a_step(i, carry):
        rows = pl.ds(pl.multiple_of(8 * i, 8), 8)
        res = fft([(zb[a, rows, 0:128], zb[a, rows, 128:256]) for a in range(32)])
        for j in range(8):
            for part, out in ((0, res_re), (1, res_im)):
                moved = swap_groups([res[4 * j + t][part] for t in range(4)], lane)
                for kc in range(4):
                    out[pl.ds(i * 256 + j * 4 + kc, 8, stride=32), :] = moved[kc]
        put(i, 0).start()
        put(i, 1).start()
        return carry

    lax.fori_loop(0, 4, a_step, 0)
    for i in range(4):
        put(i, 0).wait()
        put(i, 1).wait()


def on_device(occ, vir, docc, dvir):
    anyspace = pl.BlockSpec(memory_space=pl.ANY)
    vmem = pl.BlockSpec(memory_space=pltpu.VMEM)
    dma = pltpu.SemaphoreType.DMA
    zb = pl.pallas_call(
        kernel,
        out_shape=pltpu.VMEM((32, 32, 256), F32),
        in_specs=[anyspace] * 6,
        out_specs=vmem,
        scratch_shapes=[
            pltpu.VMEM((48, 4096), BF16),
            pltpu.VMEM((1, 1024), F32),
            pltpu.VMEM((1, 512), F32),
            pltpu.VMEM((32, 1024), F32),
            pltpu.VMEM((512, 1024), BF16),
            pltpu.VMEM((256, 256), BF16),
            pltpu.VMEM((8, 48, 512), BF16),
            pltpu.VMEM((4, 8, 48, 512), BF16),
            pltpu.VMEM((48, 1024), BF16),
            pltpu.VMEM((2, 4, 8, 48, 128), BF16),
            pltpu.VMEM((2, 128, 1024), BF16),
            pltpu.VMEM((2, 128, 512), BF16),
            pltpu.VMEM((2, 128, 512), BF16),
            pltpu.VMEM((8, 32, 512), BF16),
            pltpu.VMEM((8, 32, 1024), BF16),
            pltpu.VMEM((64, 32, 128), BF16),
            dma((6,)),
            dma, dma((8, 2)),
            dma, dma((8, 2)),
            dma, dma,
            dma, dma,
            dma, dma((8,)),
            dma, dma((8,)),
            dma, dma((2,)),
            dma, dma((8,)),
            dma, dma((4,)),
            pltpu.SemaphoreType.REGULAR,
        ],
        compiler_params=pltpu.CompilerParams(collective_id=0, has_side_effects=True),
    )(
        occ, vir, docc.reshape(1, 1024), dvir.reshape(1, 512),
        jnp.asarray(c_table()), jnp.asarray(b_table()).astype(BF16),
    )
    out = jax.ShapeDtypeStruct((1024, 128), F32)
    res = pl.pallas_call(
        finish,
        out_shape=(out, out),
        in_specs=[vmem],
        out_specs=(anyspace, anyspace),
        scratch_shapes=[
            pltpu.VMEM((1024, 128), F32),
            pltpu.VMEM((1024, 128), F32),
            dma((2, 4)),
        ],
    )(pltpu.with_memory_space_constraint(zb, pltpu.VMEM))

    def placed(part):
        return jnp.transpose(part.reshape(32, 8, 4, 128), (0, 2, 1, 3)).reshape(32, 4, 1024)

    return placed(res[0]), placed(res[1])


def solution(mesh):
    in_specs = (P("row", "col"), P("row", "col"), P(), P())
    out_specs = (P("row", "col", None), P("row", "col", None))
    return jax.shard_map(
        on_device, mesh=mesh, in_specs=in_specs, out_specs=out_specs, check_vma=False
    )
```

```python
import functools
import math

import jax
import jax.numpy as jnp
import numpy as np
from jax import lax
from jax.experimental import pallas as pl
from jax.experimental.pallas import tpu as pltpu
from jax.sharding import PartitionSpec as P

MESH = pl.DeviceIdType.MESH
F32 = jnp.float32
BF16 = jnp.bfloat16
SCALE = -(2.0**-17)
NEAR, FAR = (1, 7, 2, 6), (3, 5, 4)
DIST = NEAR + FAR


def angle_table(length):
    k = np.arange(length)
    phase = np.outer(k, k) % length
    angle = 2.0 * np.pi * phase / length
    return np.cos(angle), np.sin(angle)


def c_table():
    cos, sin = angle_table(32)
    cos, sin = cos.reshape(32, 8, 1, 4), -sin.reshape(32, 8, 1, 4)
    both = np.stack([cos, sin], axis=2)
    return np.broadcast_to(both, (32, 8, 2, 16, 4)).reshape(32, 1024).astype(np.float32)


def b_table():
    cos, sin = angle_table(32)
    table = np.zeros((2, 2, 16, 4, 2, 4, 32), np.float32)
    for kc in range(4):
        c = cos.reshape(2, 16, 32)
        s = sin.reshape(2, 16, 32)
        table[:, 0, :, kc, 0, kc, :] = c
        table[:, 0, :, kc, 1, kc, :] = -s
        table[:, 1, :, kc, 0, kc, :] = s
        table[:, 1, :, kc, 1, kc, :] = c
    return table.reshape(256, 256)


def fft(parts):
    n = len(parts)
    if n == 1:
        return parts
    half = n // 2
    even, odd = fft(parts[0::2]), fft(parts[1::2])
    low, high = [], []
    for k in range(half):
        (ar, ai), (br, bi) = even[k], odd[k]
        if k == 0:
            tr, ti = br, bi
        elif 4 * k == n:
            tr, ti = bi, -br
        else:
            c, s = math.cos(2 * math.pi * k / n), math.sin(2 * math.pi * k / n)
            tr, ti = c * br + s * bi, c * bi - s * br
        low.append((ar + tr, ai + ti))
        high.append((ar - tr, ai - ti))
    return low + high


def swap_groups(v, lane):
    v = list(v)
    for shift, pairs in ((64, ((0, 2), (1, 3))), (32, ((0, 1), (2, 3)))):
        low = lax.rem(lane, 2 * shift) < shift
        for i, j in pairs:
            a, b = v[i], v[j]
            v[i] = jnp.where(low, a, pltpu.roll(b, shift, 1))
            v[j] = jnp.where(low, pltpu.roll(a, 128 - shift, 1), b)
    return v


def tdot(a, b):
    return lax.dot_general(a, b, (((0,), (0,)), ((), ())), preferred_element_type=F32)


def mdot(a, b):
    return jnp.dot(a, b, preferred_element_type=F32)


def kernel(
    occ, vir, docc, dvir, ctab, btab, zb,
    inb, dov, dvv, ctv, mtab, ntab,
    pz, pb, rs, rc, rto, rtv, gp, pr, xs, xr,
    in_sem, p1s, p1r, p2s, p2r, p3s, p3r, ras, rar, rbs, rbr, rxs, rxr, rcs, rcr, gs, gr, ys, yr, ready,
):
    row, col = lax.axis_index("row"), lax.axis_index("col")
    core = lax.rem(row, 2)
    z = lax.rem(lax.div(row, 2), 8)
    xh = lax.div(row, 16)
    y, xl = lax.rem(col, 4), lax.div(col, 4)
    x = 2 * xh + xl

    def row_of(xh_, z_, k_):
        return (xh_ * 8 + z_) * 2 + k_

    loads = [
        pltpu.make_async_copy(occ, inb.at[pl.ds(0, 32)], in_sem.at[0]),
        pltpu.make_async_copy(vir, inb.at[pl.ds(32, 16)], in_sem.at[1]),
        pltpu.make_async_copy(docc, dov, in_sem.at[2]),
        pltpu.make_async_copy(dvir, dvv, in_sem.at[3]),
        pltpu.make_async_copy(ctab, ctv, in_sem.at[4]),
        pltpu.make_async_copy(btab, ntab, in_sem.at[5]),
    ]
    for load in loads:
        load.start()

    barrier = pltpu.get_barrier_semaphore()

    def greet_z(i, c):
        pl.semaphore_signal(barrier, inc=1, device_id=(row_of(xh, i, core), col), device_id_type=MESH)
        return c

    def greet_slab(i, c):
        pl.semaphore_signal(
            barrier, inc=1, device_id=(row_of(xh, z, lax.rem(i, 2)), lax.div(i, 2)), device_id_type=MESH
        )
        return c

    def greet_other(i, c):
        pl.semaphore_signal(
            barrier, inc=1, device_id=(row_of(1 - xh, z, lax.rem(i, 2)), lax.div(i, 2)), device_id_type=MESH
        )
        return c

    lax.fori_loop(0, 8, greet_z, 0)
    lax.fori_loop(0, 16, greet_slab, 0)
    lax.fori_loop(0, 16, greet_other, 0)

    for load in loads:
        load.wait()

    @pl.when(col == 0)
    def _():
        lane = lax.broadcasted_iota(jnp.int32, (32, 1024), 1)
        band = lax.broadcasted_iota(jnp.int32, (32, 1024), 0)
        dec = jnp.sum(jnp.where(lane == band + 32 * row, dov[...], 0.0), axis=1, keepdims=True)
        rs[0:32, :] = (inb[0:32, 0:1024].astype(F32) * dec).astype(BF16)
        lane = lax.broadcasted_iota(jnp.int32, (16, 512), 1)
        band = lax.broadcasted_iota(jnp.int32, (16, 512), 0)
        dec = jnp.sum(jnp.where(lane == band + 16 * row, dvv[...], 0.0), axis=1, keepdims=True)
        rs[32:48, :] = (inb[32:48, 0:1024].astype(F32) * dec).astype(BF16)

    pl.semaphore_wait(barrier, 40)

    def greet_ready(i, c):
        pl.semaphore_signal(
            ready, inc=1, device_id=(row_of(xh, z, lax.rem(i, 2)), lax.div(i, 2)), device_id_type=MESH
        )
        return c

    lax.fori_loop(0, 16, greet_ready, 0)

    def landed(ref, sem):
        pltpu.make_async_copy(ref, ref, sem).wait()

    def a_copy(i):
        s, kk, xt = lax.div(i, 4), lax.rem(lax.div(i, 2), 2), lax.rem(i, 2)
        lanes = pl.ds(pl.multiple_of(512 * s + 256 * kk + 128 * xt, 128), 128)
        b = 2 * xh + core
        return pltpu.make_async_remote_copy(
            src_ref=rs.at[:, lanes], dst_ref=rc.at[0, b, z], send_sem=ras, recv_sem=rar,
            device_id=(row_of(s, z, kk), xt * 4 + b), device_id_type=MESH,
        )

    def b_copy(dz):
        ref = rc.at[0, y, z]
        return pltpu.make_async_remote_copy(
            src_ref=ref, dst_ref=ref, send_sem=rbs, recv_sem=rbr.at[z],
            device_id=(row_of(xh, lax.rem(z + dz, 8), core), col), device_id_type=MESH,
        )

    def x_copy(zs):
        return pltpu.make_async_remote_copy(
            src_ref=rc.at[0, y, zs], dst_ref=rc.at[1, y, zs], send_sem=rxs, recv_sem=rxr.at[zs],
            device_id=(row, (1 - xl) * 4 + y), device_id_type=MESH,
        )

    def c_copy(o, zs, dy):
        ref = rc.at[o, y, zs]
        return pltpu.make_async_remote_copy(
            src_ref=ref, dst_ref=ref, send_sem=rcs, recv_sem=rcr.at[o],
            device_id=(row, xl * 4 + lax.rem(y + dy, 4)), device_id_type=MESH,
        )

    def near_y(o, zs):
        for dy in (1, 3, 2):
            c_copy(o, zs, dy).start()

    def p1_copy(p, dz):
        zt = lax.rem(z + dz, 8)
        return pltpu.make_async_remote_copy(
            src_ref=inb.at[:, part_of(zt, p)], dst_ref=pz.at[p, z], send_sem=p1s, recv_sem=p1r.at[p, z],
            device_id=(row_of(xh, zt, core), col), device_id_type=MESH,
        )

    def part_of(zs, p):
        return pl.ds(pl.multiple_of(zs * 512 + p * 256, 256), 256)

    def p2_copy(src, p, zs, side):
        xt = lax.rem(x + 1 + 2 * side, 4)
        return pltpu.make_async_remote_copy(
            src_ref=src, dst_ref=pb.at[p, 2 * xh + core, zs], send_sem=p2s, recv_sem=p2r.at[p, zs],
            device_id=(row_of(lax.div(xt, 2), z, core), lax.rem(xt, 2) * 4 + y), device_id_type=MESH,
        )

    def p3_copy(p, xs, zs):
        ref = pb.at[p, 2 * xs + core, zs]
        return pltpu.make_async_remote_copy(
            src_ref=ref, dst_ref=ref, send_sem=p3s, recv_sem=p3r.at[p],
            device_id=(row + 1 - 2 * core, col), device_id_type=MESH,
        )

    self_a = jnp.logical_and(col == 0, jnp.logical_and(xh == 0, core == 0))

    @pl.when(col == 0)
    def _():
        def send(i, carry):
            @pl.when(jnp.logical_or(i != 0, jnp.logical_not(self_a)))
            def _():
                a_copy(i).start()

            return carry

        lax.fori_loop(0, 8, send, 0)

    @pl.when(self_a)
    def _():
        rc[0, 0, z] = rs[:, 0:128]

    for dz in DIST:
        p1_copy(0, dz).start()
    for p in range(2):
        for side in range(2):
            p2_copy(inb.at[:, part_of(z, p)], p, z, side).start()

    @pl.when(jnp.logical_not(self_a))
    def _():
        landed(rc.at[0, y, z], rar)

    for dz in DIST:
        b_copy(dz).start()
    near_y(0, z)
    x_copy(z).start()
    for dz in DIST:
        p1_copy(1, dz).start()

    blane = lax.rem(lax.div(lax.broadcasted_iota(jnp.int32, (32, 1024), 1), 4), 16)
    ct = ctv[...]

    def table(b, c):
        rows = pl.ds(pl.multiple_of(b * 32, 32), 32)
        mtab[rows, :] = jnp.where(blane == b, ct, 0.0).astype(BF16)
        return c

    lax.fori_loop(0, 16, table, 0)

    def source(dz):
        return lax.rem(z + 8 - dz, 8)

    def relay(p, dz):
        zs = source(dz)
        landed(pz.at[p, zs], p1r.at[p, zs])
        p2_copy(pz.at[p, zs], p, zs, 0).start()
        p2_copy(pz.at[p, zs], p, zs, 1).start()

    def forward(p, dz):
        zs = source(dz)
        landed(pb.at[p, pl.ds(0, 2), zs], p2r.at[p, zs])
        p3_copy(p, 0, zs).start()
        p3_copy(p, 1, zs).start()

    def gathered_z(dz):
        zs = source(dz)
        landed(rc.at[0, y, zs], rbr.at[zs])
        near_y(0, zs)
        x_copy(zs).start()

    def gathered_x(dz):
        zs = source(dz)
        landed(rc.at[1, y, zs], rxr.at[zs])
        near_y(1, zs)

    def gathered_y(o):
        landed(rc.at[o, pl.ds(0, 3)], rcr.at[o])
        for b in range(4):
            rto[128 * o : 128 * o + 128, 256 * b : 256 * b + 256] = rc[o, b, :, 0:32, :].reshape(256, 128).T
            rtv[128 * o : 128 * o + 128, 128 * b : 128 * b + 128] = rc[o, b, :, 32:48, :].reshape(128, 128).T

    def g_rows(t, kk):
        o = jnp.abs(lax.div(t, 2) - xl)
        return pl.ds(pl.multiple_of(128 * o + 64 * lax.rem(t, 2) + 32 * kk, 32), 32)

    def g_copy(p, t, kk):
        return pltpu.make_async_remote_copy(
            src_ref=gp.at[p, g_rows(t, kk)], dst_ref=pr.at[p, z], send_sem=gs, recv_sem=gr.at[z],
            device_id=(row_of(xh, 4 * core + t, kk), col), device_id_type=MESH,
        )

    own = lax.div(z, 4) == core
    place = lax.rem(z, 4)
    inner = jnp.logical_or(place == 1, place == 2)

    def nearest(j):
        t = jnp.where(inner, 1 - j if j < 2 else j, j)
        return jnp.where(place >= 2, 3 - t, t)

    def multiply(p):
        acc_o = jnp.zeros((256, 256), F32)
        acc_v = jnp.zeros((256, 256), F32)
        for b in range(4):
            left = rto[:, 256 * b : 256 * b + 256]
            acc_o += mdot(left, pb[p, b, :, 0:32, :].reshape(256, 256))
            left = rtv[:, 128 * b : 128 * b + 128]
            acc_v += mdot(left, pb[p, b, :, 32:48, :].reshape(128, 256))
        gp[p] = (acc_o * acc_v * SCALE).astype(BF16)
        for j in range(4):
            t = jnp.where(own, nearest(j), nearest(3 - j))
            for kk in range(2):
                mine = row == row_of(xh, 4 * core + t, kk)

                @pl.when(jnp.logical_not(mine))
                def _():
                    g_copy(p, t, kk).start()

                @pl.when(mine)
                def _():
                    pr[p, z] = gp[p, g_rows(t, kk)]

    for dz in NEAR:
        relay(0, dz)
    for dz in DIST:
        gathered_z(dz)
    for dz in FAR:
        relay(0, dz)
    for dz in (0, *DIST):
        gathered_x(dz)
    for dz in (0, *NEAR):
        forward(0, dz)
    for dz in NEAR:
        relay(1, dz)
    for dz in FAR:
        forward(0, dz)
    for dz in FAR:
        relay(1, dz)
    gathered_y(0)
    gathered_y(1)
    pl.semaphore_wait(ready, 16)
    landed(pb.at[0, pl.ds(0, 2)], p3r.at[0])
    multiply(0)
    for dz in (0, *DIST):
        forward(1, dz)
    landed(pb.at[1, pl.ds(0, 2)], p3r.at[1])
    multiply(1)

    slot = 8 * ((1 - xl) * 4 + y)

    def y_copy(q, c):
        lanes = pl.ds(pl.multiple_of(c * 128, 128), 128)
        return pltpu.make_async_remote_copy(
            src_ref=xs.at[pl.ds(2 * q, 2), :, lanes], dst_ref=xr.at[pl.ds(slot + 2 * q, 2)],
            send_sem=ys, recv_sem=yr.at[q], device_id=(row, c), device_id_type=MESH,
        )

    def pair(g):
        near = 3 - 2 * lax.rem(z, 2)
        return lax.rem(lax.div(z, 2) + (0, near, 4 - near, 2)[g], 4)

    for g in range(4):
        q = pair(g)
        for t in range(2):
            zs = 2 * q + t

            @pl.when(jnp.logical_or(zs != z, jnp.logical_not(own)))
            def _():
                landed(pr.at[:, zs], gr.at[zs])

        part = jnp.concatenate([pr[p, pl.ds(2 * q, 2)].reshape(64, 256) for p in range(2)], axis=1)
        xs[pl.ds(2 * q, 2)] = mdot(part, mtab[...]).astype(BF16).reshape(2, 32, 1024)

        def y_send(j, carry):
            y_copy(q, lax.rem(col + j, 8)).start()
            return carry

        lax.fori_loop(1, 8, y_send, 0)
        lanes = pl.ds(pl.multiple_of(col * 128, 128), 128)
        xr[pl.ds(slot + 2 * q, 2)] = xs[pl.ds(2 * q, 2), :, lanes]

    for g in range(4):
        q = pair(g)
        landed(xr.at[pl.ds(0, 14)], yr.at[q])
        parts = [xr[8 * c + 2 * q + t] for t in range(2) for c in range(8)]
        both = jnp.concatenate([jnp.concatenate(parts[8 * t : 8 * t + 8], axis=0) for t in range(2)], axis=1)
        res = mdot(both, ntab[...])
        for c in range(8):
            zb[4 * c + q] = res[32 * c : 32 * c + 32]

    @pl.when(jnp.logical_and(col == 0, jnp.logical_not(self_a)))
    def _():
        landed(rc.at[0, 0], ras)

    @pl.when(self_a)
    def _():
        landed(rc.at[0, 0, pl.ds(0, 7)], ras)

    for p in range(2):
        landed(pz.at[p, pl.ds(0, 7)], p1s)
        landed(pb.at[p, pl.ds(0, 2)], p2s)
        landed(pb.at[p, pl.ds(0, 2)], p3s)
    landed(rc.at[0, 0, pl.ds(0, 7)], rbs)
    landed(rc.at[0, 0], rxs)
    landed(rc.at[0, pl.ds(0, 3)], rcs)
    landed(rc.at[1, pl.ds(0, 3)], rcs)

    landed(xr.at[pl.ds(0, 56)], ys)

    @pl.when(own)
    def _():
        landed(pr.at[:, pl.ds(0, 7)], gs)

    @pl.when(jnp.logical_not(own))
    def _():
        landed(pr, gs)


def finish(zb, out_re, out_im, res_re, res_im, sem):
    lane = lax.broadcasted_iota(jnp.int32, (8, 128), 1)

    def put(i, which):
        res, out = ((res_re, out_re), (res_im, out_im))[which]
        rows = pl.ds(pl.multiple_of(256 * i, 256), 256)
        return pltpu.make_async_copy(res.at[rows], out.at[rows], sem.at[which, i])

    def a_step(i, carry):
        rows = pl.ds(pl.multiple_of(8 * i, 8), 8)
        res = fft([(zb[a, rows, 0:128], zb[a, rows, 128:256]) for a in range(32)])
        for j in range(8):
            for part, out in ((0, res_re), (1, res_im)):
                moved = swap_groups([res[4 * j + t][part] for t in range(4)], lane)
                for kc in range(4):
                    out[pl.ds(i * 256 + j * 4 + kc, 8, stride=32), :] = moved[kc]
        put(i, 0).start()
        put(i, 1).start()
        return carry

    lax.fori_loop(0, 4, a_step, 0)
    for i in range(4):
        put(i, 0).wait()
        put(i, 1).wait()


def on_device(occ, vir, docc, dvir):
    anyspace = pl.BlockSpec(memory_space=pl.ANY)
    vmem = pl.BlockSpec(memory_space=pltpu.VMEM)
    dma = pltpu.SemaphoreType.DMA
    zb = pl.pallas_call(
        kernel,
        out_shape=pltpu.VMEM((32, 32, 256), F32),
        in_specs=[anyspace] * 6,
        out_specs=vmem,
        scratch_shapes=[
            pltpu.VMEM((48, 4096), BF16),
            pltpu.VMEM((1, 1024), F32),
            pltpu.VMEM((1, 512), F32),
            pltpu.VMEM((32, 1024), F32),
            pltpu.VMEM((512, 1024), BF16),
            pltpu.VMEM((256, 256), BF16),
            pltpu.VMEM((2, 8, 48, 256), BF16),
            pltpu.VMEM((2, 4, 8, 48, 256), BF16),
            pltpu.VMEM((48, 1024), BF16),
            pltpu.VMEM((2, 4, 8, 48, 128), BF16),
            pltpu.VMEM((256, 1024), BF16),
            pltpu.VMEM((256, 512), BF16),
            pltpu.VMEM((2, 256, 256), BF16),
            pltpu.VMEM((2, 8, 32, 256), BF16),
            pltpu.VMEM((8, 32, 1024), BF16),
            pltpu.VMEM((64, 32, 128), BF16),
            dma((6,)),
            dma, dma((2, 8)),
            dma, dma((2, 8)),
            dma, dma((2,)),
            dma, dma,
            dma, dma((8,)),
            dma, dma((8,)),
            dma, dma((2,)),
            dma, dma((8,)),
            dma, dma((4,)),
            pltpu.SemaphoreType.REGULAR,
        ],
        compiler_params=pltpu.CompilerParams(collective_id=0, has_side_effects=True),
    )(
        occ, vir, docc.reshape(1, 1024), dvir.reshape(1, 512),
        jnp.asarray(c_table()), jnp.asarray(b_table()).astype(BF16),
    )
    out = jax.ShapeDtypeStruct((1024, 128), F32)
    res = pl.pallas_call(
        finish,
        out_shape=(out, out),
        in_specs=[vmem],
        out_specs=(anyspace, anyspace),
        scratch_shapes=[
            pltpu.VMEM((1024, 128), F32),
            pltpu.VMEM((1024, 128), F32),
            dma((2, 4)),
        ],
    )(pltpu.with_memory_space_constraint(zb, pltpu.VMEM))

    def placed(part):
        return jnp.transpose(part.reshape(32, 8, 4, 128), (0, 2, 1, 3)).reshape(32, 4, 1024)

    return placed(res[0]), placed(res[1])


def solution(mesh):
    in_specs = (P("row", "col"), P("row", "col"), P(), P())
    out_specs = (P("row", "col", None), P("row", "col", None))
    return jax.shard_map(
        on_device, mesh=mesh, in_specs=in_specs, out_specs=out_specs, check_vma=False
    )
```

```python
import functools
import math

import jax
import jax.numpy as jnp
import numpy as np
from jax import lax
from jax.experimental import pallas as pl
from jax.experimental.pallas import tpu as pltpu
from jax.sharding import PartitionSpec as P

MESH = pl.DeviceIdType.MESH
F32 = jnp.float32
BF16 = jnp.bfloat16
SCALE = -(2.0**-17)
NEAR, FAR = (1, 7, 2, 6), (3, 5, 4)
DIST = NEAR + FAR


def angle_table(length):
    k = np.arange(length)
    phase = np.outer(k, k) % length
    angle = 2.0 * np.pi * phase / length
    return np.cos(angle), np.sin(angle)


def c_table():
    cos, sin = angle_table(32)
    cos, sin = cos.reshape(32, 8, 1, 4), -sin.reshape(32, 8, 1, 4)
    both = np.stack([cos, sin], axis=2)
    return np.broadcast_to(both, (32, 8, 2, 16, 4)).reshape(32, 1024).astype(np.float32)


def b_table():
    cos, sin = angle_table(32)
    c, s = cos.reshape(2, 2, 8, 32).swapaxes(0, 1), sin.reshape(2, 2, 8, 32).swapaxes(0, 1)
    table = np.zeros((2, 2, 2, 2, 8, 4, 2, 2, 4, 32), np.float32)
    for kc in range(4):
        for h in range(2):
            table[:, :, 0, h, :, kc, h, 0, kc, :] = c
            table[:, :, 0, h, :, kc, h, 1, kc, :] = -s
            table[:, :, 1, h, :, kc, h, 0, kc, :] = s
            table[:, :, 1, h, :, kc, h, 1, kc, :] = c
    return table.reshape(2, 256, 512)


def fft(parts):
    n = len(parts)
    if n == 1:
        return parts
    half = n // 2
    even, odd = fft(parts[0::2]), fft(parts[1::2])
    low, high = [], []
    for k in range(half):
        (ar, ai), (br, bi) = even[k], odd[k]
        if k == 0:
            tr, ti = br, bi
        elif 4 * k == n:
            tr, ti = bi, -br
        else:
            c, s = math.cos(2 * math.pi * k / n), math.sin(2 * math.pi * k / n)
            tr, ti = c * br + s * bi, c * bi - s * br
        low.append((ar + tr, ai + ti))
        high.append((ar - tr, ai - ti))
    return low + high


def swap_groups(v, lane):
    v = list(v)
    for shift, pairs in ((64, ((0, 2), (1, 3))), (32, ((0, 1), (2, 3)))):
        low = lax.rem(lane, 2 * shift) < shift
        for i, j in pairs:
            a, b = v[i], v[j]
            v[i] = jnp.where(low, a, pltpu.roll(b, shift, 1))
            v[j] = jnp.where(low, pltpu.roll(a, 128 - shift, 1), b)
    return v


def tdot(a, b):
    return lax.dot_general(a, b, (((0,), (0,)), ((), ())), preferred_element_type=F32)


def mdot(a, b):
    return jnp.dot(a, b, preferred_element_type=F32)


def kernel(
    occ, vir, docc, dvir, ctab, btab, zb,
    inb, dov, dvv, ctv, mtab, ntab,
    pz, pb, rs, rc, rto, rtv, gp, pr, xs, xr,
    in_sem, p1s, p1r, p2s, p2r, p3s, p3r, ras, rar, rbs, rbr, rxs, rxr, rcs, rcr, gs, gr, ys, yr, ready,
):
    row, col = lax.axis_index("row"), lax.axis_index("col")
    core = lax.rem(row, 2)
    z = lax.rem(lax.div(row, 2), 8)
    xh = lax.div(row, 16)
    y, xl = lax.rem(col, 4), lax.div(col, 4)
    x = 2 * xh + xl

    def row_of(xh_, z_, k_):
        return (xh_ * 8 + z_) * 2 + k_

    loads = [
        pltpu.make_async_copy(occ, inb.at[pl.ds(0, 32)], in_sem.at[0]),
        pltpu.make_async_copy(vir, inb.at[pl.ds(32, 16)], in_sem.at[1]),
        pltpu.make_async_copy(docc, dov, in_sem.at[2]),
        pltpu.make_async_copy(dvir, dvv, in_sem.at[3]),
        pltpu.make_async_copy(ctab, ctv, in_sem.at[4]),
        pltpu.make_async_copy(btab, ntab, in_sem.at[5]),
    ]
    for load in loads:
        load.start()

    barrier = pltpu.get_barrier_semaphore()

    def greet_z(i, c):
        pl.semaphore_signal(barrier, inc=1, device_id=(row_of(xh, i, core), col), device_id_type=MESH)
        return c

    def greet_slab(i, c):
        pl.semaphore_signal(
            barrier, inc=1, device_id=(row_of(xh, z, lax.rem(i, 2)), lax.div(i, 2)), device_id_type=MESH
        )
        return c

    def greet_other(i, c):
        pl.semaphore_signal(
            barrier, inc=1, device_id=(row_of(1 - xh, z, lax.rem(i, 2)), lax.div(i, 2)), device_id_type=MESH
        )
        return c

    lax.fori_loop(0, 8, greet_z, 0)
    lax.fori_loop(0, 16, greet_slab, 0)
    lax.fori_loop(0, 16, greet_other, 0)

    for load in loads:
        load.wait()

    @pl.when(col == 0)
    def _():
        lane = lax.broadcasted_iota(jnp.int32, (32, 1024), 1)
        band = lax.broadcasted_iota(jnp.int32, (32, 1024), 0)
        dec = jnp.sum(jnp.where(lane == band + 32 * row, dov[...], 0.0), axis=1, keepdims=True)
        rs[0:32, :] = (inb[0:32, 0:1024].astype(F32) * dec).astype(BF16)
        lane = lax.broadcasted_iota(jnp.int32, (16, 512), 1)
        band = lax.broadcasted_iota(jnp.int32, (16, 512), 0)
        dec = jnp.sum(jnp.where(lane == band + 16 * row, dvv[...], 0.0), axis=1, keepdims=True)
        rs[32:48, :] = (inb[32:48, 0:1024].astype(F32) * dec).astype(BF16)

    pl.semaphore_wait(barrier, 40)

    def greet_ready(i, c):
        pl.semaphore_signal(
            ready, inc=1, device_id=(row_of(xh, z, lax.rem(i, 2)), lax.div(i, 2)), device_id_type=MESH
        )
        return c

    lax.fori_loop(0, 16, greet_ready, 0)

    def landed(ref, sem):
        pltpu.make_async_copy(ref, ref, sem).wait()

    def a_copy(i):
        s, kk, xt = lax.div(i, 4), lax.rem(lax.div(i, 2), 2), lax.rem(i, 2)
        lanes = pl.ds(pl.multiple_of(512 * s + 256 * kk + 128 * xt, 128), 128)
        b = 2 * xh + core
        return pltpu.make_async_remote_copy(
            src_ref=rs.at[:, lanes], dst_ref=rc.at[0, b, z], send_sem=ras, recv_sem=rar,
            device_id=(row_of(s, z, kk), xt * 4 + b), device_id_type=MESH,
        )

    def b_copy(dz):
        ref = rc.at[0, y, z]
        return pltpu.make_async_remote_copy(
            src_ref=ref, dst_ref=ref, send_sem=rbs, recv_sem=rbr.at[z],
            device_id=(row_of(xh, lax.rem(z + dz, 8), core), col), device_id_type=MESH,
        )

    def x_copy(zs):
        return pltpu.make_async_remote_copy(
            src_ref=rc.at[0, y, zs], dst_ref=rc.at[1, y, zs], send_sem=rxs, recv_sem=rxr.at[zs],
            device_id=(row, (1 - xl) * 4 + y), device_id_type=MESH,
        )

    def c_copy(o, zs, dy):
        ref = rc.at[o, y, zs]
        return pltpu.make_async_remote_copy(
            src_ref=ref, dst_ref=ref, send_sem=rcs, recv_sem=rcr.at[o],
            device_id=(row, xl * 4 + lax.rem(y + dy, 4)), device_id_type=MESH,
        )

    def near_y(o, zs):
        for dy in (1, 3, 2):
            c_copy(o, zs, dy).start()

    def p1_copy(p, dz):
        zt = lax.rem(z + dz, 8)
        return pltpu.make_async_remote_copy(
            src_ref=inb.at[:, part_of(zt, p)], dst_ref=pz.at[p, z], send_sem=p1s, recv_sem=p1r.at[p, z],
            device_id=(row_of(xh, zt, core), col), device_id_type=MESH,
        )

    def part_of(zs, p):
        return pl.ds(pl.multiple_of(zs * 512 + p * 256, 256), 256)

    def p2_copy(src, p, zs, side):
        xt = lax.rem(x + 1 + 2 * side, 4)
        return pltpu.make_async_remote_copy(
            src_ref=src, dst_ref=pb.at[p, 2 * xh + core, zs], send_sem=p2s, recv_sem=p2r.at[p, zs],
            device_id=(row_of(lax.div(xt, 2), z, core), lax.rem(xt, 2) * 4 + y), device_id_type=MESH,
        )

    def p3_copy(p, xs, zs):
        ref = pb.at[p, 2 * xs + core, zs]
        return pltpu.make_async_remote_copy(
            src_ref=ref, dst_ref=ref, send_sem=p3s, recv_sem=p3r.at[p],
            device_id=(row + 1 - 2 * core, col), device_id_type=MESH,
        )

    self_a = jnp.logical_and(col == 0, jnp.logical_and(xh == 0, core == 0))

    @pl.when(col == 0)
    def _():
        def send(i, carry):
            @pl.when(jnp.logical_or(i != 0, jnp.logical_not(self_a)))
            def _():
                a_copy(i).start()

            return carry

        lax.fori_loop(0, 8, send, 0)

    @pl.when(self_a)
    def _():
        rc[0, 0, z] = rs[:, 0:128]

    for dz in DIST:
        p1_copy(0, dz).start()
    for p in range(2):
        for side in range(2):
            p2_copy(inb.at[:, part_of(z, p)], p, z, side).start()

    @pl.when(jnp.logical_not(self_a))
    def _():
        landed(rc.at[0, y, z], rar)

    for dz in DIST:
        b_copy(dz).start()
    near_y(0, z)
    x_copy(z).start()
    for dz in DIST:
        p1_copy(1, dz).start()

    blane = lax.rem(lax.div(lax.broadcasted_iota(jnp.int32, (32, 1024), 1), 4), 16)
    ct = ctv[...]

    def table(b, c):
        rows = pl.ds(pl.multiple_of(b * 32, 32), 32)
        mtab[rows, :] = jnp.where(blane == b, ct, 0.0).astype(BF16)
        return c

    lax.fori_loop(0, 16, table, 0)

    def source(dz):
        return lax.rem(z + 8 - dz, 8)

    def relay(p, dz):
        zs = source(dz)
        landed(pz.at[p, zs], p1r.at[p, zs])
        p2_copy(pz.at[p, zs], p, zs, 0).start()
        p2_copy(pz.at[p, zs], p, zs, 1).start()

    def forward(p, dz):
        zs = source(dz)
        landed(pb.at[p, pl.ds(0, 2), zs], p2r.at[p, zs])
        p3_copy(p, 0, zs).start()
        p3_copy(p, 1, zs).start()

    def gathered_z(dz):
        zs = source(dz)
        landed(rc.at[0, y, zs], rbr.at[zs])
        near_y(0, zs)
        x_copy(zs).start()

    def gathered_x(dz):
        zs = source(dz)
        landed(rc.at[1, y, zs], rxr.at[zs])
        near_y(1, zs)

    def gathered_y(o):
        landed(rc.at[o, pl.ds(0, 3)], rcr.at[o])
        for b in range(4):
            rto[128 * o : 128 * o + 128, 256 * b : 256 * b + 256] = rc[o, b, :, 0:32, :].reshape(256, 128).T
            rtv[128 * o : 128 * o + 128, 128 * b : 128 * b + 128] = rc[o, b, :, 32:48, :].reshape(128, 128).T

    def g_rows(t, kk):
        o = jnp.abs(lax.div(t, 2) - xl)
        return pl.ds(pl.multiple_of(128 * o + 64 * lax.rem(t, 2) + 32 * kk, 32), 32)

    def g_copy(p, t, kk):
        return pltpu.make_async_remote_copy(
            src_ref=gp.at[p, g_rows(t, kk)], dst_ref=pr.at[p, z], send_sem=gs, recv_sem=gr.at[p, z],
            device_id=(row_of(xh, 4 * core + t, kk), col), device_id_type=MESH,
        )

    own = lax.div(z, 4) == core
    place = lax.rem(z, 4)
    inner = jnp.logical_or(place == 1, place == 2)

    def nearest(j):
        t = jnp.where(inner, 1 - j if j < 2 else j, j)
        return jnp.where(place >= 2, 3 - t, t)

    def multiply(p):
        acc_o = jnp.zeros((256, 256), F32)
        acc_v = jnp.zeros((256, 256), F32)
        for b in range(4):
            left = rto[:, 256 * b : 256 * b + 256]
            acc_o += mdot(left, pb[p, b, :, 0:32, :].reshape(256, 256))
            left = rtv[:, 128 * b : 128 * b + 128]
            acc_v += mdot(left, pb[p, b, :, 32:48, :].reshape(128, 256))
        gp[p] = (acc_o * acc_v * SCALE).astype(BF16)
        for j in range(4):
            t = jnp.where(own, nearest(j), nearest(3 - j))
            for kk in range(2):
                mine = row == row_of(xh, 4 * core + t, kk)

                @pl.when(jnp.logical_not(mine))
                def _():
                    g_copy(p, t, kk).start()

                @pl.when(mine)
                def _():
                    pr[p, z] = gp[p, g_rows(t, kk)]

    for dz in NEAR:
        relay(0, dz)
    for dz in DIST:
        gathered_z(dz)
    for dz in FAR:
        relay(0, dz)
    for dz in (0, *DIST):
        gathered_x(dz)
    for dz in (0, *NEAR):
        forward(0, dz)
    for dz in NEAR:
        relay(1, dz)
    for dz in FAR:
        forward(0, dz)
    for dz in FAR:
        relay(1, dz)
    gathered_y(0)
    gathered_y(1)
    pl.semaphore_wait(ready, 16)
    landed(pb.at[0, pl.ds(0, 2)], p3r.at[0])
    multiply(0)
    for dz in (0, *DIST):
        forward(1, dz)
    landed(pb.at[1, pl.ds(0, 2)], p3r.at[1])
    multiply(1)

    slot = 8 * ((1 - xl) * 4 + y)

    def y_copy(p, q, c):
        lanes = pl.ds(pl.multiple_of(c * 128, 128), 128)
        return pltpu.make_async_remote_copy(
            src_ref=xs.at[p, pl.ds(2 * q, 2), :, lanes], dst_ref=xr.at[p, pl.ds(slot + 2 * q, 2)],
            send_sem=ys, recv_sem=yr.at[p, q], device_id=(row, c), device_id_type=MESH,
        )

    def pair(g):
        near = 3 - 2 * lax.rem(z, 2)
        return lax.rem(lax.div(z, 2) + (0, near, 4 - near, 2)[g], 4)

    def spread(p, groups):
        sides = [[], []]
        for q in groups:
            for t in range(2):
                zs = 2 * q + t

                @pl.when(jnp.logical_or(zs != z, jnp.logical_not(own)))
                def _():
                    landed(pr.at[p, zs], gr.at[p, zs])

        for q in groups:
            block = pr[p, pl.ds(2 * q, 2)]
            for side in range(2):
                sides[side].append(block[:, 16 * side : 16 * side + 16].reshape(32, 256))
        both = jnp.concatenate([jnp.concatenate(side, axis=0) for side in sides], axis=1)
        res = mdot(both, mtab[...]).astype(BF16)
        for n, q in enumerate(groups):
            xs[p, pl.ds(2 * q, 2)] = res[32 * n : 32 * n + 32].reshape(2, 16, 1024)

        def y_send(j, carry):
            for q in groups:
                y_copy(p, q, lax.rem(col + j, 8)).start()
            return carry

        lax.fori_loop(1, 8, y_send, 0)
        lanes = pl.ds(pl.multiple_of(col * 128, 128), 128)
        for q in groups:
            xr[p, pl.ds(slot + 2 * q, 2)] = xs[p, pl.ds(2 * q, 2), :, lanes]

    spread(0, (pair(0), pair(1)))
    spread(0, (pair(2), pair(3)))
    for g in range(4):
        spread(1, (pair(g),))

    for p in range(2):
        for g in range(4):
            q = pair(g)
            landed(xr.at[p, pl.ds(0, 14)], yr.at[p, q])
            parts = [xr[p, 8 * c + 2 * q + t] for t in range(2) for c in range(8)]
            both = jnp.concatenate([jnp.concatenate(parts[8 * t : 8 * t + 8], axis=0) for t in range(2)], axis=1)
            res = mdot(both, ntab[p])
            for c in range(8):
                block = res[16 * c : 16 * c + 16]
                zb[4 * c + q] = block if p == 0 else zb[4 * c + q] + block

    @pl.when(jnp.logical_and(col == 0, jnp.logical_not(self_a)))
    def _():
        landed(rc.at[0, 0], ras)

    @pl.when(self_a)
    def _():
        landed(rc.at[0, 0, pl.ds(0, 7)], ras)

    for p in range(2):
        landed(pz.at[p, pl.ds(0, 7)], p1s)
        landed(pb.at[p, pl.ds(0, 2)], p2s)
        landed(pb.at[p, pl.ds(0, 2)], p3s)
    landed(rc.at[0, 0, pl.ds(0, 7)], rbs)
    landed(rc.at[0, 0], rxs)
    landed(rc.at[0, pl.ds(0, 3)], rcs)
    landed(rc.at[1, pl.ds(0, 3)], rcs)

    for p in range(2):
        landed(xr.at[p, pl.ds(0, 56)], ys)

    @pl.when(own)
    def _():
        landed(pr.at[:, pl.ds(0, 7)], gs)

    @pl.when(jnp.logical_not(own))
    def _():
        landed(pr, gs)


def finish(zb, out_re, out_im, res_re, res_im, sem):
    lane = lax.broadcasted_iota(jnp.int32, (8, 128), 1)

    def put(i, which):
        res, out = ((res_re, out_re), (res_im, out_im))[which]
        rows = pl.ds(pl.multiple_of(256 * i, 256), 256)
        return pltpu.make_async_copy(res.at[rows], out.at[rows], sem.at[which, i])

    def a_step(i, carry):
        rows = pl.ds(pl.multiple_of(8 * lax.rem(i, 2), 8), 8)
        real = pl.ds(pl.multiple_of(256 * lax.div(i, 2), 128), 128)
        imag = pl.ds(pl.multiple_of(256 * lax.div(i, 2) + 128, 128), 128)
        res = fft([(zb[a, rows, real], zb[a, rows, imag]) for a in range(32)])
        for j in range(8):
            for part, out in ((0, res_re), (1, res_im)):
                moved = swap_groups([res[4 * j + t][part] for t in range(4)], lane)
                for kc in range(4):
                    out[pl.ds(i * 256 + j * 4 + kc, 8, stride=32), :] = moved[kc]
        put(i, 0).start()
        put(i, 1).start()
        return carry

    lax.fori_loop(0, 4, a_step, 0)
    for i in range(4):
        put(i, 0).wait()
        put(i, 1).wait()


def on_device(occ, vir, docc, dvir):
    anyspace = pl.BlockSpec(memory_space=pl.ANY)
    vmem = pl.BlockSpec(memory_space=pltpu.VMEM)
    dma = pltpu.SemaphoreType.DMA
    zb = pl.pallas_call(
        kernel,
        out_shape=pltpu.VMEM((32, 16, 512), F32),
        in_specs=[anyspace] * 6,
        out_specs=vmem,
        scratch_shapes=[
            pltpu.VMEM((48, 4096), BF16),
            pltpu.VMEM((1, 1024), F32),
            pltpu.VMEM((1, 512), F32),
            pltpu.VMEM((32, 1024), F32),
            pltpu.VMEM((512, 1024), BF16),
            pltpu.VMEM((2, 256, 512), BF16),
            pltpu.VMEM((2, 8, 48, 256), BF16),
            pltpu.VMEM((2, 4, 8, 48, 256), BF16),
            pltpu.VMEM((48, 1024), BF16),
            pltpu.VMEM((2, 4, 8, 48, 128), BF16),
            pltpu.VMEM((256, 1024), BF16),
            pltpu.VMEM((256, 512), BF16),
            pltpu.VMEM((2, 256, 256), BF16),
            pltpu.VMEM((2, 8, 32, 256), BF16),
            pltpu.VMEM((2, 8, 16, 1024), BF16),
            pltpu.VMEM((2, 64, 16, 128), BF16),
            dma((6,)),
            dma, dma((2, 8)),
            dma, dma((2, 8)),
            dma, dma((2,)),
            dma, dma,
            dma, dma((8,)),
            dma, dma((8,)),
            dma, dma((2,)),
            dma, dma((2, 8)),
            dma, dma((2, 4)),
            pltpu.SemaphoreType.REGULAR,
        ],
        compiler_params=pltpu.CompilerParams(collective_id=0, has_side_effects=True),
    )(
        occ, vir, docc.reshape(1, 1024), dvir.reshape(1, 512),
        jnp.asarray(c_table()), jnp.asarray(b_table()).astype(BF16),
    )
    out = jax.ShapeDtypeStruct((1024, 128), F32)
    res = pl.pallas_call(
        finish,
        out_shape=(out, out),
        in_specs=[vmem],
        out_specs=(anyspace, anyspace),
        scratch_shapes=[
            pltpu.VMEM((1024, 128), F32),
            pltpu.VMEM((1024, 128), F32),
            dma((2, 4)),
        ],
    )(pltpu.with_memory_space_constraint(zb, pltpu.VMEM))

    def placed(part):
        return jnp.transpose(part.reshape(32, 8, 4, 128), (0, 2, 1, 3)).reshape(32, 4, 1024)

    return placed(res[0]), placed(res[1])


def solution(mesh):
    in_specs = (P("row", "col"), P("row", "col"), P(), P())
    out_specs = (P("row", "col", None), P("row", "col", None))
    return jax.shard_map(
        on_device, mesh=mesh, in_specs=in_specs, out_specs=out_specs, check_vma=False
    )
```

```python
import functools
import math

import jax
import jax.numpy as jnp
import numpy as np
from jax import lax
from jax.experimental import pallas as pl
from jax.experimental.pallas import tpu as pltpu
from jax.sharding import PartitionSpec as P

MESH = pl.DeviceIdType.MESH
F32 = jnp.float32
BF16 = jnp.bfloat16
SCALE = -(2.0**-17)
DIST = (1, 7, 2, 6, 3, 5, 4)


def angle_table(length):
    k = np.arange(length)
    phase = np.outer(k, k) % length
    angle = 2.0 * np.pi * phase / length
    return np.cos(angle), np.sin(angle)


def c_table():
    cos, sin = angle_table(32)
    cos, sin = cos.reshape(32, 8, 1, 4), -sin.reshape(32, 8, 1, 4)
    both = np.stack([cos, sin], axis=2)
    return np.broadcast_to(both, (32, 8, 2, 16, 4)).reshape(32, 1024).astype(np.float32)


def b_table():
    cos, sin = angle_table(32)
    c, s = cos.reshape(2, 2, 8, 32).swapaxes(0, 1), sin.reshape(2, 2, 8, 32).swapaxes(0, 1)
    table = np.zeros((2, 2, 2, 2, 8, 4, 2, 2, 4, 32), np.float32)
    for kc in range(4):
        for h in range(2):
            table[:, :, 0, h, :, kc, h, 0, kc, :] = c
            table[:, :, 0, h, :, kc, h, 1, kc, :] = -s
            table[:, :, 1, h, :, kc, h, 0, kc, :] = s
            table[:, :, 1, h, :, kc, h, 1, kc, :] = c
    return table.reshape(2, 256, 512)


def fft(parts):
    n = len(parts)
    if n == 1:
        return parts
    half = n // 2
    even, odd = fft(parts[0::2]), fft(parts[1::2])
    low, high = [], []
    for k in range(half):
        (ar, ai), (br, bi) = even[k], odd[k]
        if k == 0:
            tr, ti = br, bi
        elif 4 * k == n:
            tr, ti = bi, -br
        else:
            c, s = math.cos(2 * math.pi * k / n), math.sin(2 * math.pi * k / n)
            tr, ti = c * br + s * bi, c * bi - s * br
        low.append((ar + tr, ai + ti))
        high.append((ar - tr, ai - ti))
    return low + high


def swap_groups(v, lane):
    v = list(v)
    for shift, pairs in ((64, ((0, 2), (1, 3))), (32, ((0, 1), (2, 3)))):
        low = lax.rem(lane, 2 * shift) < shift
        for i, j in pairs:
            a, b = v[i], v[j]
            v[i] = jnp.where(low, a, pltpu.roll(b, shift, 1))
            v[j] = jnp.where(low, pltpu.roll(a, 128 - shift, 1), b)
    return v


def tdot(a, b):
    return lax.dot_general(a, b, (((0,), (0,)), ((), ())), preferred_element_type=F32)


def mdot(a, b):
    return jnp.dot(a, b, preferred_element_type=F32)


def kernel(
    occ, vir, docc, dvir, ctab, btab, zb,
    inb, dov, dvv, ctv, mtab, ntab,
    pz, pb, rs, rc, rto, rtv, gp, pr, xs, xr,
    in_sem, p1s, p1r, p2s, p2r, p3s, p3r, ras, rar, rbs, rbr, rxs, rxr, rcs, rcr, gs, gr, ys, yr, ready,
):
    row, col = lax.axis_index("row"), lax.axis_index("col")
    core = lax.rem(row, 2)
    z = lax.rem(lax.div(row, 2), 8)
    xh = lax.div(row, 16)
    y, xl = lax.rem(col, 4), lax.div(col, 4)
    x = 2 * xh + xl

    def row_of(xh_, z_, k_):
        return (xh_ * 8 + z_) * 2 + k_

    barrier = pltpu.get_barrier_semaphore()

    for i in range(1, 8):
        pl.semaphore_signal(
            barrier, inc=1, device_id=(row_of(xh, lax.rem(z + i, 8), core), col), device_id_type=MESH
        )
    for i in range(16):
        pl.semaphore_signal(barrier, inc=1, device_id=(row_of(xh, z, i % 2), i // 2), device_id_type=MESH)
    for i in range(16):
        pl.semaphore_signal(barrier, inc=1, device_id=(row_of(1 - xh, z, i % 2), i // 2), device_id_type=MESH)

    loads = [
        pltpu.make_async_copy(occ, inb.at[pl.ds(0, 32)], in_sem.at[0]),
        pltpu.make_async_copy(vir, inb.at[pl.ds(32, 16)], in_sem.at[1]),
        pltpu.make_async_copy(docc, dov, in_sem.at[2]),
        pltpu.make_async_copy(dvir, dvv, in_sem.at[3]),
        pltpu.make_async_copy(ctab, ctv, in_sem.at[4]),
        pltpu.make_async_copy(btab, ntab, in_sem.at[5]),
    ]
    for load in loads:
        load.start()

    for load in loads:
        load.wait()

    @pl.when(col == 0)
    def _():
        lane = lax.broadcasted_iota(jnp.int32, (32, 1024), 1)
        band = lax.broadcasted_iota(jnp.int32, (32, 1024), 0)
        dec = jnp.sum(jnp.where(lane == band + 32 * row, dov[...], 0.0), axis=1, keepdims=True)
        rs[0:32, :] = (inb[0:32, 0:1024].astype(F32) * dec).astype(BF16)
        lane = lax.broadcasted_iota(jnp.int32, (16, 512), 1)
        band = lax.broadcasted_iota(jnp.int32, (16, 512), 0)
        dec = jnp.sum(jnp.where(lane == band + 16 * row, dvv[...], 0.0), axis=1, keepdims=True)
        rs[32:48, :] = (inb[32:48, 0:1024].astype(F32) * dec).astype(BF16)

    pl.semaphore_wait(barrier, 39)

    def greet_ready(i, c):
        pl.semaphore_signal(
            ready, inc=1, device_id=(row_of(xh, z, lax.rem(i, 2)), lax.div(i, 2)), device_id_type=MESH
        )
        return c

    lax.fori_loop(0, 16, greet_ready, 0)

    def landed(ref, sem):
        pltpu.make_async_copy(ref, ref, sem).wait()

    def a_copy(i):
        s, kk, xt = lax.div(i, 4), lax.rem(lax.div(i, 2), 2), lax.rem(i, 2)
        lanes = pl.ds(pl.multiple_of(512 * s + 256 * kk + 128 * xt, 128), 128)
        b = 2 * xh + core
        return pltpu.make_async_remote_copy(
            src_ref=rs.at[:, lanes], dst_ref=rc.at[0, b, z], send_sem=ras, recv_sem=rar,
            device_id=(row_of(s, z, kk), xt * 4 + b), device_id_type=MESH,
        )

    def b_copy(dz):
        ref = rc.at[0, y, z]
        return pltpu.make_async_remote_copy(
            src_ref=ref, dst_ref=ref, send_sem=rbs, recv_sem=rbr.at[min(dz, 8 - dz) - 1],
            device_id=(row_of(xh, lax.rem(z + dz, 8), core), col), device_id_type=MESH,
        )

    def x_copy(zs, d):
        return pltpu.make_async_remote_copy(
            src_ref=rc.at[0, y, zs], dst_ref=rc.at[1, y, zs], send_sem=rxs, recv_sem=rxr.at[d],
            device_id=(row, (1 - xl) * 4 + y), device_id_type=MESH,
        )

    def c_copy(o, zs, dy):
        ref = rc.at[o, y, zs]
        return pltpu.make_async_remote_copy(
            src_ref=ref, dst_ref=ref, send_sem=rcs, recv_sem=rcr.at[o],
            device_id=(row, xl * 4 + lax.rem(y + dy, 4)), device_id_type=MESH,
        )

    def near_y(o, zs):
        for dy in (1, 3, 2):
            c_copy(o, zs, dy).start()

    def p1_copy(p, dz):
        zt = lax.rem(z + dz, 8)
        return pltpu.make_async_remote_copy(
            src_ref=inb.at[:, part_of(zt, p)], dst_ref=pz.at[p, z], send_sem=p1s, recv_sem=p1r.at[p, min(dz, 8 - dz) - 1],
            device_id=(row_of(xh, zt, core), col), device_id_type=MESH,
        )

    def part_of(zs, p):
        return pl.ds(pl.multiple_of(zs * 512 + p * 256, 256), 256)

    def p2_copy(src, p, zs, side, d):
        xt = lax.rem(x + 1 + 2 * side, 4)
        return pltpu.make_async_remote_copy(
            src_ref=src, dst_ref=pb.at[p, 2 * xh + core, zs], send_sem=p2s, recv_sem=p2r.at[p, d],
            device_id=(row_of(lax.div(xt, 2), z, core), lax.rem(xt, 2) * 4 + y), device_id_type=MESH,
        )

    def p3_copy(p, xs, zs):
        ref = pb.at[p, 2 * xs + core, zs]
        return pltpu.make_async_remote_copy(
            src_ref=ref, dst_ref=ref, send_sem=p3s, recv_sem=p3r.at[p],
            device_id=(row + 1 - 2 * core, col), device_id_type=MESH,
        )

    self_a = jnp.logical_and(col == 0, jnp.logical_and(xh == 0, core == 0))

    @pl.when(col == 0)
    def _():
        def send(i, carry):
            @pl.when(jnp.logical_or(i != 0, jnp.logical_not(self_a)))
            def _():
                a_copy(i).start()

            return carry

        lax.fori_loop(0, 8, send, 0)

    @pl.when(self_a)
    def _():
        rc[0, 0, z] = rs[:, 0:128]

    for dz in DIST:
        p1_copy(0, dz).start()
    for p in range(2):
        for side in range(2):
            p2_copy(inb.at[:, part_of(z, p)], p, z, side, 0).start()

    @pl.when(jnp.logical_not(self_a))
    def _():
        landed(rc.at[0, y, z], rar)

    for dz in DIST:
        b_copy(dz).start()
    near_y(0, z)
    x_copy(z, 0).start()
    for dz in DIST:
        p1_copy(1, dz).start()

    blane = lax.rem(lax.div(lax.broadcasted_iota(jnp.int32, (32, 1024), 1), 4), 16)
    ct = ctv[...]

    def table(b, c):
        rows = pl.ds(pl.multiple_of(b * 32, 32), 32)
        mtab[rows, :] = jnp.where(blane == b, ct, 0.0).astype(BF16)
        return c

    lax.fori_loop(0, 16, table, 0)

    def source(dz):
        return lax.rem(z + 8 - dz, 8)

    def at(d):
        return [source(dz) for dz in ((d,) if d in (0, 4) else (d, 8 - d))]

    def relay(p, d):
        landed(pz.at[p, pl.ds(0, len(at(d)))], p1r.at[p, d - 1])
        for zs in at(d):
            for side in range(2):
                p2_copy(pz.at[p, zs], p, zs, side, d).start()

    def forward(p, d):
        landed(pb.at[p, 0, pl.ds(0, 2 * len(at(d)))], p2r.at[p, d])
        for zs in at(d):
            p3_copy(p, 0, zs).start()
            p3_copy(p, 1, zs).start()

    def gathered_z(d):
        landed(rc.at[0, 0, pl.ds(0, len(at(d)))], rbr.at[d - 1])
        for zs in at(d):
            x_copy(zs, d).start()
            near_y(0, zs)

    def gathered_x(d):
        landed(rc.at[1, 0, pl.ds(0, len(at(d)))], rxr.at[d])
        for zs in at(d):
            near_y(1, zs)

    def gathered_y(o):
        landed(rc.at[o, pl.ds(0, 3)], rcr.at[o])
        for b in range(4):
            rto[128 * o : 128 * o + 128, 256 * b : 256 * b + 256] = rc[o, b, :, 0:32, :].reshape(256, 128).T
            rtv[128 * o : 128 * o + 128, 128 * b : 128 * b + 128] = rc[o, b, :, 32:48, :].reshape(128, 128).T

    def g_rows(t, kk):
        o = jnp.abs(lax.div(t, 2) - xl)
        return pl.ds(pl.multiple_of(128 * o + 64 * lax.rem(t, 2) + 32 * kk, 32), 32)

    def g_copy(p, t, kk):
        return pltpu.make_async_remote_copy(
            src_ref=gp.at[p, g_rows(t, kk)], dst_ref=pr.at[p, z], send_sem=gs, recv_sem=gr.at[p, lax.div(z, 2)],
            device_id=(row_of(xh, 4 * core + t, kk), col), device_id_type=MESH,
        )

    own = lax.div(z, 4) == core
    place = lax.rem(z, 4)
    inner = jnp.logical_or(place == 1, place == 2)

    def nearest(j):
        t = jnp.where(inner, 1 - j if j < 2 else j, j)
        return jnp.where(place >= 2, 3 - t, t)

    def multiply(p):
        acc_o = jnp.zeros((256, 256), F32)
        acc_v = jnp.zeros((256, 256), F32)
        for b in range(4):
            left = rto[:, 256 * b : 256 * b + 256]
            acc_o += mdot(left, pb[p, b, :, 0:32, :].reshape(256, 256))
            left = rtv[:, 128 * b : 128 * b + 128]
            acc_v += mdot(left, pb[p, b, :, 32:48, :].reshape(128, 256))
        gp[p] = (acc_o * acc_v * SCALE).astype(BF16)
        for j in range(4):
            t = jnp.where(own, nearest(j), nearest(3 - j))
            for kk in range(2):
                mine = row == row_of(xh, 4 * core + t, kk)

                @pl.when(jnp.logical_not(mine))
                def _():
                    g_copy(p, t, kk).start()

                @pl.when(mine)
                def _():
                    pr[p, z] = gp[p, g_rows(t, kk)]

    relay(0, 1)
    relay(0, 2)
    for d in range(1, 5):
        gathered_z(d)
    relay(0, 3)
    relay(0, 4)
    for d in range(5):
        gathered_x(d)
    for d in range(3):
        forward(0, d)
    relay(1, 1)
    relay(1, 2)
    forward(0, 3)
    forward(0, 4)
    relay(1, 3)
    relay(1, 4)
    gathered_y(0)
    gathered_y(1)
    pl.semaphore_wait(ready, 16)
    landed(pb.at[0, pl.ds(0, 2)], p3r.at[0])
    multiply(0)
    for d in range(5):
        forward(1, d)
    landed(pb.at[1, pl.ds(0, 2)], p3r.at[1])
    multiply(1)

    slot = 8 * ((1 - xl) * 4 + y)

    def y_copy(p, q, c):
        lanes = pl.ds(pl.multiple_of(c * 128, 128), 128)
        return pltpu.make_async_remote_copy(
            src_ref=xs.at[p, pl.ds(2 * q, 2), :, lanes], dst_ref=xr.at[p, pl.ds(slot + 2 * q, 2)],
            send_sem=ys, recv_sem=yr.at[p, q], device_id=(row, c), device_id_type=MESH,
        )

    def pair(g):
        near = 3 - 2 * lax.rem(z, 2)
        return lax.rem(lax.div(z, 2) + (0, near, 4 - near, 2)[g], 4)

    def spread(p, groups):
        sides = [[], []]
        for q in groups:
            mine = jnp.logical_and(own, q == lax.div(z, 2))

            @pl.when(mine)
            def _():
                landed(pr.at[p, 0], gr.at[p, q])

            @pl.when(jnp.logical_not(mine))
            def _():
                landed(pr.at[p, pl.ds(0, 2)], gr.at[p, q])

        for q in groups:
            block = pr[p, pl.ds(2 * q, 2)]
            for side in range(2):
                sides[side].append(block[:, 16 * side : 16 * side + 16].reshape(32, 256))
        both = jnp.concatenate([jnp.concatenate(side, axis=0) for side in sides], axis=1)
        res = mdot(both, mtab[...]).astype(BF16)
        for n, q in enumerate(groups):
            xs[p, pl.ds(2 * q, 2)] = res[32 * n : 32 * n + 32].reshape(2, 16, 1024)

        def y_send(j, carry):
            for q in groups:
                y_copy(p, q, lax.rem(col + j, 8)).start()
            return carry

        lax.fori_loop(1, 8, y_send, 0)
        lanes = pl.ds(pl.multiple_of(col * 128, 128), 128)
        for q in groups:
            xr[p, pl.ds(slot + 2 * q, 2)] = xs[p, pl.ds(2 * q, 2), :, lanes]

    spread(0, (pair(0), pair(1)))
    spread(0, (pair(2), pair(3)))
    for g in range(4):
        spread(1, (pair(g),))

    for p in range(2):
        for g in range(4):
            q = pair(g)
            landed(xr.at[p, pl.ds(0, 14)], yr.at[p, q])
            parts = [xr[p, 8 * c + 2 * q + t] for t in range(2) for c in range(8)]
            both = jnp.concatenate([jnp.concatenate(parts[8 * t : 8 * t + 8], axis=0) for t in range(2)], axis=1)
            res = mdot(both, ntab[p])
            for c in range(8):
                block = res[16 * c : 16 * c + 16]
                zb[4 * c + q] = block if p == 0 else zb[4 * c + q] + block

    @pl.when(jnp.logical_and(col == 0, jnp.logical_not(self_a)))
    def _():
        landed(rc.at[0, 0], ras)

    @pl.when(self_a)
    def _():
        landed(rc.at[0, 0, pl.ds(0, 7)], ras)

    for p in range(2):
        landed(pz.at[p, pl.ds(0, 7)], p1s)
        landed(pb.at[p, pl.ds(0, 2)], p2s)
        landed(pb.at[p, pl.ds(0, 2)], p3s)
    landed(rc.at[0, 0, pl.ds(0, 7)], rbs)
    landed(rc.at[0, 0], rxs)
    landed(rc.at[0, pl.ds(0, 3)], rcs)
    landed(rc.at[1, pl.ds(0, 3)], rcs)

    for p in range(2):
        landed(xr.at[p, pl.ds(0, 56)], ys)

    @pl.when(own)
    def _():
        landed(pr.at[:, pl.ds(0, 7)], gs)

    @pl.when(jnp.logical_not(own))
    def _():
        landed(pr, gs)


def finish(zb, out_re, out_im, res_re, res_im, first, second, sem):
    lane = lax.broadcasted_iota(jnp.int32, (8, 128), 1)

    def put(i, which):
        res, out = ((res_re, out_re), (res_im, out_im))[which]
        rows = pl.ds(8 * i, 8)
        return pltpu.make_async_copy(res.at[rows], out.at[rows], sem.at[which, i])

    def a_step(i, carry):
        rows = pl.ds(pl.multiple_of(8 * lax.rem(i, 2), 8), 8)
        real = pl.ds(pl.multiple_of(256 * lax.div(i, 2), 128), 128)
        imag = pl.ds(pl.multiple_of(256 * lax.div(i, 2) + 128, 128), 128)
        for q in range(8):
            quarter = fft([(zb[8 * n + q, rows, real], zb[8 * n + q, rows, imag]) for n in range(4)])
            for k in range(4):
                c, s = math.cos(2 * math.pi * q * k / 32), math.sin(2 * math.pi * q * k / 32)
                (re, im) = quarter[k]
                first[k, q, 0] = c * re + s * im if q * k else re
                first[k, q, 1] = c * im - s * re if q * k else im
        for k in range(4):
            eighth = fft([(first[k, q, 0], first[k, q, 1]) for q in range(8)])
            for j in range(8):
                second[j, k, 0], second[j, k, 1] = eighth[j]
        for n in range(4):
            for part, out in ((0, res_re), (1, res_im)):
                moved = []
                for j in (2 * n, 2 * n + 1):
                    moved += swap_groups([second[j, t, part] for t in range(4)], lane)
                out[pl.ds(8 * i, 8), 8 * n : 8 * n + 8, :] = jnp.swapaxes(jnp.stack(moved), 0, 1)
        put(i, 0).start()
        put(i, 1).start()
        return carry

    lax.fori_loop(0, 4, a_step, 0)
    for i in range(4):
        put(i, 0).wait()
        put(i, 1).wait()


def on_device(occ, vir, docc, dvir):
    anyspace = pl.BlockSpec(memory_space=pl.ANY)
    vmem = pl.BlockSpec(memory_space=pltpu.VMEM)
    dma = pltpu.SemaphoreType.DMA
    zb = pl.pallas_call(
        kernel,
        out_shape=pltpu.VMEM((32, 16, 512), F32),
        in_specs=[anyspace] * 6,
        out_specs=vmem,
        scratch_shapes=[
            pltpu.VMEM((48, 4096), BF16),
            pltpu.VMEM((1, 1024), F32),
            pltpu.VMEM((1, 512), F32),
            pltpu.VMEM((32, 1024), F32),
            pltpu.VMEM((512, 1024), BF16),
            pltpu.VMEM((2, 256, 512), BF16),
            pltpu.VMEM((2, 8, 48, 256), BF16),
            pltpu.VMEM((2, 4, 8, 48, 256), BF16),
            pltpu.VMEM((48, 1024), BF16),
            pltpu.VMEM((2, 4, 8, 48, 128), BF16),
            pltpu.VMEM((256, 1024), BF16),
            pltpu.VMEM((256, 512), BF16),
            pltpu.VMEM((2, 256, 256), BF16),
            pltpu.VMEM((2, 8, 32, 256), BF16),
            pltpu.VMEM((2, 8, 16, 1024), BF16),
            pltpu.VMEM((2, 64, 16, 128), BF16),
            dma((6,)),
            dma, dma((2, 4)),
            dma, dma((2, 5)),
            dma, dma((2,)),
            dma, dma,
            dma, dma((4,)),
            dma, dma((5,)),
            dma, dma((2,)),
            dma, dma((2, 4)),
            dma, dma((2, 4)),
            pltpu.SemaphoreType.REGULAR,
        ],
        compiler_params=pltpu.CompilerParams(collective_id=0, has_side_effects=True),
    )(
        occ, vir, docc.reshape(1, 1024), dvir.reshape(1, 512),
        jnp.asarray(c_table()), jnp.asarray(b_table()).astype(BF16),
    )
    out = jax.ShapeDtypeStruct((32, 32, 128), F32)
    res = pl.pallas_call(
        finish,
        out_shape=(out, out),
        in_specs=[vmem],
        out_specs=(anyspace, anyspace),
        scratch_shapes=[
            pltpu.VMEM((32, 32, 128), F32),
            pltpu.VMEM((32, 32, 128), F32),
            pltpu.VMEM((4, 8, 2, 8, 128), F32),
            pltpu.VMEM((8, 4, 2, 8, 128), F32),
            dma((2, 4)),
        ],
    )(pltpu.with_memory_space_constraint(zb, pltpu.VMEM))

    def placed(part):
        return jnp.transpose(part.reshape(32, 8, 4, 128), (0, 2, 1, 3)).reshape(32, 4, 1024)

    return placed(res[0]), placed(res[1])


def solution(mesh):
    in_specs = (P("row", "col"), P("row", "col"), P(), P())
    out_specs = (P("row", "col", None), P("row", "col", None))
    return jax.shard_map(
        on_device, mesh=mesh, in_specs=in_specs, out_specs=out_specs, check_vma=False
    )
```

```python
import functools
import math

import jax
import jax.numpy as jnp
import numpy as np
from jax import lax
from jax.experimental import pallas as pl
from jax.experimental.pallas import tpu as pltpu
from jax.sharding import PartitionSpec as P

MESH = pl.DeviceIdType.MESH
F32 = jnp.float32
BF16 = jnp.bfloat16
SCALE = -(2.0**-17)
DIST = (1, 7, 2, 6, 3, 5, 4)


def angle_table(length):
    k = np.arange(length)
    phase = np.outer(k, k) % length
    angle = 2.0 * np.pi * phase / length
    return np.cos(angle), np.sin(angle)


def c_table():
    cos, sin = angle_table(32)
    cos, sin = cos.reshape(32, 8, 1, 4), -sin.reshape(32, 8, 1, 4)
    both = np.stack([cos, sin], axis=2)
    return np.broadcast_to(both, (32, 8, 2, 16, 4)).reshape(32, 1024).astype(np.float32)


def b_table():
    cos, sin = angle_table(32)
    c, s = cos.reshape(2, 2, 8, 32).swapaxes(0, 1), sin.reshape(2, 2, 8, 32).swapaxes(0, 1)
    table = np.zeros((2, 2, 2, 2, 8, 4, 2, 2, 4, 32), np.float32)
    for kc in range(4):
        for h in range(2):
            table[:, :, 0, h, :, kc, h, 0, kc, :] = c
            table[:, :, 0, h, :, kc, h, 1, kc, :] = -s
            table[:, :, 1, h, :, kc, h, 0, kc, :] = s
            table[:, :, 1, h, :, kc, h, 1, kc, :] = c
    return table.reshape(2, 256, 512)


def fft(parts):
    n = len(parts)
    if n == 1:
        return parts
    half = n // 2
    even, odd = fft(parts[0::2]), fft(parts[1::2])
    low, high = [], []
    for k in range(half):
        (ar, ai), (br, bi) = even[k], odd[k]
        if k == 0:
            tr, ti = br, bi
        elif 4 * k == n:
            tr, ti = bi, -br
        else:
            c, s = math.cos(2 * math.pi * k / n), math.sin(2 * math.pi * k / n)
            tr, ti = c * br + s * bi, c * bi - s * br
        low.append((ar + tr, ai + ti))
        high.append((ar - tr, ai - ti))
    return low + high


def swap_groups(v, lane):
    v = list(v)
    for shift, pairs in ((64, ((0, 2), (1, 3))), (32, ((0, 1), (2, 3)))):
        low = lax.rem(lane, 2 * shift) < shift
        for i, j in pairs:
            a, b = v[i], v[j]
            v[i] = jnp.where(low, a, pltpu.roll(b, shift, 1))
            v[j] = jnp.where(low, pltpu.roll(a, 128 - shift, 1), b)
    return v


def tdot(a, b):
    return lax.dot_general(a, b, (((0,), (0,)), ((), ())), preferred_element_type=F32)


def mdot(a, b):
    return jnp.dot(a, b, preferred_element_type=F32)


def kernel(
    occ, vir, docc, dvir, ctab, btab, zb,
    inb, dov, dvv, ctv, mtab, ntab,
    pz, pb, rs, rc, rto, rtv, gp, pr, xs, xr,
    in_sem, p1s, p1r, p2s, p2r, p3s, p3r, ras, rar, rbs, rbr, rxs, rxr, rcs, rcr, gs, gr, ys, yr, ready,
):
    row, col = lax.axis_index("row"), lax.axis_index("col")
    core = lax.rem(row, 2)
    z = lax.rem(lax.div(row, 2), 8)
    xh = lax.div(row, 16)
    y, xl = lax.rem(col, 4), lax.div(col, 4)
    x = 2 * xh + xl

    def row_of(xh_, z_, k_):
        return (xh_ * 8 + z_) * 2 + k_

    barrier = pltpu.get_barrier_semaphore()

    for i in range(1, 8):
        pl.semaphore_signal(
            barrier, inc=1, device_id=(row_of(xh, lax.rem(z + i, 8), core), col), device_id_type=MESH
        )
    for i in range(16):
        pl.semaphore_signal(barrier, inc=1, device_id=(row_of(xh, z, i % 2), i // 2), device_id_type=MESH)
    for i in range(16):
        pl.semaphore_signal(barrier, inc=1, device_id=(row_of(1 - xh, z, i % 2), i // 2), device_id_type=MESH)

    loads = [
        pltpu.make_async_copy(occ, inb.at[pl.ds(0, 32)], in_sem.at[0]),
        pltpu.make_async_copy(vir, inb.at[pl.ds(32, 16)], in_sem.at[1]),
        pltpu.make_async_copy(docc, dov, in_sem.at[2]),
        pltpu.make_async_copy(dvir, dvv, in_sem.at[3]),
        pltpu.make_async_copy(ctab, ctv, in_sem.at[4]),
        pltpu.make_async_copy(btab, ntab, in_sem.at[5]),
    ]
    for load in loads:
        load.start()

    for load in loads:
        load.wait()

    @pl.when(col == 0)
    def _():
        lane = lax.broadcasted_iota(jnp.int32, (32, 1024), 1)
        band = lax.broadcasted_iota(jnp.int32, (32, 1024), 0)
        dec = jnp.sum(jnp.where(lane == band + 32 * row, dov[...], 0.0), axis=1, keepdims=True)
        rs[0:32, :] = (inb[0:32, 0:1024].astype(F32) * dec).astype(BF16)
        lane = lax.broadcasted_iota(jnp.int32, (16, 512), 1)
        band = lax.broadcasted_iota(jnp.int32, (16, 512), 0)
        dec = jnp.sum(jnp.where(lane == band + 16 * row, dvv[...], 0.0), axis=1, keepdims=True)
        rs[32:48, :] = (inb[32:48, 0:1024].astype(F32) * dec).astype(BF16)

    pl.semaphore_wait(barrier, 39)

    def greet_ready(i, c):
        pl.semaphore_signal(
            ready, inc=1, device_id=(row_of(xh, z, lax.rem(i, 2)), lax.div(i, 2)), device_id_type=MESH
        )
        return c

    lax.fori_loop(0, 16, greet_ready, 0)

    def landed(ref, sem):
        pltpu.make_async_copy(ref, ref, sem).wait()

    def a_copy(i):
        s, kk, xt = lax.div(i, 4), lax.rem(lax.div(i, 2), 2), lax.rem(i, 2)
        lanes = pl.ds(pl.multiple_of(512 * s + 256 * kk + 128 * xt, 128), 128)
        b = 2 * xh + core
        return pltpu.make_async_remote_copy(
            src_ref=rs.at[:, lanes], dst_ref=rc.at[0, b, z], send_sem=ras, recv_sem=rar,
            device_id=(row_of(s, z, kk), xt * 4 + b), device_id_type=MESH,
        )

    def b_copy(dz):
        ref = rc.at[0, y, z]
        return pltpu.make_async_remote_copy(
            src_ref=ref, dst_ref=ref, send_sem=rbs, recv_sem=rbr.at[min(dz, 8 - dz) - 1],
            device_id=(row_of(xh, lax.rem(z + dz, 8), core), col), device_id_type=MESH,
        )

    def x_copy(zs, d):
        return pltpu.make_async_remote_copy(
            src_ref=rc.at[0, y, zs], dst_ref=rc.at[1, y, zs], send_sem=rxs, recv_sem=rxr.at[d],
            device_id=(row, (1 - xl) * 4 + y), device_id_type=MESH,
        )

    def c_copy(o, zs, dy):
        ref = rc.at[o, y, zs]
        return pltpu.make_async_remote_copy(
            src_ref=ref, dst_ref=ref, send_sem=rcs, recv_sem=rcr.at[o],
            device_id=(row, xl * 4 + lax.rem(y + dy, 4)), device_id_type=MESH,
        )

    def near_y(o, zs):
        for dy in (1, 3, 2):
            c_copy(o, zs, dy).start()

    def p1_copy(p, dz):
        zt = lax.rem(z + dz, 8)
        return pltpu.make_async_remote_copy(
            src_ref=inb.at[:, part_of(zt, p)], dst_ref=pz.at[p, z], send_sem=p1s, recv_sem=p1r.at[p, min(dz, 8 - dz) - 1],
            device_id=(row_of(xh, zt, core), col), device_id_type=MESH,
        )

    def part_of(zs, p):
        return pl.ds(pl.multiple_of(zs * 512 + p * 256, 256), 256)

    def p2_copy(src, p, zs, side, d):
        xt = lax.rem(x + 1 + 2 * side, 4)
        return pltpu.make_async_remote_copy(
            src_ref=src, dst_ref=pb.at[p, 2 * xh + core, zs], send_sem=p2s, recv_sem=p2r.at[p, d],
            device_id=(row_of(lax.div(xt, 2), z, core), lax.rem(xt, 2) * 4 + y), device_id_type=MESH,
        )

    def p3_copy(p, xs, zs):
        ref = pb.at[p, 2 * xs + core, zs]
        return pltpu.make_async_remote_copy(
            src_ref=ref, dst_ref=ref, send_sem=p3s, recv_sem=p3r.at[p],
            device_id=(row + 1 - 2 * core, col), device_id_type=MESH,
        )

    self_a = jnp.logical_and(col == 0, jnp.logical_and(xh == 0, core == 0))

    @pl.when(col == 0)
    def _():
        def send(i, carry):
            @pl.when(jnp.logical_or(i != 0, jnp.logical_not(self_a)))
            def _():
                a_copy(i).start()

            return carry

        lax.fori_loop(0, 8, send, 0)

    @pl.when(self_a)
    def _():
        rc[0, 0, z] = rs[:, 0:128]

    for dz in DIST:
        p1_copy(0, dz).start()
    for side in range(2):
        p2_copy(inb.at[:, part_of(z, 0)], 0, z, side, 0).start()

    @pl.when(jnp.logical_not(self_a))
    def _():
        landed(rc.at[0, y, z], rar)

    for dz in DIST:
        b_copy(dz).start()
    near_y(0, z)
    x_copy(z, 0).start()
    for dz in DIST:
        p1_copy(1, dz).start()

    blane = lax.rem(lax.div(lax.broadcasted_iota(jnp.int32, (32, 1024), 1), 4), 16)
    ct = ctv[...]

    def table(b, c):
        rows = pl.ds(pl.multiple_of(b * 32, 32), 32)
        mtab[rows, :] = jnp.where(blane == b, ct, 0.0).astype(BF16)
        return c

    lax.fori_loop(0, 16, table, 0)

    def source(dz):
        return lax.rem(z + 8 - dz, 8)

    def at(d):
        return [source(dz) for dz in ((d,) if d in (0, 4) else (d, 8 - d))]

    def relay(p, d):
        landed(pz.at[p, pl.ds(0, len(at(d)))], p1r.at[p, d - 1])
        for zs in at(d):
            for side in range(2):
                p2_copy(pz.at[p, zs], p, zs, side, d).start()

    def forward(p, d):
        landed(pb.at[p, 0, pl.ds(0, 2 * len(at(d)))], p2r.at[p, d])
        for zs in at(d):
            p3_copy(p, 0, zs).start()
            p3_copy(p, 1, zs).start()

    def gathered_z(d):
        landed(rc.at[0, 0, pl.ds(0, len(at(d)))], rbr.at[d - 1])
        for zs in at(d):
            x_copy(zs, d).start()
            near_y(0, zs)

    def gathered_x(d):
        landed(rc.at[1, 0, pl.ds(0, len(at(d)))], rxr.at[d])
        for zs in at(d):
            near_y(1, zs)

    def gathered_y(o):
        landed(rc.at[o, pl.ds(0, 3)], rcr.at[o])
        for b in range(4):
            rto[128 * o : 128 * o + 128, 256 * b : 256 * b + 256] = rc[o, b, :, 0:32, :].reshape(256, 128).T
            rtv[128 * o : 128 * o + 128, 128 * b : 128 * b + 128] = rc[o, b, :, 32:48, :].reshape(128, 128).T

    def g_rows(t, kk):
        o = jnp.abs(lax.div(t, 2) - xl)
        return pl.ds(pl.multiple_of(128 * o + 64 * lax.rem(t, 2) + 32 * kk, 32), 32)

    def g_copy(p, t, kk):
        return pltpu.make_async_remote_copy(
            src_ref=gp.at[p, g_rows(t, kk)], dst_ref=pr.at[p, z], send_sem=gs, recv_sem=gr.at[p, lax.div(z, 2)],
            device_id=(row_of(xh, 4 * core + t, kk), col), device_id_type=MESH,
        )

    own = lax.div(z, 4) == core
    place = lax.rem(z, 4)
    inner = jnp.logical_or(place == 1, place == 2)

    def nearest(j):
        t = jnp.where(inner, 1 - j if j < 2 else j, j)
        return jnp.where(place >= 2, 3 - t, t)

    def multiply(p):
        acc_o = jnp.zeros((256, 256), F32)
        acc_v = jnp.zeros((256, 256), F32)
        for b in range(4):
            left = rto[:, 256 * b : 256 * b + 256]
            acc_o += mdot(left, pb[p, b, :, 0:32, :].reshape(256, 256))
            left = rtv[:, 128 * b : 128 * b + 128]
            acc_v += mdot(left, pb[p, b, :, 32:48, :].reshape(128, 256))
        gp[p] = (acc_o * acc_v * SCALE).astype(BF16)
        for j in range(4):
            t = jnp.where(own, nearest(j), nearest(3 - j))
            for kk in range(2):
                mine = row == row_of(xh, 4 * core + t, kk)

                @pl.when(jnp.logical_not(mine))
                def _():
                    g_copy(p, t, kk).start()

                @pl.when(mine)
                def _():
                    pr[p, z] = gp[p, g_rows(t, kk)]

    relay(0, 1)
    relay(0, 2)
    for d in range(1, 5):
        gathered_z(d)
    relay(0, 3)
    relay(0, 4)
    for side in range(2):
        p2_copy(inb.at[:, part_of(z, 1)], 1, z, side, 0).start()
    for d in range(5):
        gathered_x(d)
    for d in range(3):
        forward(0, d)
    relay(1, 1)
    relay(1, 2)
    forward(0, 3)
    forward(0, 4)
    relay(1, 3)
    relay(1, 4)
    gathered_y(0)
    gathered_y(1)
    pl.semaphore_wait(ready, 16)
    def compute(p, carry):
        landed(pb.at[p, pl.ds(0, 2)], p3r.at[p])
        multiply(p)

        @pl.when(p == 0)
        def _():
            for d in range(5):
                forward(1, d)

        return carry

    lax.fori_loop(0, 2, compute, 0)

    slot = 8 * ((1 - xl) * 4 + y)

    def y_copy(p, q, c):
        lanes = pl.ds(pl.multiple_of(c * 128, 128), 128)
        return pltpu.make_async_remote_copy(
            src_ref=xs.at[p, pl.ds(2 * q, 2), :, lanes], dst_ref=xr.at[p, pl.ds(slot + 2 * q, 2)],
            send_sem=ys, recv_sem=yr.at[p, q], device_id=(row, c), device_id_type=MESH,
        )

    def pair(g):
        near = 3 - 2 * lax.rem(z, 2)
        step = jnp.where(g == 0, 0, jnp.where(g == 1, near, jnp.where(g == 2, 4 - near, 2)))
        return lax.rem(lax.div(z, 2) + step, 4)

    def spread(p, groups):
        sides = [[], []]
        for q in groups:
            mine = jnp.logical_and(own, q == lax.div(z, 2))

            @pl.when(mine)
            def _():
                landed(pr.at[p, 0], gr.at[p, q])

            @pl.when(jnp.logical_not(mine))
            def _():
                landed(pr.at[p, pl.ds(0, 2)], gr.at[p, q])

        for q in groups:
            block = pr[p, pl.ds(2 * q, 2)]
            for side in range(2):
                sides[side].append(block[:, 16 * side : 16 * side + 16].reshape(32, 256))
        both = jnp.concatenate([jnp.concatenate(side, axis=0) for side in sides], axis=1)
        res = mdot(both, mtab[...]).astype(BF16)
        for n, q in enumerate(groups):
            xs[p, pl.ds(2 * q, 2)] = res[32 * n : 32 * n + 32].reshape(2, 16, 1024)

        def y_send(j, carry):
            for q in groups:
                y_copy(p, q, lax.rem(col + j, 8)).start()
            return carry

        lax.fori_loop(1, 8, y_send, 0)
        lanes = pl.ds(pl.multiple_of(col * 128, 128), 128)
        for q in groups:
            xr[p, pl.ds(slot + 2 * q, 2)] = xs[p, pl.ds(2 * q, 2), :, lanes]

    def spread_next(n, carry):
        spread(lax.div(n, 4), (pair(lax.rem(n, 4)),))
        return carry

    lax.fori_loop(0, 8, spread_next, 0)

    for p in range(2):
        def b_step(g, carry):
            q = pair(g)
            landed(xr.at[p, pl.ds(0, 14)], yr.at[p, q])
            parts = [xr[p, 8 * c + 2 * q + t] for t in range(2) for c in range(8)]
            both = jnp.concatenate([jnp.concatenate(parts[8 * t : 8 * t + 8], axis=0) for t in range(2)], axis=1)
            res = mdot(both, ntab[p])
            for c in range(8):
                block = res[16 * c : 16 * c + 16]
                zb[4 * c + q] = block if p == 0 else zb[4 * c + q] + block
            return carry

        lax.fori_loop(0, 4, b_step, 0)

    @pl.when(jnp.logical_and(col == 0, jnp.logical_not(self_a)))
    def _():
        landed(rc.at[0, 0], ras)

    @pl.when(self_a)
    def _():
        landed(rc.at[0, 0, pl.ds(0, 7)], ras)

    for p in range(2):
        landed(pz.at[p, pl.ds(0, 7)], p1s)
        landed(pb.at[p, pl.ds(0, 2)], p2s)
        landed(pb.at[p, pl.ds(0, 2)], p3s)
    landed(rc.at[0, 0, pl.ds(0, 7)], rbs)
    landed(rc.at[0, 0], rxs)
    landed(rc.at[0, pl.ds(0, 3)], rcs)
    landed(rc.at[1, pl.ds(0, 3)], rcs)

    for p in range(2):
        landed(xr.at[p, pl.ds(0, 56)], ys)

    @pl.when(own)
    def _():
        landed(pr.at[:, pl.ds(0, 7)], gs)

    @pl.when(jnp.logical_not(own))
    def _():
        landed(pr, gs)


def finish(zb, out_re, out_im, res_re, res_im, first, second, sem):
    lane = lax.broadcasted_iota(jnp.int32, (8, 128), 1)

    def put(i, which):
        res, out = ((res_re, out_re), (res_im, out_im))[which]
        rows = pl.ds(8 * i, 8)
        return pltpu.make_async_copy(res.at[rows], out.at[rows], sem.at[which, i])

    def a_step(i, carry):
        rows = pl.ds(pl.multiple_of(8 * lax.rem(i, 2), 8), 8)
        real = pl.ds(pl.multiple_of(256 * lax.div(i, 2), 128), 128)
        imag = pl.ds(pl.multiple_of(256 * lax.div(i, 2) + 128, 128), 128)
        for q in range(8):
            quarter = fft([(zb[8 * n + q, rows, real], zb[8 * n + q, rows, imag]) for n in range(4)])
            for k in range(4):
                c, s = math.cos(2 * math.pi * q * k / 32), math.sin(2 * math.pi * q * k / 32)
                (re, im) = quarter[k]
                first[k, q, 0] = c * re + s * im if q * k else re
                first[k, q, 1] = c * im - s * re if q * k else im
        for k in range(4):
            eighth = fft([(first[k, q, 0], first[k, q, 1]) for q in range(8)])
            for j in range(8):
                second[j, k, 0], second[j, k, 1] = eighth[j]
        for n in range(4):
            for part, out in ((0, res_re), (1, res_im)):
                moved = []
                for j in (2 * n, 2 * n + 1):
                    moved += swap_groups([second[j, t, part] for t in range(4)], lane)
                out[pl.ds(8 * i, 8), 8 * n : 8 * n + 8, :] = jnp.swapaxes(jnp.stack(moved), 0, 1)
        put(i, 0).start()
        put(i, 1).start()
        return carry

    lax.fori_loop(0, 4, a_step, 0)
    for i in range(4):
        put(i, 0).wait()
        put(i, 1).wait()


def on_device(occ, vir, docc, dvir):
    anyspace = pl.BlockSpec(memory_space=pl.ANY)
    vmem = pl.BlockSpec(memory_space=pltpu.VMEM)
    dma = pltpu.SemaphoreType.DMA
    zb = pl.pallas_call(
        kernel,
        out_shape=pltpu.VMEM((32, 16, 512), F32),
        in_specs=[anyspace] * 6,
        out_specs=vmem,
        scratch_shapes=[
            pltpu.VMEM((48, 4096), BF16),
            pltpu.VMEM((1, 1024), F32),
            pltpu.VMEM((1, 512), F32),
            pltpu.VMEM((32, 1024), F32),
            pltpu.VMEM((512, 1024), BF16),
            pltpu.VMEM((2, 256, 512), BF16),
            pltpu.VMEM((2, 8, 48, 256), BF16),
            pltpu.VMEM((2, 4, 8, 48, 256), BF16),
            pltpu.VMEM((48, 1024), BF16),
            pltpu.VMEM((2, 4, 8, 48, 128), BF16),
            pltpu.VMEM((256, 1024), BF16),
            pltpu.VMEM((256, 512), BF16),
            pltpu.VMEM((2, 256, 256), BF16),
            pltpu.VMEM((2, 8, 32, 256), BF16),
            pltpu.VMEM((2, 8, 16, 1024), BF16),
            pltpu.VMEM((2, 64, 16, 128), BF16),
            dma((6,)),
            dma, dma((2, 4)),
            dma, dma((2, 5)),
            dma, dma((2,)),
            dma, dma,
            dma, dma((4,)),
            dma, dma((5,)),
            dma, dma((2,)),
            dma, dma((2, 4)),
            dma, dma((2, 4)),
            pltpu.SemaphoreType.REGULAR,
        ],
        compiler_params=pltpu.CompilerParams(collective_id=0, has_side_effects=True),
    )(
        occ, vir, docc.reshape(1, 1024), dvir.reshape(1, 512),
        jnp.asarray(c_table()), jnp.asarray(b_table()).astype(BF16),
    )
    out = jax.ShapeDtypeStruct((32, 32, 128), F32)
    res = pl.pallas_call(
        finish,
        out_shape=(out, out),
        in_specs=[vmem],
        out_specs=(anyspace, anyspace),
        scratch_shapes=[
            pltpu.VMEM((32, 32, 128), F32),
            pltpu.VMEM((32, 32, 128), F32),
            pltpu.VMEM((4, 8, 2, 8, 128), F32),
            pltpu.VMEM((8, 4, 2, 8, 128), F32),
            dma((2, 4)),
        ],
    )(pltpu.with_memory_space_constraint(zb, pltpu.VMEM))

    def placed(part):
        return jnp.transpose(part.reshape(32, 8, 4, 128), (0, 2, 1, 3)).reshape(32, 4, 1024)

    return placed(res[0]), placed(res[1])


def solution(mesh):
    in_specs = (P("row", "col"), P("row", "col"), P(), P())
    out_specs = (P("row", "col", None), P("row", "col", None))
    return jax.shard_map(
        on_device, mesh=mesh, in_specs=in_specs, out_specs=out_specs, check_vma=False
    )
```

```python
import functools
import math

import jax
import jax.numpy as jnp
import numpy as np
from jax import lax
from jax.experimental import pallas as pl
from jax.experimental.pallas import tpu as pltpu
from jax.sharding import PartitionSpec as P

MESH = pl.DeviceIdType.MESH
F32 = jnp.float32
BF16 = jnp.bfloat16
SCALE = -(2.0**-17)
DIST = (1, 7, 2, 6, 3, 5, 4)


def angle_table(length):
    k = np.arange(length)
    phase = np.outer(k, k) % length
    angle = 2.0 * np.pi * phase / length
    return np.cos(angle), np.sin(angle)


def c_table():
    cos, sin = angle_table(32)
    cos, sin = cos.reshape(32, 8, 1, 4), -sin.reshape(32, 8, 1, 4)
    both = np.stack([cos, sin], axis=2)
    return np.broadcast_to(both, (32, 8, 2, 16, 4)).reshape(32, 1024).astype(np.float32)


def b_table():
    cos, sin = angle_table(32)
    c, s = cos.reshape(2, 2, 8, 32).swapaxes(0, 1), sin.reshape(2, 2, 8, 32).swapaxes(0, 1)
    table = np.zeros((2, 2, 2, 2, 8, 4, 2, 2, 4, 32), np.float32)
    for kc in range(4):
        for h in range(2):
            table[:, :, 0, h, :, kc, h, 0, kc, :] = c
            table[:, :, 0, h, :, kc, h, 1, kc, :] = -s
            table[:, :, 1, h, :, kc, h, 0, kc, :] = s
            table[:, :, 1, h, :, kc, h, 1, kc, :] = c
    return table.reshape(2, 256, 512)


def fft(parts):
    n = len(parts)
    if n == 1:
        return parts
    half = n // 2
    even, odd = fft(parts[0::2]), fft(parts[1::2])
    low, high = [], []
    for k in range(half):
        (ar, ai), (br, bi) = even[k], odd[k]
        if k == 0:
            tr, ti = br, bi
        elif 4 * k == n:
            tr, ti = bi, -br
        else:
            c, s = math.cos(2 * math.pi * k / n), math.sin(2 * math.pi * k / n)
            tr, ti = c * br + s * bi, c * bi - s * br
        low.append((ar + tr, ai + ti))
        high.append((ar - tr, ai - ti))
    return low + high


def swap_groups(v, lane):
    v = list(v)
    for shift, pairs in ((64, ((0, 2), (1, 3))), (32, ((0, 1), (2, 3)))):
        low = lax.rem(lane, 2 * shift) < shift
        for i, j in pairs:
            a, b = v[i], v[j]
            v[i] = jnp.where(low, a, pltpu.roll(b, shift, 1))
            v[j] = jnp.where(low, pltpu.roll(a, 128 - shift, 1), b)
    return v


def tdot(a, b):
    return lax.dot_general(a, b, (((0,), (0,)), ((), ())), preferred_element_type=F32)


def mdot(a, b):
    return jnp.dot(a, b, preferred_element_type=F32)


def kernel(
    occ, vir, docc, dvir, ctab, btab, zb,
    inb, dov, dvv, ctv, mtab, ntab,
    pz, pb, rs, rc, rto, rtv, gp, pr, xs, xr,
    in_sem, p1s, p1r, p2s, p2r, p3s, p3r, ras, rar, rbs, rbr, rxs, rxr, rcs, rcr, gs, gr, ys, yr, ready,
):
    row, col = lax.axis_index("row"), lax.axis_index("col")
    core = lax.rem(row, 2)
    z = lax.rem(lax.div(row, 2), 8)
    xh = lax.div(row, 16)
    y, xl = lax.rem(col, 4), lax.div(col, 4)
    x = 2 * xh + xl

    def row_of(xh_, z_, k_):
        return (xh_ * 8 + z_) * 2 + k_

    barrier = pltpu.get_barrier_semaphore()

    for i in range(1, 8):
        pl.semaphore_signal(
            barrier, inc=1, device_id=(row_of(xh, lax.rem(z + i, 8), core), col), device_id_type=MESH
        )
    for i in range(16):
        pl.semaphore_signal(barrier, inc=1, device_id=(row_of(xh, z, i % 2), i // 2), device_id_type=MESH)
    for i in range(16):
        pl.semaphore_signal(barrier, inc=1, device_id=(row_of(1 - xh, z, i % 2), i // 2), device_id_type=MESH)

    loads = [
        pltpu.make_async_copy(occ, inb.at[pl.ds(0, 32)], in_sem.at[0]),
        pltpu.make_async_copy(vir, inb.at[pl.ds(32, 16)], in_sem.at[1]),
        pltpu.make_async_copy(docc, dov, in_sem.at[2]),
        pltpu.make_async_copy(dvir, dvv, in_sem.at[3]),
        pltpu.make_async_copy(ctab, ctv, in_sem.at[4]),
        pltpu.make_async_copy(btab, ntab, in_sem.at[5]),
    ]
    for load in loads:
        load.start()

    for load in loads:
        load.wait()

    @pl.when(col == 0)
    def _():
        lane = lax.broadcasted_iota(jnp.int32, (32, 1024), 1)
        band = lax.broadcasted_iota(jnp.int32, (32, 1024), 0)
        dec = jnp.sum(jnp.where(lane == band + 32 * row, dov[...], 0.0), axis=1, keepdims=True)
        rs[0:32, :] = (inb[0:32, 0:1024].astype(F32) * dec).astype(BF16)
        lane = lax.broadcasted_iota(jnp.int32, (16, 512), 1)
        band = lax.broadcasted_iota(jnp.int32, (16, 512), 0)
        dec = jnp.sum(jnp.where(lane == band + 16 * row, dvv[...], 0.0), axis=1, keepdims=True)
        rs[32:48, :] = (inb[32:48, 0:1024].astype(F32) * dec).astype(BF16)

    pl.semaphore_wait(barrier, 39)

    def greet_ready(i, c):
        pl.semaphore_signal(
            ready, inc=1, device_id=(row_of(xh, z, lax.rem(i, 2)), lax.div(i, 2)), device_id_type=MESH
        )
        return c

    lax.fori_loop(0, 16, greet_ready, 0)

    def landed(ref, sem):
        pltpu.make_async_copy(ref, ref, sem).wait()

    def a_copy(i):
        s, kk, xt = lax.div(i, 4), lax.rem(lax.div(i, 2), 2), lax.rem(i, 2)
        lanes = pl.ds(pl.multiple_of(512 * s + 256 * kk + 128 * xt, 128), 128)
        b = 2 * xh + core
        return pltpu.make_async_remote_copy(
            src_ref=rs.at[:, lanes], dst_ref=rc.at[0, b, z], send_sem=ras, recv_sem=rar,
            device_id=(row_of(s, z, kk), xt * 4 + b), device_id_type=MESH,
        )

    def b_copy(dz):
        ref = rc.at[0, y, z]
        return pltpu.make_async_remote_copy(
            src_ref=ref, dst_ref=ref, send_sem=rbs, recv_sem=rbr.at[min(dz, 8 - dz) - 1],
            device_id=(row_of(xh, lax.rem(z + dz, 8), core), col), device_id_type=MESH,
        )

    def x_copy(zs, d):
        return pltpu.make_async_remote_copy(
            src_ref=rc.at[0, y, zs], dst_ref=rc.at[1, y, zs], send_sem=rxs, recv_sem=rxr.at[d],
            device_id=(row, (1 - xl) * 4 + y), device_id_type=MESH,
        )

    def c_copy(o, zs, dy):
        ref = rc.at[o, y, zs]
        return pltpu.make_async_remote_copy(
            src_ref=ref, dst_ref=ref, send_sem=rcs, recv_sem=rcr.at[o],
            device_id=(row, xl * 4 + lax.rem(y + dy, 4)), device_id_type=MESH,
        )

    def near_y(o, zs):
        for dy in (1, 3, 2):
            c_copy(o, zs, dy).start()

    def p1_copy(p, dz):
        zt = lax.rem(z + dz, 8)
        return pltpu.make_async_remote_copy(
            src_ref=inb.at[:, part_of(zt, p)], dst_ref=pz.at[p, z], send_sem=p1s, recv_sem=p1r.at[p, min(dz, 8 - dz) - 1],
            device_id=(row_of(xh, zt, core), col), device_id_type=MESH,
        )

    def part_of(zs, p):
        return pl.ds(pl.multiple_of(zs * 512 + p * 256, 256), 256)

    def p2_copy(src, p, zs, side, d):
        xt = lax.rem(x + 1 + 2 * side, 4)
        return pltpu.make_async_remote_copy(
            src_ref=src, dst_ref=pb.at[p, 2 * xh + core, zs], send_sem=p2s, recv_sem=p2r.at[p, d],
            device_id=(row_of(lax.div(xt, 2), z, core), lax.rem(xt, 2) * 4 + y), device_id_type=MESH,
        )

    def p3_copy(p, xs, zs):
        ref = pb.at[p, 2 * xs + core, zs]
        return pltpu.make_async_remote_copy(
            src_ref=ref, dst_ref=ref, send_sem=p3s, recv_sem=p3r.at[p],
            device_id=(row + 1 - 2 * core, col), device_id_type=MESH,
        )

    self_a = jnp.logical_and(col == 0, jnp.logical_and(xh == 0, core == 0))

    @pl.when(col == 0)
    def _():
        def send(i, carry):
            @pl.when(jnp.logical_or(i != 0, jnp.logical_not(self_a)))
            def _():
                a_copy(i).start()

            return carry

        lax.fori_loop(0, 8, send, 0)

    @pl.when(self_a)
    def _():
        rc[0, 0, z] = rs[:, 0:128]

    for dz in DIST:
        p1_copy(0, dz).start()
    for side in range(2):
        p2_copy(inb.at[:, part_of(z, 0)], 0, z, side, 0).start()

    @pl.when(jnp.logical_not(self_a))
    def _():
        landed(rc.at[0, y, z], rar)

    for dz in DIST:
        b_copy(dz).start()
    near_y(0, z)
    x_copy(z, 0).start()
    for dz in DIST:
        p1_copy(1, dz).start()

    blane = lax.rem(lax.div(lax.broadcasted_iota(jnp.int32, (32, 1024), 1), 4), 16)
    ct = ctv[...]

    def table(b, c):
        rows = pl.ds(pl.multiple_of(b * 32, 32), 32)
        mtab[rows, :] = jnp.where(blane == b, ct, 0.0).astype(BF16)
        return c

    lax.fori_loop(0, 16, table, 0)

    def source(dz):
        return lax.rem(z + 8 - dz, 8)

    def at(d):
        return [source(dz) for dz in ((d,) if d in (0, 4) else (d, 8 - d))]

    def relay(p, d):
        landed(pz.at[p, pl.ds(0, len(at(d)))], p1r.at[p, d - 1])
        for zs in at(d):
            for side in range(2):
                p2_copy(pz.at[p, zs], p, zs, side, d).start()

    def forward(p, d):
        landed(pb.at[p, 0, pl.ds(0, 2 * len(at(d)))], p2r.at[p, d])
        for zs in at(d):
            p3_copy(p, 0, zs).start()
            p3_copy(p, 1, zs).start()

    def gathered_z(d):
        landed(rc.at[0, 0, pl.ds(0, len(at(d)))], rbr.at[d - 1])
        for zs in at(d):
            x_copy(zs, d).start()
            near_y(0, zs)

    def gathered_x(d):
        landed(rc.at[1, 0, pl.ds(0, len(at(d)))], rxr.at[d])
        for zs in at(d):
            near_y(1, zs)

    def gathered_y(o):
        landed(rc.at[o, pl.ds(0, 3)], rcr.at[o])
        for b in range(4):
            rto[128 * o : 128 * o + 128, 256 * b : 256 * b + 256] = rc[o, b, :, 0:32, :].reshape(256, 128).T
            rtv[128 * o : 128 * o + 128, 128 * b : 128 * b + 128] = rc[o, b, :, 32:48, :].reshape(128, 128).T

    def g_rows(t, kk):
        o = jnp.abs(lax.div(t, 2) - xl)
        return pl.ds(pl.multiple_of(128 * o + 64 * lax.rem(t, 2) + 32 * kk, 32), 32)

    def g_copy(p, t, kk):
        return pltpu.make_async_remote_copy(
            src_ref=gp.at[p, g_rows(t, kk)], dst_ref=pr.at[p, z], send_sem=gs, recv_sem=gr.at[p, lax.div(z, 2)],
            device_id=(row_of(xh, 4 * core + t, kk), col), device_id_type=MESH,
        )

    own = lax.div(z, 4) == core
    place = lax.rem(z, 4)
    inner = jnp.logical_or(place == 1, place == 2)

    def nearest(j):
        t = jnp.where(inner, 1 - j if j < 2 else j, j)
        return jnp.where(place >= 2, 3 - t, t)

    def multiply(p):
        acc_o = jnp.zeros((256, 256), F32)
        acc_v = jnp.zeros((256, 256), F32)
        for b in range(4):
            left = rto[:, 256 * b : 256 * b + 256]
            acc_o += mdot(left, pb[p, b, :, 0:32, :].reshape(256, 256))
            left = rtv[:, 128 * b : 128 * b + 128]
            acc_v += mdot(left, pb[p, b, :, 32:48, :].reshape(128, 256))
        gp[p] = (acc_o * acc_v * SCALE).astype(BF16)
        for j in range(4):
            t = jnp.where(own, nearest(j), nearest(3 - j))
            for kk in range(2):
                mine = row == row_of(xh, 4 * core + t, kk)

                @pl.when(jnp.logical_not(mine))
                def _():
                    g_copy(p, t, kk).start()

                @pl.when(mine)
                def _():
                    pr[p, z] = gp[p, g_rows(t, kk)]

    relay(0, 1)
    relay(0, 2)
    for d in range(1, 5):
        gathered_z(d)
    relay(0, 3)
    relay(0, 4)
    for side in range(2):
        p2_copy(inb.at[:, part_of(z, 1)], 1, z, side, 0).start()
    for d in range(5):
        gathered_x(d)
    for d in range(3):
        forward(0, d)
    relay(1, 1)
    relay(1, 2)
    forward(0, 3)
    forward(0, 4)
    relay(1, 3)
    relay(1, 4)
    gathered_y(0)
    gathered_y(1)
    pl.semaphore_wait(ready, 16)
    def compute(p, carry):
        landed(pb.at[p, pl.ds(0, 2)], p3r.at[p])
        multiply(p)

        @pl.when(p == 0)
        def _():
            for d in range(5):
                forward(1, d)

        return carry

    lax.fori_loop(0, 2, compute, 0)

    slot = 8 * ((1 - xl) * 4 + y)

    def y_copy(p, q, c):
        lanes = pl.ds(pl.multiple_of(c * 128, 128), 128)
        return pltpu.make_async_remote_copy(
            src_ref=xs.at[p, pl.ds(2 * q, 2), :, lanes], dst_ref=xr.at[p, pl.ds(slot + 2 * q, 2)],
            send_sem=ys, recv_sem=yr.at[p, q], device_id=(row, c), device_id_type=MESH,
        )

    def pair(g):
        near = 3 - 2 * lax.rem(z, 2)
        step = jnp.where(g == 0, 0, jnp.where(g == 1, near, jnp.where(g == 2, 4 - near, 2)))
        return lax.rem(lax.div(z, 2) + step, 4)

    def spread(p, groups):
        sides = [[], []]
        for q in groups:
            mine = jnp.logical_and(own, q == lax.div(z, 2))

            @pl.when(mine)
            def _():
                landed(pr.at[p, 0], gr.at[p, q])

            @pl.when(jnp.logical_not(mine))
            def _():
                landed(pr.at[p, pl.ds(0, 2)], gr.at[p, q])

        for q in groups:
            block = pr[p, pl.ds(2 * q, 2)]
            for side in range(2):
                sides[side].append(block[:, 16 * side : 16 * side + 16].reshape(32, 256))
        both = jnp.concatenate([jnp.concatenate(side, axis=0) for side in sides], axis=1)
        res = mdot(both, mtab[...]).astype(BF16)
        for n, q in enumerate(groups):
            xs[p, pl.ds(2 * q, 2)] = res[32 * n : 32 * n + 32].reshape(2, 16, 1024)

        def y_send(j, carry):
            for q in groups:
                y_copy(p, q, lax.rem(col + j, 8)).start()
            return carry

        lax.fori_loop(1, 8, y_send, 0)
        lanes = pl.ds(pl.multiple_of(col * 128, 128), 128)
        for q in groups:
            xr[p, pl.ds(slot + 2 * q, 2)] = xs[p, pl.ds(2 * q, 2), :, lanes]

    def spread_next(n, carry):
        spread(lax.div(n, 4), (pair(lax.rem(n, 4)),))
        return carry

    lax.fori_loop(0, 8, spread_next, 0)

    for p in range(2):
        def b_step(g, carry):
            q = pair(g)
            landed(xr.at[p, pl.ds(0, 14)], yr.at[p, q])
            parts = [xr[p, 8 * c + 2 * q + t] for t in range(2) for c in range(8)]
            both = jnp.concatenate([jnp.concatenate(parts[8 * t : 8 * t + 8], axis=0) for t in range(2)], axis=1)
            res = mdot(both, ntab[p])
            for c in range(8):
                block = res[16 * c : 16 * c + 16]
                zb[4 * c + q] = block if p == 0 else zb[4 * c + q] + block
            return carry

        lax.fori_loop(0, 4, b_step, 0)

    @pl.when(jnp.logical_and(col == 0, jnp.logical_not(self_a)))
    def _():
        landed(rc.at[0, 0], ras)

    @pl.when(self_a)
    def _():
        landed(rc.at[0, 0, pl.ds(0, 7)], ras)

    for p in range(2):
        landed(pz.at[p, pl.ds(0, 7)], p1s)
        landed(pb.at[p, pl.ds(0, 2)], p2s)
        landed(pb.at[p, pl.ds(0, 2)], p3s)
    landed(rc.at[0, 0, pl.ds(0, 7)], rbs)
    landed(rc.at[0, 0], rxs)
    landed(rc.at[0, pl.ds(0, 3)], rcs)
    landed(rc.at[1, pl.ds(0, 3)], rcs)

    for p in range(2):
        landed(xr.at[p, pl.ds(0, 56)], ys)

    @pl.when(own)
    def _():
        landed(pr.at[:, pl.ds(0, 7)], gs)

    @pl.when(jnp.logical_not(own))
    def _():
        landed(pr, gs)


def finish(zb, out_re, out_im, res_re, res_im, first, second, sem):
    lane = lax.broadcasted_iota(jnp.int32, (8, 128), 1)

    def put(i, which):
        res, out = ((res_re, out_re), (res_im, out_im))[which]
        rows = pl.ds(8 * i, 8)
        return pltpu.make_async_copy(res.at[rows], out.at[rows], sem.at[which, i])

    def a_step(i, carry):
        rows = pl.ds(pl.multiple_of(8 * lax.rem(i, 2), 8), 8)
        real = pl.ds(pl.multiple_of(256 * lax.div(i, 2), 128), 128)
        imag = pl.ds(pl.multiple_of(256 * lax.div(i, 2) + 128, 128), 128)
        for q in range(8):
            quarter = fft([(zb[8 * n + q, rows, real], zb[8 * n + q, rows, imag]) for n in range(4)])
            for k in range(4):
                c, s = math.cos(2 * math.pi * q * k / 32), math.sin(2 * math.pi * q * k / 32)
                (re, im) = quarter[k]
                first[k, q, 0] = c * re + s * im if q * k else re
                first[k, q, 1] = c * im - s * re if q * k else im
        for k in range(4):
            eighth = fft([(first[k, q, 0], first[k, q, 1]) for q in range(8)])
            for j in range(8):
                second[j, k, 0], second[j, k, 1] = eighth[j]
        for part, out in ((0, res_re), (1, res_im)):
            for n in range(4):
                moved = []
                for j in (2 * n, 2 * n + 1):
                    moved += swap_groups([second[j, t, part] for t in range(4)], lane)
                out[pl.ds(8 * i, 8), 8 * n : 8 * n + 8, :] = jnp.swapaxes(jnp.stack(moved), 0, 1)
            put(i, part).start()
        return carry

    lax.fori_loop(0, 4, a_step, 0)
    for i in range(4):
        put(i, 0).wait()
        put(i, 1).wait()


def on_device(occ, vir, docc, dvir):
    anyspace = pl.BlockSpec(memory_space=pl.ANY)
    vmem = pl.BlockSpec(memory_space=pltpu.VMEM)
    dma = pltpu.SemaphoreType.DMA
    zb = pl.pallas_call(
        kernel,
        out_shape=pltpu.VMEM((32, 16, 512), F32),
        in_specs=[anyspace] * 6,
        out_specs=vmem,
        scratch_shapes=[
            pltpu.VMEM((48, 4096), BF16),
            pltpu.VMEM((1, 1024), F32),
            pltpu.VMEM((1, 512), F32),
            pltpu.VMEM((32, 1024), F32),
            pltpu.VMEM((512, 1024), BF16),
            pltpu.VMEM((2, 256, 512), BF16),
            pltpu.VMEM((2, 8, 48, 256), BF16),
            pltpu.VMEM((2, 4, 8, 48, 256), BF16),
            pltpu.VMEM((48, 1024), BF16),
            pltpu.VMEM((2, 4, 8, 48, 128), BF16),
            pltpu.VMEM((256, 1024), BF16),
            pltpu.VMEM((256, 512), BF16),
            pltpu.VMEM((2, 256, 256), BF16),
            pltpu.VMEM((2, 8, 32, 256), BF16),
            pltpu.VMEM((2, 8, 16, 1024), BF16),
            pltpu.VMEM((2, 64, 16, 128), BF16),
            dma((6,)),
            dma, dma((2, 4)),
            dma, dma((2, 5)),
            dma, dma((2,)),
            dma, dma,
            dma, dma((4,)),
            dma, dma((5,)),
            dma, dma((2,)),
            dma, dma((2, 4)),
            dma, dma((2, 4)),
            pltpu.SemaphoreType.REGULAR,
        ],
        compiler_params=pltpu.CompilerParams(collective_id=0, has_side_effects=True),
    )(
        occ, vir, docc.reshape(1, 1024), dvir.reshape(1, 512),
        jnp.asarray(c_table()), jnp.asarray(b_table()).astype(BF16),
    )
    out = jax.ShapeDtypeStruct((32, 32, 128), F32)
    res = pl.pallas_call(
        finish,
        out_shape=(out, out),
        in_specs=[vmem],
        out_specs=(anyspace, anyspace),
        scratch_shapes=[
            pltpu.VMEM((32, 32, 128), F32),
            pltpu.VMEM((32, 32, 128), F32),
            pltpu.VMEM((4, 8, 2, 8, 128), F32),
            pltpu.VMEM((8, 4, 2, 8, 128), F32),
            dma((2, 4)),
        ],
    )(pltpu.with_memory_space_constraint(zb, pltpu.VMEM))

    def placed(part):
        return jnp.transpose(part.reshape(32, 8, 4, 128), (0, 2, 1, 3)).reshape(32, 4, 1024)

    return placed(res[0]), placed(res[1])


def solution(mesh):
    in_specs = (P("row", "col"), P("row", "col"), P(), P())
    out_specs = (P("row", "col", None), P("row", "col", None))
    return jax.shard_map(
        on_device, mesh=mesh, in_specs=in_specs, out_specs=out_specs, check_vma=False
    )
```
